16 devices in a mesh: dp: 4 (over z, y), sp: 4 (over x, core).
Axes of the slice: x: 2, y: 2, z: 2, core: 2. Of those that a mesh axis runs over, the one named last changes fastest.
Arguments:
- x_special: bfloat16 [16, 2, 768], P('dp'), parts along dimension 0
- x_patch: bfloat16 [16, 1024, 768], P('dp', 'sp'), parts along dimension 0
- dy_special: bfloat16 [16, 2, 768], P('dp'), parts along dimension 0
- dy_patch: bfloat16 [16, 1024, 768], P('dp', 'sp'), parts along dimension 0
- ln_scale: float32 [768], replicated
- ln_bias: float32 [768], replicated
- w_qkv: bfloat16 [768, 2304], replicated
- b_qkv: float32 [2304], replicated
- w_proj: bfloat16 [768, 768], replicated
- b_proj: float32 [768], replicated
- layer_scale: float32 [768], replicated
Outputs:
- output 1: bfloat16 [16, 2, 768], P('dp'), parts along dimension 0
- output 2: bfloat16 [16, 1024, 768], P('dp', 'sp'), parts along dimension 0
- output 3: bfloat16 [16, 2, 768], P('dp'), parts along dimension 0
- output 4: bfloat16 [16, 1024, 768], P('dp', 'sp'), parts along dimension 0
- output 5: float32 [3072], P('dp'), parts along dimension 0
- output 6: float32 [3072], P('dp'), parts along dimension 0
- output 7: float32 [3072, 2304], P('dp'), parts along dimension 0
- output 8: float32 [9216], P('dp'), parts along dimension 0
- output 9: float32 [3072, 768], P('dp'), parts along dimension 0
- output 10: float32 [3072], P('dp'), parts along dimension 0
- output 11: float32 [3072], P('dp'), parts along dimension 0
There are 4 independent parts. The reference program is written for one: setup_inputs(seed, part) draws one part's arguments, and reference() takes and returns one part's arrays. A program takes and returns all parts, laid end to end along the dimension named above; an argument that names none is the same for every part.
All inputs are finite; a program needn't handle non-finite values.
Results may differ from the reference program's by a relative error of at most 0.0101605.
Values are sent between devices in bfloat16 or wider.
A program may use at most 1 GiB of HBM per device.

```python
import jax
import jax.numpy as jnp
from jax import lax

IMAGES = 4
PATCHES = 1024
SPECIAL = 2
D_MODEL = 768
NUM_HEADS = 12
HEAD_DIM = 64
TEXTURES = 8
TOKENS = SPECIAL + PATCHES
LN_EPS = 1e-6
ATTN_SCALE = HEAD_DIM ** -0.5


def setup_inputs(seed: int = 0, part: int = 0) -> dict:
    part_keys = jax.random.split(jax.random.fold_in(jax.random.key(seed), part), 7)
    weight_keys = jax.random.split(jax.random.key(seed + 1), 9)
    common = jax.random.normal(part_keys[0], (IMAGES, 1, D_MODEL), jnp.float32)
    texture = jax.random.normal(part_keys[1], (IMAGES, TEXTURES, D_MODEL), jnp.float32)
    tex_id = jax.random.randint(part_keys[2], (IMAGES, PATCHES), 0, TEXTURES)
    onehot = (tex_id[:, :, None] == jnp.arange(TEXTURES)[None, None, :]).astype(jnp.float32)
    patch_vals = jnp.einsum('bnt,btd->bnd', onehot, texture) + 0.7 * common + 0.5 * jax.random.normal(part_keys[3], (IMAGES, PATCHES, D_MODEL), jnp.float32)
    special_vals = 3.0 * common + 0.5 * jax.random.normal(part_keys[4], (IMAGES, SPECIAL, D_MODEL), jnp.float32)
    dy_special = jax.random.normal(part_keys[5], (IMAGES, SPECIAL, D_MODEL), jnp.float32)
    dy_patch = jax.random.normal(part_keys[6], (IMAGES, PATCHES, D_MODEL), jnp.float32)
    fan_scale = D_MODEL ** -0.5
    w_query = jax.random.normal(weight_keys[0], (D_MODEL, D_MODEL), jnp.float32)
    w_key = 0.6 * w_query + 0.8 * jax.random.normal(weight_keys[1], (D_MODEL, D_MODEL), jnp.float32)
    w_value = jax.random.normal(weight_keys[2], (D_MODEL, D_MODEL), jnp.float32)
    w_qkv = jnp.concatenate([w_query, w_key, w_value], axis=1) * fan_scale
    w_proj = jax.random.normal(weight_keys[3], (D_MODEL, D_MODEL), jnp.float32) * fan_scale
    return {
        'x_special': special_vals.astype(jnp.bfloat16),
        'x_patch': patch_vals.astype(jnp.bfloat16),
        'dy_special': dy_special.astype(jnp.bfloat16),
        'dy_patch': dy_patch.astype(jnp.bfloat16),
        'ln_scale': 1.0 + 0.2 * jax.random.normal(weight_keys[4], (D_MODEL,), jnp.float32),
        'ln_bias': 0.3 * jax.random.normal(weight_keys[5], (D_MODEL,), jnp.float32),
        'w_qkv': w_qkv.astype(jnp.bfloat16),
        'b_qkv': 0.3 * jax.random.normal(weight_keys[6], (3 * D_MODEL,), jnp.float32),
        'w_proj': w_proj.astype(jnp.bfloat16),
        'b_proj': 0.3 * jax.random.normal(weight_keys[7], (D_MODEL,), jnp.float32),
        'layer_scale': jax.random.uniform(weight_keys[8], (D_MODEL,), jnp.float32, 0.4, 1.2),
    }


def head_attention(head_qkv):
    queries = head_qkv[0].astype(jnp.float32)
    key_rows = head_qkv[1].astype(jnp.float32)
    value_rows = head_qkv[2].astype(jnp.float32)
    scores = jnp.dot(queries, key_rows.T) * ATTN_SCALE
    attn_prob = jax.nn.softmax(scores, axis=-1)
    return jnp.dot(attn_prob.astype(jnp.bfloat16).astype(jnp.float32), value_rows).astype(jnp.bfloat16)


def block_forward(x_all, ln_scale, ln_bias, w_qkv, b_qkv, w_proj, b_proj, layer_scale):
    x_float = x_all.astype(jnp.float32)
    centered = x_float - jnp.mean(x_float, axis=-1, keepdims=True)
    inv_std = lax.rsqrt(jnp.mean(centered * centered, axis=-1, keepdims=True) + LN_EPS)
    normed = (centered * inv_std * ln_scale + ln_bias).astype(jnp.bfloat16)
    qkv_rows = jnp.einsum('btd,de->bte', normed.astype(jnp.float32), w_qkv.astype(jnp.float32)) + b_qkv
    qkv_rows = qkv_rows.astype(jnp.bfloat16).reshape(IMAGES, TOKENS, 3, NUM_HEADS, HEAD_DIM)
    per_head = jnp.transpose(qkv_rows, (0, 3, 2, 1, 4)).reshape(IMAGES * NUM_HEADS, 3, TOKENS, HEAD_DIM)
    attn_out = lax.map(jax.checkpoint(head_attention), per_head)
    attn_out = jnp.transpose(attn_out.reshape(IMAGES, NUM_HEADS, TOKENS, HEAD_DIM), (0, 2, 1, 3)).reshape(IMAGES, TOKENS, D_MODEL)
    proj_out = jnp.einsum('btd,de->bte', attn_out.astype(jnp.float32), w_proj.astype(jnp.float32)) + b_proj
    return (x_float + layer_scale * proj_out).astype(jnp.bfloat16)


def reference(x_special, x_patch, dy_special, dy_patch, ln_scale, ln_bias, w_qkv, b_qkv, w_proj, b_proj, layer_scale):
    x_all = jnp.concatenate([x_special, x_patch], axis=1)
    dy_all = jnp.concatenate([dy_special, dy_patch], axis=1)
    out_all, block_vjp = jax.vjp(block_forward, x_all, ln_scale, ln_bias, w_qkv, b_qkv, w_proj, b_proj, layer_scale)
    grad_list = block_vjp(dy_all)
    dx_all = grad_list[0]
    return (out_all[:, :SPECIAL], out_all[:, SPECIAL:], dx_all[:, :SPECIAL], dx_all[:, SPECIAL:], grad_list[1], grad_list[2], grad_list[3].astype(jnp.float32), grad_list[4], grad_list[5].astype(jnp.float32), grad_list[6], grad_list[7])
```

```python
import functools
import jax, jax.numpy as jnp
from jax import lax
from jax.sharding import PartitionSpec as P
from jax.experimental import pallas as pl
from jax.experimental.pallas import tpu as pltpu
F32=jnp.float32; BF=jnp.bfloat16
T=1040; NT=1026; QB=256
NEG=-1e30
def nt(a,b): return lax.dot_general(a,b,(((1,),(1,)),((),())),preferred_element_type=F32)
def nn(a,b): return jnp.dot(a,b,preferred_element_type=F32)
CH=[(0,256),(256,256),(512,256),(768,272)]
def fold(x,op):
    r=x.shape[0]//8
    x=x.reshape(r,8,x.shape[1])
    g=[x[i] for i in range(r)]
    while len(g)>1:
        g=[op(g[i],g[i+1]) for i in range(0,len(g)-1,2)]+([g[-1]] if len(g)%2 else [])
    return g[0]

def attn_kernel(num_alias,q_ref,k_ref,v_ref,do_ref,*refs):
    a_ref,dqkv_ref,qs,s_scr,p_scr,ds_scr,dor,qr,kT,vT,doT,dvk=refs[num_alias:]
    lane=lax.broadcasted_iota(jnp.int32,(1,128),1)
    kT[...]=k_ref[...].T; vT[...]=v_ref[...].T; doT[...]=do_ref[...].T
    qs[...]=(q_ref[...].astype(F32)*0.125).astype(BF)
    z=jnp.zeros((QB,128),BF)
    units=[(qb,h) for qb in range(4) for h in range(2)]
    U=len(units)
    st=[dict() for _ in units]
    for u,(qb,h) in enumerate(units):
        mh=(lane<64) if h==0 else (lane>=64)
        rows=slice(qb*QB,(qb+1)*QB)
        qr[u*QB:(u+1)*QB,:]=jnp.where(mh,qs[rows,:],z)
        dor[u*QB:(u+1)*QB,:]=jnp.where(mh,do_ref[rows,:],z)
    def A(u,c):
        r0,n=CH[c]; s_ref=s_scr.at[u%4]
        s=nt(k_ref[r0:r0+n,:],qr[u*QB:(u+1)*QB,:])
        if c==3:
            s=jnp.concatenate([s[:256],jnp.where(lax.broadcasted_iota(jnp.int32,(16,QB),0)<2,s[256:],NEG)],0)
        s_ref[r0:r0+n,:]=s
        f=fold(s,jnp.maximum)
        st[u]['m']=f if c==0 else jnp.maximum(st[u]['m'],f)
        if c==3: st[u]['m']=jnp.max(st[u]['m'],axis=0,keepdims=True)
    def B(u,c):
        r0,n=CH[c]; s_ref=s_scr.at[u%4]
        e=jnp.exp(s_ref[r0:r0+n,:]-st[u]['m'])
        s_ref[r0:r0+n,:]=e
        f=fold(e,jnp.add)
        st[u]['l']=f if c==0 else st[u]['l']+f
        if c==3: st[u]['rl']=1.0/jnp.sum(st[u]['l'],axis=0,keepdims=True)
    def C(u,c):
        qb,h=units[u]; r0,n=CH[c]; s_ref=s_scr.at[u%4]
        plo=(s_ref[r0:r0+n,:]*st[u]['rl']).astype(BF)
        p_scr[r0:r0+n,u*QB:(u+1)*QB]=plo
        o=nn(vT[64*h:64*h+64,r0:r0+n],plo)
        st[u]['o']=o if c==0 else st[u]['o']+o
        if c==3:
            st[u]['delta']=jnp.sum(st[u]['o']*doT[64*h:64*h+64,qb*QB:(qb+1)*QB].astype(F32),axis=0,keepdims=True)
            if h==1:
                a_ref[qb*QB:(qb+1)*QB,:]=jnp.concatenate([st[u-1]['o'],st[u]['o']],0).T.astype(BF)
    def D(u,c):
        qb,h=units[u]; r0,n=CH[c]; s_ref=s_scr.at[u%4]
        dp=nt(v_ref[r0:r0+n,:],dor[u*QB:(u+1)*QB,:]).astype(BF).astype(F32)
        ds=((s_ref[r0:r0+n,:]*st[u]['rl'])*(dp-st[u]['delta'])).astype(BF)
        ds_scr[r0:r0+n,u*QB:(u+1)*QB]=ds
        o=nn(kT[64*h:64*h+64,r0:r0+n],ds)
        st[u]['dq']=o if c==0 else st[u]['dq']+o
        if c==3 and h==1:
            dqkv_ref[0,qb*QB:(qb+1)*QB,:]=(jnp.concatenate([st[u-1]['dq'],st[u]['dq']],0)*0.125).T.astype(BF)
    def E(qb,c):
        r0,n=CH[c]
        cols=slice(qb*512,(qb+1)*512)
        for w,(src,rhs) in enumerate(((p_scr,dor),(ds_scr,qr))):
            x=nn(src[r0:r0+n,cols],rhs[cols,:])
            dvk[w,r0:r0+n,:]=dvk[w,r0:r0+n,:]+x
    q16=qs[1024:,:]; do16=do_ref[1024:,:]
    z16=jnp.zeros_like(q16)
    qm=jnp.concatenate([jnp.where(lane<64,q16,z16),jnp.where(lane>=64,q16,z16)],0)
    dom=jnp.concatenate([jnp.where(lane<64,do16,z16),jnp.where(lane>=64,do16,z16)],0)
    s=nt(k_ref[...],qm)
    rowi=lax.broadcasted_iota(jnp.int32,(T,32),0)
    s=jnp.where(rowi<NT,s,NEG)
    m=jnp.max(fold(s,jnp.maximum),axis=0,keepdims=True); e=jnp.exp(s-m); l=jnp.sum(fold(e,jnp.add),axis=0,keepdims=True)
    p=e*(1.0/l); plo=p.astype(BF)
    oT=nn(vT[...],plo)
    domT=dom.T
    dp=nt(v_ref[...],dom).astype(BF).astype(F32)
    delta=jnp.sum(oT*domT.astype(F32),axis=0,keepdims=True)
    ds=(p*(dp-delta)).astype(BF)
    dqT=nn(kT[...],ds)*0.125
    def pick(xT):
        x=xT.T
        return jnp.where(lane<64,x[:16],x[16:])
    a_ref[1024:,:]=pick(oT).astype(BF)
    dqkv_ref[0,1024:,:]=pick(dqT).astype(BF)
    dvk[0]=nn(plo,dom)
    dvk[1]=nn(ds,qm)
    for t in range(U+5):
        for c in range(4):
            if t<U: A(t,c)
            if 0<=t-1<U: B(t-1,c)
            if 0<=t-2<U: C(t-2,c)
            if 0<=t-3<U: D(t-3,c)
            e=t-5
            if e>=0 and e//2<4 and c%2==0:
                E(e//2,(e%2)*2+c//2)
    if True:
        dqkv_ref[2]=dvk[0].astype(BF)
        dqkv_ref[1]=dvk[1].astype(BF)


LN_EPS = 1e-6
ANY = pl.BlockSpec(memory_space=pl.ANY)
RB = 208


def whole(shape):
    return pl.BlockSpec(shape, lambda *g: (0,) * len(shape))


def layer_stats(xf):
    cen = xf - jnp.mean(xf, axis=-1, keepdims=True)
    inv = lax.rsqrt(jnp.mean(cen * cen, axis=-1, keepdims=True) + LN_EPS)
    return cen * inv, inv


def attention(i, qkv, do, prev):
    spec = lambda o: pl.BlockSpec((T, 128), lambda j, o=o: (0, o + j))
    n = len(prev)
    return pl.pallas_call(
        functools.partial(attn_kernel, n), grid=(6,),
        in_specs=[spec(0), spec(6), spec(12), spec(0)] + [ANY] * n,
        out_specs=[pl.BlockSpec((None, T, 128), lambda j: (i, 0, j)), pl.BlockSpec((3, None, T, 128), lambda j: (0, i, 0, j))],
        out_shape=[jax.ShapeDtypeStruct((2, T, 768), BF), jax.ShapeDtypeStruct((3, 2, T, 768), BF)],
        input_output_aliases={4 + m: m for m in range(n)},
        scratch_shapes=[pltpu.VMEM((T, 128), BF), pltpu.VMEM((4, T, QB), F32), pltpu.VMEM((T, 2048), BF), pltpu.VMEM((T, 2048), BF),
                        pltpu.VMEM((2048, 128), BF), pltpu.VMEM((2048, 128), BF),
                        pltpu.VMEM((128, T), BF), pltpu.VMEM((128, T), BF), pltpu.VMEM((128, T), BF), pltpu.VMEM((2, T, 128), F32)],
        compiler_params=pltpu.CompilerParams(vmem_limit_bytes=60 * 1024 * 1024),
        cost_estimate=pl.CostEstimate(flops=48 * 12 * 1026 * 1026 * 64, bytes_accessed=12 * 1024 * 1024, transcendentals=12 * 1026 * 1026),
        name="attn")(qkv, qkv, qkv, do, *prev)


def assemble(i, patch, special, parts, buf, spec, sems):
    shard = lax.axis_index('sp')
    img = 2 * (shard & 1) + i
    copies = [pltpu.make_async_copy(special.at[img], spec, sems.at[4])]
    for b, src in enumerate((patch.at[img],) + tuple(parts)):
        rows = pl.ds(pl.multiple_of((shard ^ b) * 256, 256), 256)
        copies.append(pltpu.make_async_copy(src, buf.at[rows], sems.at[b]))
    for c in copies:
        c.start()
    for c in copies:
        c.wait()
    buf[1024:, :] = jnp.concatenate([spec[...], jnp.zeros((14, 768), BF)], 0)


def front_x_kernel(i, num_alias, patch, special, r1, r2, r3, w, b, ls, lb, *refs):
    qkv, normed, xs, buf, spec, sems = refs[num_alias:]
    g = pl.program_id(0)

    @pl.when(g == 0)
    def _():
        assemble(i, patch, special, (r1, r2, r3), buf, spec, sems)

    x = buf[pl.ds(pl.multiple_of(g * RB, 16), RB), :]
    xs[...] = x
    x_hat, _ = layer_stats(x.astype(F32))
    nb = (x_hat * ls[...] + lb[...]).astype(BF)
    normed[...] = nb
    for j in range(3):
        c = slice(768 * j, 768 * j + 768)
        qkv[:, c] = (nn(nb, w[:, c]) + b[:, c]).astype(BF)


def front_dy_kernel(i, num_alias, patch, special, r1, r2, r3, w, scale, *refs):
    do, d_proj, dys, buf, spec, sems = refs[num_alias:]
    g = pl.program_id(0)

    @pl.when(g == 0)
    def _():
        assemble(i, patch, special, (r1, r2, r3), buf, spec, sems)

    x = buf[pl.ds(pl.multiple_of(g * RB, 16), RB), :]
    dys[...] = x
    dp = (x.astype(F32) * scale[...]).astype(BF)
    d_proj[...] = dp
    do[...] = nt(dp, w[...]).astype(BF)


def front(i, kernel, width, patch, special, parts, consts, prev, flops):
    n = len(prev)
    first = 5 + len(consts)
    return pl.pallas_call(
        functools.partial(kernel, i, n), grid=(T // RB,),
        in_specs=[ANY] * 5 + [whole(c.shape) for c in consts] + [ANY] * n,
        out_specs=[pl.BlockSpec((RB, width), lambda g: (g, 0))] + [pl.BlockSpec((None, RB, 768), lambda g: (i, g, 0))] * 2,
        out_shape=[jax.ShapeDtypeStruct((T, width), BF)] + [jax.ShapeDtypeStruct((2, T, 768), BF)] * 2,
        input_output_aliases={first + m: 1 + m for m in range(n)},
        scratch_shapes=[pltpu.VMEM((T, 768), BF), pltpu.VMEM((2, 768), BF), pltpu.SemaphoreType.DMA((5,))],
        compiler_params=pltpu.CompilerParams(vmem_limit_bytes=32 * 1024 * 1024),
        cost_estimate=pl.CostEstimate(flops=flops, bytes_accessed=12 * 1024 * 1024, transcendentals=0),
        name="front")(patch, special, *parts, *consts, *prev)


def back_kernel(chip, x_ref, dy_ref, a_ref, dq_ref, xs_ref, dys_ref, as_ref, dqs_ref, w_ref, wp_ref, ls, bp, lsc, o_ref, os_ref, vec):
    i, r = pl.program_id(0), pl.program_id(1)

    def rows(x, dy, a, dq):
        xf, dyf = x.astype(F32), dy.astype(F32)
        x_hat, inv = layer_stats(xf)
        proj = nn(a, wp_ref[...]) + bp[...]
        out = (xf + lsc[...] * proj).astype(BF)
        dn = sum(nt(dq[j], w_ref[:, 768 * j:768 * j + 768]) for j in range(3)).astype(BF).astype(F32)
        gh = dn * ls[...]
        dr = inv * (gh - jnp.mean(gh, -1, keepdims=True) - x_hat * jnp.mean(gh * x_hat, -1, keepdims=True))
        red = lambda t: jnp.sum(t, axis=0, keepdims=True)
        sums = [red(dn * x_hat), red(dn), red(dyf * lsc[...]), red(dyf * proj)] + [red(dq[j].astype(F32)) for j in range(3)]
        return out, (dyf + dr).astype(BF), jnp.concatenate(sums + [jnp.zeros((1, 768), F32)], 0)

    out, dx, v = rows(x_ref[...], dy_ref[...], a_ref[...], [dq_ref[j] for j in range(3)])
    o_ref[0] = out
    o_ref[1] = dx

    @pl.when(r == 0)
    def _():
        @pl.when(i == 0)
        def _():
            vec[...] = jnp.zeros((8, 768), F32)
        so, sdx, sv = rows(xs_ref[...], dys_ref[...], as_ref[...], [dqs_ref[j] for j in range(3)])
        os_ref[0] = so
        os_ref[1] = sdx
        vec[...] += jnp.where(chip[0] == 0, 1.0, 0.0) * sv

    vec[...] += v


def back(chip, xs, dys, a, d_qkv, w_qkv, w_proj, ln_scale, b_proj, layer_scale):
    blk = pl.BlockSpec((None, 256, 768), lambda i, r, c: (i, 2 * c[0] + r, 0))
    sblk = pl.BlockSpec((None, 16, 768), lambda i, r, c: (i, 64, 0))
    return pl.pallas_call(
        back_kernel,
        grid_spec=pltpu.PrefetchScalarGridSpec(
            num_scalar_prefetch=1, grid=(2, 2),
            in_specs=[blk, blk, blk, pl.BlockSpec((3, None, 256, 768), lambda i, r, c: (0, i, 2 * c[0] + r, 0)),
                      sblk, sblk, sblk, pl.BlockSpec((3, None, 16, 768), lambda i, r, c: (0, i, 64, 0))]
            + [whole(s) for s in ((768, 2304), (768, 768), (1, 768), (1, 768), (1, 768))],
            out_specs=[pl.BlockSpec((2, None, None, 256, 768), lambda i, r, c: (0, r, i, 0, 0)),
                       pl.BlockSpec((2, None, 16, 768), lambda i, r, c: (0, i, 0, 0)), whole((8, 768))]),
        out_shape=[jax.ShapeDtypeStruct((2, 2, 2, 256, 768), BF), jax.ShapeDtypeStruct((2, 2, 16, 768), BF), jax.ShapeDtypeStruct((8, 768), F32)],
        compiler_params=pltpu.CompilerParams(vmem_limit_bytes=48 * 1024 * 1024),
        cost_estimate=pl.CostEstimate(flops=2 * 1056 * 768 * 3072, bytes_accessed=20 * 1024 * 1024, transcendentals=0),
        name="back")(chip, xs, dys, a, d_qkv, xs, dys, a, d_qkv, w_qkv, w_proj, ln_scale, b_proj, layer_scale)


def dyn(x, start, size, axis):
    return lax.dynamic_slice_in_dim(x, start, size, axis)


def solution(mesh):
    n = mesh.shape['sp']
    swaps = {b: [(s, s ^ b) for s in range(n)] for b in (1, 2, 3)}

    def swap(x, b):
        return lax.ppermute(x, 'sp', swaps[b])

    def local_block(x_special, x_patch, dy_special, dy_patch, ln_scale, ln_bias, w_qkv, b_qkv, w_proj, b_proj, layer_scale):
        shard = lax.axis_index('sp')
        chip, core = shard // 2, shard % 2
        row = lambda t: t.reshape(1, -1)

        def send(patch, i):
            mine = dyn(patch, 2 * core + i, 1, 0)[0]
            other = dyn(patch, 2 * (1 - core) + i, 1, 0)[0]
            return swap(other, 1), swap(mine, 2), swap(other, 3)

        parts = {}
        for i in range(2):
            parts['x', i] = send(x_patch, i)
            parts['dy', i] = send(dy_patch, i)
        prev_x, prev_dy, prev_a = (), (), ()
        for i in range(2):
            qkv, *prev_x = front(i, front_x_kernel, 2304, x_patch, x_special, parts['x', i],
                                 (w_qkv, row(b_qkv), row(ln_scale), row(ln_bias)), prev_x, 2 * T * 768 * 2304)
            d_attn, *prev_dy = front(i, front_dy_kernel, 768, dy_patch, dy_special, parts['dy', i],
                                     (w_proj, row(layer_scale)), prev_dy, 2 * T * 768 * 768)
            prev_a = attention(i, qkv, d_attn, prev_a)
        normed, xs = prev_x
        d_proj, dys = prev_dy
        a, d_qkv = prev_a
        both, both_spec, vec = back(chip.reshape(1), xs, dys, a, d_qkv, w_qkv, w_proj, row(ln_scale), row(b_proj), row(layer_scale))
        t = vec + swap(vec, 1)
        t = t + swap(t, 2)
        got = swap(dyn(both, 1 - core, 1, 1)[:, 0], 1)
        keep = dyn(both, core, 1, 1)[:, 0]
        spec = both_spec[:, :, :2]
        gspec = swap(spec, 1)
        lo = core == 0

        def merge(p, q):
            return jnp.concatenate([jnp.where(lo, p, q), jnp.where(lo, q, p)], 0)

        def tn(p, q):
            return lax.dot_general(p.reshape(2 * T, 768), q.reshape(2 * T, 768), (((0,), (0,)), ((), ())), preferred_element_type=F32)

        gp = tn(a, d_proj)
        gp = gp + swap(gp, 1)
        cols = []
        for j in range(3):
            part = tn(normed, d_qkv[j])
            cols.append(part + swap(part, 1))
        gq = jnp.concatenate(cols, 1)
        return (merge(spec[0], gspec[0]), merge(keep[0], got[0]), merge(spec[1], gspec[1]), merge(keep[1], got[1]),
                t[0], t[1], gq, t[4:7].reshape(-1), gp, t[2], t[3])

    rows, seq, rep = P('dp'), P('dp', 'sp'), P()
    return jax.shard_map(local_block, mesh=mesh,
                         in_specs=(rows, seq, rows, seq) + (rep,) * 7,
                         out_specs=(rows, seq, rows, seq) + (rows,) * 7, check_vma=False)
```

```python
import functools
import jax, jax.numpy as jnp
from jax import lax
from jax.sharding import PartitionSpec as P
from jax.experimental import pallas as pl
from jax.experimental.pallas import tpu as pltpu
F32=jnp.float32; BF=jnp.bfloat16
T=1040; NT=1026; QB=256
NEG=-1e30
def nt(a,b): return lax.dot_general(a,b,(((1,),(1,)),((),())),preferred_element_type=F32)
def nn(a,b): return jnp.dot(a,b,preferred_element_type=F32)
CH=[(0,256),(256,256),(512,256),(768,272)]
def fold(x,op):
    r=x.shape[0]//8
    x=x.reshape(r,8,x.shape[1])
    g=[x[i] for i in range(r)]
    while len(g)>1:
        g=[op(g[i],g[i+1]) for i in range(0,len(g)-1,2)]+([g[-1]] if len(g)%2 else [])
    return g[0]

def attn_kernel(num_alias,q_ref,k_ref,v_ref,do_ref,*refs):
    a_ref,dqkv_ref,qs,s_scr,p_scr,ds_scr,dor,qr,kT,vT,doT,dvk=refs[num_alias:]
    lane=lax.broadcasted_iota(jnp.int32,(1,128),1)
    kT[...]=k_ref[...].T; vT[...]=v_ref[...].T; doT[...]=do_ref[...].T
    qs[...]=(q_ref[...].astype(F32)*0.125).astype(BF)
    z=jnp.zeros((QB,128),BF)
    units=[(qb,h) for qb in range(4) for h in range(2)]
    U=len(units)
    st=[dict() for _ in units]
    for u,(qb,h) in enumerate(units):
        mh=(lane<64) if h==0 else (lane>=64)
        rows=slice(qb*QB,(qb+1)*QB)
        qr[u*QB:(u+1)*QB,:]=jnp.where(mh,qs[rows,:],z)
        dor[u*QB:(u+1)*QB,:]=jnp.where(mh,do_ref[rows,:],z)
    def A(u,c):
        r0,n=CH[c]; s_ref=s_scr.at[u%4]
        s=nt(k_ref[r0:r0+n,:],qr[u*QB:(u+1)*QB,:])
        if c==3:
            s=jnp.concatenate([s[:256],jnp.where(lax.broadcasted_iota(jnp.int32,(16,QB),0)<2,s[256:],NEG)],0)
        s_ref[r0:r0+n,:]=s
        f=fold(s,jnp.maximum)
        st[u]['m']=f if c==0 else jnp.maximum(st[u]['m'],f)
        if c==3: st[u]['m']=jnp.max(st[u]['m'],axis=0,keepdims=True)
    def B(u,c):
        r0,n=CH[c]; s_ref=s_scr.at[u%4]
        e=jnp.exp(s_ref[r0:r0+n,:]-st[u]['m'])
        s_ref[r0:r0+n,:]=e
        f=fold(e,jnp.add)
        st[u]['l']=f if c==0 else st[u]['l']+f
        if c==3: st[u]['rl']=1.0/jnp.sum(st[u]['l'],axis=0,keepdims=True)
    def C(u,c):
        qb,h=units[u]; r0,n=CH[c]; s_ref=s_scr.at[u%4]
        plo=(s_ref[r0:r0+n,:]*st[u]['rl']).astype(BF)
        p_scr[r0:r0+n,u*QB:(u+1)*QB]=plo
        o=nn(vT[64*h:64*h+64,r0:r0+n],plo)
        st[u]['o']=o if c==0 else st[u]['o']+o
        if c==3:
            st[u]['delta']=jnp.sum(st[u]['o']*doT[64*h:64*h+64,qb*QB:(qb+1)*QB].astype(F32),axis=0,keepdims=True)
            if h==1:
                a_ref[qb*QB:(qb+1)*QB,:]=jnp.concatenate([st[u-1]['o'],st[u]['o']],0).T.astype(BF)
    def D(u,c):
        qb,h=units[u]; r0,n=CH[c]; s_ref=s_scr.at[u%4]
        dp=nt(v_ref[r0:r0+n,:],dor[u*QB:(u+1)*QB,:]).astype(BF).astype(F32)
        ds=((s_ref[r0:r0+n,:]*st[u]['rl'])*(dp-st[u]['delta'])).astype(BF)
        ds_scr[r0:r0+n,u*QB:(u+1)*QB]=ds
        o=nn(kT[64*h:64*h+64,r0:r0+n],ds)
        st[u]['dq']=o if c==0 else st[u]['dq']+o
        if c==3 and h==1:
            dqkv_ref[0,qb*QB:(qb+1)*QB,:]=(jnp.concatenate([st[u-1]['dq'],st[u]['dq']],0)*0.125).T.astype(BF)
    def E(qb,c):
        r0,n=CH[c]
        cols=slice(qb*512,(qb+1)*512)
        for w,(src,rhs) in enumerate(((p_scr,dor),(ds_scr,qr))):
            x=nn(src[r0:r0+n,cols],rhs[cols,:])
            dvk[w,r0:r0+n,:]=dvk[w,r0:r0+n,:]+x
    q16=qs[1024:,:]; do16=do_ref[1024:,:]
    z16=jnp.zeros_like(q16)
    qm=jnp.concatenate([jnp.where(lane<64,q16,z16),jnp.where(lane>=64,q16,z16)],0)
    dom=jnp.concatenate([jnp.where(lane<64,do16,z16),jnp.where(lane>=64,do16,z16)],0)
    s=nt(k_ref[...],qm)
    rowi=lax.broadcasted_iota(jnp.int32,(T,32),0)
    s=jnp.where(rowi<NT,s,NEG)
    m=jnp.max(fold(s,jnp.maximum),axis=0,keepdims=True); e=jnp.exp(s-m); l=jnp.sum(fold(e,jnp.add),axis=0,keepdims=True)
    p=e*(1.0/l); plo=p.astype(BF)
    oT=nn(vT[...],plo)
    domT=dom.T
    dp=nt(v_ref[...],dom).astype(BF).astype(F32)
    delta=jnp.sum(oT*domT.astype(F32),axis=0,keepdims=True)
    ds=(p*(dp-delta)).astype(BF)
    dqT=nn(kT[...],ds)*0.125
    def pick(xT):
        x=xT.T
        return jnp.where(lane<64,x[:16],x[16:])
    a_ref[1024:,:]=pick(oT).astype(BF)
    dqkv_ref[0,1024:,:]=pick(dqT).astype(BF)
    dvk[0]=nn(plo,dom)
    dvk[1]=nn(ds,qm)
    for t in range(U+5):
        for c in range(4):
            if t<U: A(t,c)
            if 0<=t-1<U: B(t-1,c)
            if 0<=t-2<U: C(t-2,c)
            if 0<=t-3<U: D(t-3,c)
            e=t-5
            if e>=0 and e//2<4 and c%2==0:
                E(e//2,(e%2)*2+c//2)
    if True:
        dqkv_ref[2]=dvk[0].astype(BF)
        dqkv_ref[1]=dvk[1].astype(BF)


LN_EPS = 1e-6
ANY = pl.BlockSpec(memory_space=pl.ANY)
RB = 208


def whole(shape):
    return pl.BlockSpec(shape, lambda *g: (0,) * len(shape))


def layer_stats(xf):
    cen = xf - jnp.mean(xf, axis=-1, keepdims=True)
    inv = lax.rsqrt(jnp.mean(cen * cen, axis=-1, keepdims=True) + LN_EPS)
    return cen * inv, inv


def attention(i, qkv, do, prev):
    spec = lambda o: pl.BlockSpec((T, 128), lambda j, o=o: (0, o + j))
    n = len(prev)
    return pl.pallas_call(
        functools.partial(attn_kernel, n), grid=(6,),
        in_specs=[spec(0), spec(6), spec(12), spec(0)] + [ANY] * n,
        out_specs=[pl.BlockSpec((None, T, 128), lambda j: (i, 0, j)), pl.BlockSpec((3, None, T, 128), lambda j: (0, i, 0, j))],
        out_shape=[jax.ShapeDtypeStruct((2, T, 768), BF), jax.ShapeDtypeStruct((3, 2, T, 768), BF)],
        input_output_aliases={4 + m: m for m in range(n)},
        scratch_shapes=[pltpu.VMEM((T, 128), BF), pltpu.VMEM((4, T, QB), F32), pltpu.VMEM((T, 2048), BF), pltpu.VMEM((T, 2048), BF),
                        pltpu.VMEM((2048, 128), BF), pltpu.VMEM((2048, 128), BF),
                        pltpu.VMEM((128, T), BF), pltpu.VMEM((128, T), BF), pltpu.VMEM((128, T), BF), pltpu.VMEM((2, T, 128), F32)],
        compiler_params=pltpu.CompilerParams(vmem_limit_bytes=63 * 1024 * 1024),
        cost_estimate=pl.CostEstimate(flops=48 * 12 * 1026 * 1026 * 64, bytes_accessed=12 * 1024 * 1024, transcendentals=12 * 1026 * 1026),
        name="attn")(qkv, qkv, qkv, do, *prev)


def assemble(i, patch, special, parts, buf, spec, sems):
    shard = lax.axis_index('sp')
    img = 2 * (shard & 1) + i
    copies = [pltpu.make_async_copy(special.at[img], spec, sems.at[4])]
    for b, src in enumerate((patch.at[img],) + tuple(parts)):
        rows = pl.ds(pl.multiple_of((shard ^ b) * 256, 256), 256)
        copies.append(pltpu.make_async_copy(src, buf.at[rows], sems.at[b]))
    for c in copies:
        c.start()
    for c in copies:
        c.wait()
    buf[1024:, :] = jnp.concatenate([spec[...], jnp.zeros((14, 768), BF)], 0)


def front_x_kernel(i, num_alias, patch, special, r1, r2, r3, w, b, ls, lb, *refs):
    qkv, normed, xs, buf, spec, sems = refs[num_alias:]
    g = pl.program_id(0)

    @pl.when(g == 0)
    def _():
        assemble(i, patch, special, (r1, r2, r3), buf, spec, sems)

    x = buf[pl.ds(pl.multiple_of(g * RB, 16), RB), :]
    xs[...] = x
    x_hat, _ = layer_stats(x.astype(F32))
    nb = (x_hat * ls[...] + lb[...]).astype(BF)
    normed[...] = nb
    for j in range(3):
        c = slice(768 * j, 768 * j + 768)
        qkv[:, c] = (nn(nb, w[:, c]) + b[:, c]).astype(BF)


def front_dy_kernel(i, num_alias, patch, special, r1, r2, r3, w, scale, *refs):
    do, d_proj, dys, buf, spec, sems = refs[num_alias:]
    g = pl.program_id(0)

    @pl.when(g == 0)
    def _():
        assemble(i, patch, special, (r1, r2, r3), buf, spec, sems)

    x = buf[pl.ds(pl.multiple_of(g * RB, 16), RB), :]
    dys[...] = x
    dp = (x.astype(F32) * scale[...]).astype(BF)
    d_proj[...] = dp
    do[...] = nt(dp, w[...]).astype(BF)


def front(i, kernel, width, patch, special, parts, consts, prev, flops):
    n = len(prev)
    first = 5 + len(consts)
    return pl.pallas_call(
        functools.partial(kernel, i, n), grid=(T // RB,),
        in_specs=[ANY] * 5 + [whole(c.shape) for c in consts] + [ANY] * n,
        out_specs=[pl.BlockSpec((RB, width), lambda g: (g, 0))] + [pl.BlockSpec((None, RB, 768), lambda g: (i, g, 0))] * 2,
        out_shape=[jax.ShapeDtypeStruct((T, width), BF)] + [jax.ShapeDtypeStruct((2, T, 768), BF)] * 2,
        input_output_aliases={first + m: 1 + m for m in range(n)},
        scratch_shapes=[pltpu.VMEM((T, 768), BF), pltpu.VMEM((2, 768), BF), pltpu.SemaphoreType.DMA((5,))],
        compiler_params=pltpu.CompilerParams(vmem_limit_bytes=63 * 1024 * 1024),
        cost_estimate=pl.CostEstimate(flops=flops, bytes_accessed=12 * 1024 * 1024, transcendentals=0),
        name="front")(patch, special, *parts, *consts, *prev)


def first_kernel(x_patch, dy_patch, x_special, dy_special, wq, bq, ls, lb, wp, lsc,
                 qkv_o, do_o, normed_o, xs_o, dproj_o, dys_o,
                 xbuf, dbuf, spec, qkv, do, normed, dproj, send, recv, loc, osem):
    dp, me = lax.axis_index('dp'), lax.axis_index('sp')
    core = me & 1
    barrier = pltpu.get_barrier_semaphore()
    for b in (1, 2, 3):
        pl.semaphore_signal(barrier, inc=1, device_id=(dp, me ^ b), device_id_type=pl.DeviceIdType.MESH)
    pl.semaphore_wait(barrier, 3)
    rows = lambda b: pl.ds(pl.multiple_of((me ^ b) * 256, 256), 256)
    remote = {}
    for k, (patch, buf) in enumerate(((x_patch, xbuf), (dy_patch, dbuf))):
        for b in (1, 2, 3):
            c = pltpu.make_async_remote_copy(
                src_ref=patch.at[2 * (core ^ (b & 1))], dst_ref=buf.at[rows(0)],
                send_sem=send.at[3 * k + b - 1], recv_sem=recv.at[3 * k + b - 1],
                device_id=(dp, me ^ b), device_id_type=pl.DeviceIdType.MESH)
            c.start()
            remote[k, b] = c
    local = []
    for k, (patch, buf, special) in enumerate(((x_patch, xbuf, x_special), (dy_patch, dbuf, dy_special))):
        own = pltpu.make_async_copy(patch.at[2 * core], buf.at[rows(0)], loc.at[2 * k])
        sp = pltpu.make_async_copy(special.at[2 * core], spec.at[k], loc.at[2 * k + 1])
        own.start()
        sp.start()
        local.append((own, sp))
    outs = []

    def emit(src, dst, r):
        c = pltpu.make_async_copy(src.at[r], dst.at[r], osem.at[len(outs)])
        c.start()
        outs.append(c)

    def do_x(r):
        x = xbuf[r, :]
        x_hat, _ = layer_stats(x.astype(F32))
        nb = (x_hat * ls[...] + lb[...]).astype(BF)
        normed[r, :] = nb
        for j in range(3):
            c = slice(768 * j, 768 * j + 768)
            qkv[r, c] = (nn(nb, wq[:, c]) + bq[:, c]).astype(BF)
        emit(xbuf, xs_o.at[0], r)
        emit(normed, normed_o.at[0], r)
        emit(qkv, qkv_o, r)

    def do_dy(r):
        d = (dbuf[r, :].astype(F32) * lsc[...]).astype(BF)
        dproj[r, :] = d
        do[r, :] = nt(d, wp[...]).astype(BF)
        emit(dbuf, dys_o.at[0], r)
        emit(dproj, dproj_o.at[0], r)
        emit(do, do_o, r)

    tail = pl.ds(1024, 16)
    for k, (buf, step) in enumerate(((xbuf, do_x), (dbuf, do_dy))):
        local[k][0].wait()
        local[k][1].wait()
        buf[1024:, :] = jnp.concatenate([spec[k], jnp.zeros((14, 768), BF)], 0)
        step(rows(0))
        step(tail)
        remote[k, 1].wait_recv()
        step(rows(1))
    for k, step in enumerate((do_x, do_dy)):
        for b in (2, 3):
            remote[k, b].wait_recv()
            step(rows(b))
    for c in remote.values():
        c.wait_send()
    for c in outs:
        c.wait()


def first(x_patch, dy_patch, x_special, dy_special, consts):
    two = jax.ShapeDtypeStruct((2, T, 768), BF)
    v = lambda s: pltpu.VMEM(s, BF)
    return pl.pallas_call(
        first_kernel,
        in_specs=[ANY] * 4 + [pl.BlockSpec(memory_space=pltpu.VMEM)] * 6,
        out_specs=[ANY] * 6,
        out_shape=[jax.ShapeDtypeStruct((T, 2304), BF), jax.ShapeDtypeStruct((T, 768), BF), two, two, two, two],
        scratch_shapes=[v((T, 768)), v((T, 768)), v((2, 2, 768)), v((T, 2304)), v((T, 768)), v((T, 768)), v((T, 768)),
                        pltpu.SemaphoreType.DMA((6,)), pltpu.SemaphoreType.DMA((6,)), pltpu.SemaphoreType.DMA((4,)), pltpu.SemaphoreType.DMA((30,))],
        compiler_params=pltpu.CompilerParams(collective_id=0, has_side_effects=True, vmem_limit_bytes=63 * 1024 * 1024),
        cost_estimate=pl.CostEstimate(flops=2 * T * 768 * 3072, bytes_accessed=24 * 1024 * 1024, transcendentals=0),
        name="first")(x_patch, dy_patch, x_special, dy_special, *consts)


def add_kernel(num_cols, num_alias, *refs):
    n = num_cols
    ins, outs = refs[:2 * n], refs[2 * n + num_alias:]
    cols = outs[0].shape[1] // 768
    for m in range(cols):
        outs[0][:, 768 * m:768 * m + 768] = ins[2 * m][...] + ins[2 * m + 1][...]
    for m in range(cols, n):
        outs[1][...] = ins[2 * m][...] + ins[2 * m + 1][...]


def add_parts(pairs, first_col, cols, prev):
    flat = [t for p in pairs for t in p]
    n = len(pairs)
    blk = pl.BlockSpec((128, 768), lambda g: (g, 0))
    out_specs = [pl.BlockSpec((128, 768 * cols), lambda g: (g, first_col // cols))]
    out_shape = [jax.ShapeDtypeStruct((768, 2304), F32)]
    if n > cols:
        out_specs.append(blk)
        out_shape.append(jax.ShapeDtypeStruct((768, 768), F32))
    return pl.pallas_call(
        functools.partial(add_kernel, n, len(prev)), grid=(6,),
        in_specs=[blk] * (2 * n) + [ANY] * len(prev), out_specs=out_specs, out_shape=out_shape,
        input_output_aliases={2 * n + m: m for m in range(len(prev))},
        compiler_params=pltpu.CompilerParams(vmem_limit_bytes=63 * 1024 * 1024),
        cost_estimate=pl.CostEstimate(flops=768 * 768 * n, bytes_accessed=12 * 768 * 768 * n, transcendentals=0),
        name="add_parts")(*flat, *prev)


def back_kernel(chip, x_ref, dy_ref, a_ref, dq_ref, xs_ref, dys_ref, as_ref, dqs_ref, w_ref, wp_ref, ls, bp, lsc, o_ref, os_ref, vec):
    i, r = pl.program_id(0), pl.program_id(1)

    def rows(x, dy, a, dq):
        xf, dyf = x.astype(F32), dy.astype(F32)
        x_hat, inv = layer_stats(xf)
        proj = nn(a, wp_ref[...]) + bp[...]
        out = (xf + lsc[...] * proj).astype(BF)
        dn = sum(nt(dq[j], w_ref[:, 768 * j:768 * j + 768]) for j in range(3)).astype(BF).astype(F32)
        gh = dn * ls[...]
        dr = inv * (gh - jnp.mean(gh, -1, keepdims=True) - x_hat * jnp.mean(gh * x_hat, -1, keepdims=True))
        red = lambda t: jnp.sum(t, axis=0, keepdims=True)
        sums = [red(dn * x_hat), red(dn), red(dyf * lsc[...]), red(dyf * proj)] + [red(dq[j].astype(F32)) for j in range(3)]
        return out, (dyf + dr).astype(BF), jnp.concatenate(sums + [jnp.zeros((1, 768), F32)], 0)

    out, dx, v = rows(x_ref[...], dy_ref[...], a_ref[...], [dq_ref[j] for j in range(3)])
    o_ref[0] = out
    o_ref[1] = dx

    @pl.when(r == 0)
    def _():
        @pl.when(i == 0)
        def _():
            vec[...] = jnp.zeros((8, 768), F32)
        so, sdx, sv = rows(xs_ref[...], dys_ref[...], as_ref[...], [dqs_ref[j] for j in range(3)])
        os_ref[0] = so
        os_ref[1] = sdx
        vec[...] += jnp.where(chip[0] == 0, 1.0, 0.0) * sv

    vec[...] += v


def back(chip, xs, dys, a, d_qkv, w_qkv, w_proj, ln_scale, b_proj, layer_scale):
    blk = pl.BlockSpec((None, 256, 768), lambda i, r, c: (i, 2 * c[0] + r, 0))
    sblk = pl.BlockSpec((None, 16, 768), lambda i, r, c: (i, 64, 0))
    return pl.pallas_call(
        back_kernel,
        grid_spec=pltpu.PrefetchScalarGridSpec(
            num_scalar_prefetch=1, grid=(2, 2),
            in_specs=[blk, blk, blk, pl.BlockSpec((3, None, 256, 768), lambda i, r, c: (0, i, 2 * c[0] + r, 0)),
                      sblk, sblk, sblk, pl.BlockSpec((3, None, 16, 768), lambda i, r, c: (0, i, 64, 0))]
            + [whole(s) for s in ((768, 2304), (768, 768), (1, 768), (1, 768), (1, 768))],
            out_specs=[pl.BlockSpec((2, None, None, 256, 768), lambda i, r, c: (0, r, i, 0, 0)),
                       pl.BlockSpec((2, None, 16, 768), lambda i, r, c: (0, i, 0, 0)), whole((8, 768))]),
        out_shape=[jax.ShapeDtypeStruct((2, 2, 2, 256, 768), BF), jax.ShapeDtypeStruct((2, 2, 16, 768), BF), jax.ShapeDtypeStruct((8, 768), F32)],
        compiler_params=pltpu.CompilerParams(vmem_limit_bytes=63 * 1024 * 1024),
        cost_estimate=pl.CostEstimate(flops=2 * 1056 * 768 * 3072, bytes_accessed=20 * 1024 * 1024, transcendentals=0),
        name="back")(chip, xs, dys, a, d_qkv, xs, dys, a, d_qkv, w_qkv, w_proj, ln_scale, b_proj, layer_scale)


def dyn(x, start, size, axis):
    return lax.dynamic_slice_in_dim(x, start, size, axis)


def solution(mesh):
    n = mesh.shape['sp']
    swaps = {b: [(s, s ^ b) for s in range(n)] for b in (1, 2, 3)}

    def swap(x, b):
        return lax.ppermute(x, 'sp', swaps[b])

    def local_block(x_special, x_patch, dy_special, dy_patch, ln_scale, ln_bias, w_qkv, b_qkv, w_proj, b_proj, layer_scale):
        shard = lax.axis_index('sp')
        chip, core = shard // 2, shard % 2
        row = lambda t: t.reshape(1, -1)

        def send(patch, i):
            mine = dyn(patch, 2 * core + i, 1, 0)[0]
            other = dyn(patch, 2 * (1 - core) + i, 1, 0)[0]
            return swap(other, 1), swap(mine, 2), swap(other, 3)

        qkv, d_attn, normed, xs, d_proj, dys = first(
            x_patch, dy_patch, x_special, dy_special,
            (w_qkv, row(b_qkv), row(ln_scale), row(ln_bias), w_proj, row(layer_scale)))
        d_attn, later_x, later_dy = lax.optimization_barrier((d_attn, x_patch, dy_patch))
        parts_x, parts_dy = send(later_x, 1), send(later_dy, 1)
        prev_a = attention(0, qkv, d_attn, ())
        qkv, *prev_x = front(1, front_x_kernel, 2304, x_patch, x_special, parts_x,
                             (w_qkv, row(b_qkv), row(ln_scale), row(ln_bias)), (normed, xs), 2 * T * 768 * 2304)
        d_attn, *prev_dy = front(1, front_dy_kernel, 768, dy_patch, dy_special, parts_dy,
                                 (w_proj, row(layer_scale)), (d_proj, dys), 2 * T * 768 * 768)
        prev_a = attention(1, qkv, d_attn, prev_a)
        normed, xs = prev_x
        d_proj, dys = prev_dy
        a, d_qkv = prev_a
        both, both_spec, vec = back(chip.reshape(1), xs, dys, a, d_qkv, w_qkv, w_proj, row(ln_scale), row(b_proj), row(layer_scale))
        t = vec + swap(vec, 1)
        t = t + swap(t, 2)
        got = swap(dyn(both, 1 - core, 1, 1)[:, 0], 1)
        keep = dyn(both, core, 1, 1)[:, 0]
        spec = both_spec[:, :, :2]
        gspec = swap(spec, 1)
        lo = core == 0

        def merge(p, q):
            return jnp.concatenate([jnp.where(lo, p, q), jnp.where(lo, q, p)], 0)

        def tn(p, q):
            return lax.dot_general(p.reshape(2 * T, 768), q.reshape(2 * T, 768), (((0,), (0,)), ((), ())), preferred_element_type=F32)

        gp = tn(a, d_proj)
        parts = [tn(normed, d_qkv[j]) for j in range(3)]
        pairs = [(p, swap(p, 1)) for p in parts]
        gq, gp = add_parts([pairs[0], pairs[1], (gp, swap(gp, 1))], 0, 2, ())
        gq, = add_parts([pairs[2]], 2, 1, (gq,))
        return (merge(spec[0], gspec[0]), merge(keep[0], got[0]), merge(spec[1], gspec[1]), merge(keep[1], got[1]),
                t[0], t[1], gq, t[4:7].reshape(-1), gp, t[2], t[3])

    rows, seq, rep = P('dp'), P('dp', 'sp'), P()
    return jax.shard_map(local_block, mesh=mesh,
                         in_specs=(rows, seq, rows, seq) + (rep,) * 7,
                         out_specs=(rows, seq, rows, seq) + (rows,) * 7, check_vma=False)
```

```python
import functools
import jax, jax.numpy as jnp
from jax import lax
from jax.sharding import PartitionSpec as P
from jax.experimental import pallas as pl
from jax.experimental.pallas import tpu as pltpu
F32=jnp.float32; BF=jnp.bfloat16
T=1040; NT=1026; QB=256
NEG=-1e30
def nt(a,b): return lax.dot_general(a,b,(((1,),(1,)),((),())),preferred_element_type=F32)
def nn(a,b): return jnp.dot(a,b,preferred_element_type=F32)
CH=[(0,256),(256,256),(512,256),(768,272)]
def fold(x,op):
    r=x.shape[0]//8
    x=x.reshape(r,8,x.shape[1])
    g=[x[i] for i in range(r)]
    while len(g)>1:
        g=[op(g[i],g[i+1]) for i in range(0,len(g)-1,2)]+([g[-1]] if len(g)%2 else [])
    return g[0]

def attn_kernel(num_alias,q_ref,k_ref,v_ref,do_ref,*refs):
    a_ref,dq_ref,dk_ref,dv_ref,qs,s_scr,p_scr,ds_scr,dor,qr,kT,vT,doT,dvk=refs[num_alias:]
    lane=lax.broadcasted_iota(jnp.int32,(1,128),1)
    kT[...]=k_ref[...].T; vT[...]=v_ref[...].T; doT[...]=do_ref[...].T
    qs[...]=(q_ref[...].astype(F32)*0.125).astype(BF)
    z=jnp.zeros((QB,128),BF)
    units=[(qb,h) for qb in range(4) for h in range(2)]
    U=len(units)
    st=[dict() for _ in units]
    for u,(qb,h) in enumerate(units):
        mh=(lane<64) if h==0 else (lane>=64)
        rows=slice(qb*QB,(qb+1)*QB)
        qr[u*QB:(u+1)*QB,:]=jnp.where(mh,qs[rows,:],z)
        dor[u*QB:(u+1)*QB,:]=jnp.where(mh,do_ref[rows,:],z)
    def A(u,c):
        r0,n=CH[c]; s_ref=s_scr.at[u%4]
        s=nt(k_ref[r0:r0+n,:],qr[u*QB:(u+1)*QB,:])
        if c==3:
            s=jnp.concatenate([s[:256],jnp.where(lax.broadcasted_iota(jnp.int32,(16,QB),0)<2,s[256:],NEG)],0)
        s_ref[r0:r0+n,:]=s
        f=fold(s,jnp.maximum)
        st[u]['m']=f if c==0 else jnp.maximum(st[u]['m'],f)
        if c==3: st[u]['m']=jnp.max(st[u]['m'],axis=0,keepdims=True)
    def B(u,c):
        r0,n=CH[c]; s_ref=s_scr.at[u%4]
        e=jnp.exp(s_ref[r0:r0+n,:]-st[u]['m'])
        s_ref[r0:r0+n,:]=e
        f=fold(e,jnp.add)
        st[u]['l']=f if c==0 else st[u]['l']+f
        if c==3: st[u]['rl']=1.0/jnp.sum(st[u]['l'],axis=0,keepdims=True)
    def C(u,c):
        qb,h=units[u]; r0,n=CH[c]; s_ref=s_scr.at[u%4]
        plo=(s_ref[r0:r0+n,:]*st[u]['rl']).astype(BF)
        p_scr[r0:r0+n,u*QB:(u+1)*QB]=plo
        o=nn(vT[64*h:64*h+64,r0:r0+n],plo)
        st[u]['o']=o if c==0 else st[u]['o']+o
        if c==3:
            st[u]['delta']=jnp.sum(st[u]['o']*doT[64*h:64*h+64,qb*QB:(qb+1)*QB].astype(F32),axis=0,keepdims=True)
            if h==1:
                a_ref[qb*QB:(qb+1)*QB,:]=jnp.concatenate([st[u-1]['o'],st[u]['o']],0).T.astype(BF)
    def D(u,c):
        qb,h=units[u]; r0,n=CH[c]; s_ref=s_scr.at[u%4]
        dp=nt(v_ref[r0:r0+n,:],dor[u*QB:(u+1)*QB,:]).astype(BF).astype(F32)
        ds=((s_ref[r0:r0+n,:]*st[u]['rl'])*(dp-st[u]['delta'])).astype(BF)
        ds_scr[r0:r0+n,u*QB:(u+1)*QB]=ds
        o=nn(kT[64*h:64*h+64,r0:r0+n],ds)
        st[u]['dq']=o if c==0 else st[u]['dq']+o
        if c==3 and h==1:
            dq_ref[qb*QB:(qb+1)*QB,:]=(jnp.concatenate([st[u-1]['dq'],st[u]['dq']],0)*0.125).T.astype(BF)
    def E(qb,c):
        r0,n=CH[c]
        cols=slice(qb*512,(qb+1)*512)
        for w,(src,rhs) in enumerate(((p_scr,dor),(ds_scr,qr))):
            x=nn(src[r0:r0+n,cols],rhs[cols,:])
            dvk[w,r0:r0+n,:]=dvk[w,r0:r0+n,:]+x
    q16=qs[1024:,:]; do16=do_ref[1024:,:]
    z16=jnp.zeros_like(q16)
    qm=jnp.concatenate([jnp.where(lane<64,q16,z16),jnp.where(lane>=64,q16,z16)],0)
    dom=jnp.concatenate([jnp.where(lane<64,do16,z16),jnp.where(lane>=64,do16,z16)],0)
    s=nt(k_ref[...],qm)
    rowi=lax.broadcasted_iota(jnp.int32,(T,32),0)
    s=jnp.where(rowi<NT,s,NEG)
    m=jnp.max(fold(s,jnp.maximum),axis=0,keepdims=True); e=jnp.exp(s-m); l=jnp.sum(fold(e,jnp.add),axis=0,keepdims=True)
    p=e*(1.0/l); plo=p.astype(BF)
    oT=nn(vT[...],plo)
    domT=dom.T
    dp=nt(v_ref[...],dom).astype(BF).astype(F32)
    delta=jnp.sum(oT*domT.astype(F32),axis=0,keepdims=True)
    ds=(p*(dp-delta)).astype(BF)
    dqT=nn(kT[...],ds)*0.125
    def pick(xT):
        x=xT.T
        return jnp.where(lane<64,x[:16],x[16:])
    a_ref[1024:,:]=pick(oT).astype(BF)
    dq_ref[1024:,:]=pick(dqT).astype(BF)
    dvk[0]=nn(plo,dom)
    dvk[1]=nn(ds,qm)
    for t in range(U+5):
        for c in range(4):
            if t<U: A(t,c)
            if 0<=t-1<U: B(t-1,c)
            if 0<=t-2<U: C(t-2,c)
            if 0<=t-3<U: D(t-3,c)
            e=t-5
            if e>=0 and e//2<4 and c%2==0:
                E(e//2,(e%2)*2+c//2)
    if True:
        dv_ref[...]=dvk[0].astype(BF)
        dk_ref[...]=dvk[1].astype(BF)


LN_EPS = 1e-6
ANY = pl.BlockSpec(memory_space=pl.ANY)
VM = pl.BlockSpec(memory_space=pltpu.VMEM)
VMEM_LIMIT = 63 * 1024 * 1024
TWO = jax.ShapeDtypeStruct((2, T, 768), BF)


def whole(shape):
    return pl.BlockSpec(shape, lambda *g: (0,) * len(shape))


def params(**kw):
    return pltpu.CompilerParams(vmem_limit_bytes=VMEM_LIMIT, **kw)


def layer_stats(xf):
    cen = xf - jnp.mean(xf, axis=-1, keepdims=True)
    inv = lax.rsqrt(jnp.mean(cen * cen, axis=-1, keepdims=True) + LN_EPS)
    return cen * inv, inv


def row(ref):
    return ref[...].reshape(1, -1)


def attention(i, qkv, do, prev):
    spec = lambda o: pl.BlockSpec((T, 128), lambda j, o=o: (0, o + j))
    n = len(prev)
    return pl.pallas_call(
        functools.partial(attn_kernel, n), grid=(6,),
        in_specs=[spec(0), spec(6), spec(12), spec(0)] + [ANY] * n,
        out_specs=[pl.BlockSpec((None, T, 128), lambda j: (i, 0, j))] * 4,
        out_shape=[TWO] * 4,
        input_output_aliases={4 + m: m for m in range(n)},
        scratch_shapes=[pltpu.VMEM((T, 128), BF), pltpu.VMEM((4, T, QB), F32), pltpu.VMEM((T, 2048), BF), pltpu.VMEM((T, 2048), BF),
                        pltpu.VMEM((2048, 128), BF), pltpu.VMEM((2048, 128), BF),
                        pltpu.VMEM((128, T), BF), pltpu.VMEM((128, T), BF), pltpu.VMEM((128, T), BF), pltpu.VMEM((2, T, 128), F32)],
        compiler_params=params(),
        cost_estimate=pl.CostEstimate(flops=48 * 12 * 1026 * 1026 * 64, bytes_accessed=12 * 1024 * 1024, transcendentals=12 * 1026 * 1026),
        name="attn")(qkv, qkv, qkv, do, *prev)


def front_kernel(i, num_in, *refs):
    ins = refs[:num_in]
    x_patch, dy_patch, x_special, dy_special, wq, bq, ls, lb, wp, lsc = ins[:10]
    if i == 0:
        outs, refs = refs[num_in:num_in + 8], refs[num_in + 8:]
    else:
        outs, refs = refs[num_in:num_in + 6], refs[num_in + 6:]
    qkv_o, do_o, normed_o, xs_o, dproj_o, dys_o = outs[:6]
    xbuf, dbuf, spec, qkv, do, normed, dproj, recv, loc, osem = refs[:10]
    me = lax.axis_index('sp')
    core = me & 1
    img = 2 * core + i
    rows = lambda b: pl.ds(pl.multiple_of((me ^ b) * 256, 256), 256)
    remote, arrive = [], {}
    if i == 0:
        send, stage, ssem = refs[10:]
        dp = lax.axis_index('dp')
        barrier = pltpu.get_barrier_semaphore()
        for b in (1, 2, 3):
            pl.semaphore_signal(barrier, inc=1, device_id=(dp, me ^ b), device_id_type=pl.DeviceIdType.MESH)
        pl.semaphore_wait(barrier, 3)
        for k, (patch, buf) in enumerate(((x_patch, xbuf), (dy_patch, dbuf))):
            for b in (1, 2, 3):
                c = pltpu.make_async_remote_copy(
                    src_ref=patch.at[2 * (core ^ (b & 1))], dst_ref=buf.at[rows(0)],
                    send_sem=send.at[3 * k + b - 1], recv_sem=recv.at[3 * k + b - 1],
                    device_id=(dp, me ^ b), device_id_type=pl.DeviceIdType.MESH)
                c.start()
                remote.append(c)
                arrive[k, b] = c.wait_recv
    else:
        parts = ins[10:13]
        for k, buf in enumerate((xbuf, dbuf)):
            for b in (1, 2, 3):
                c = pltpu.make_async_copy(parts[b - 1].at[k], buf.at[rows(b)], recv.at[3 * k + b - 1])
                c.start()
                arrive[k, b] = c.wait
    local = []
    for k, (patch, buf, special) in enumerate(((x_patch, xbuf, x_special), (dy_patch, dbuf, dy_special))):
        own = pltpu.make_async_copy(patch.at[img], buf.at[rows(0)], loc.at[2 * k])
        sp = pltpu.make_async_copy(special.at[img], spec.at[k], loc.at[2 * k + 1])
        own.start()
        sp.start()
        local.append((own, sp))
    later = []
    if i == 0:
        for k, patch in enumerate((x_patch, dy_patch)):
            for m, target in enumerate((img + 1, 2 * (1 - core) + 1)):
                c = pltpu.make_async_copy(patch.at[target], stage.at[m, k], ssem.at[2 * m + k])
                c.start()
                later.append((c, pltpu.make_async_copy(stage.at[m, k], outs[6 + m].at[k], ssem.at[4 + 2 * m + k])))
    emitted = []

    def emit(src, dst, r):
        c = pltpu.make_async_copy(src.at[r], dst.at[r], osem.at[len(emitted)])
        c.start()
        emitted.append(c)

    def do_x(r):
        x = xbuf[r, :]
        x_hat, _ = layer_stats(x.astype(F32))
        nb = (x_hat * row(ls) + row(lb)).astype(BF)
        normed[r, :] = nb
        for j in range(3):
            c = slice(768 * j, 768 * j + 768)
            qkv[r, c] = (nn(nb, wq[:, c]) + row(bq)[:, c]).astype(BF)
        emit(xbuf, xs_o.at[i], r)
        emit(normed, normed_o.at[i], r)
        emit(qkv, qkv_o, r)

    def do_dy(r):
        d = (dbuf[r, :].astype(F32) * row(lsc)).astype(BF)
        dproj[r, :] = d
        do[r, :] = nt(d, wp[...]).astype(BF)
        emit(dbuf, dys_o.at[i], r)
        emit(dproj, dproj_o.at[i], r)
        emit(do, do_o, r)

    for k, (buf, step) in enumerate(((xbuf, do_x), (dbuf, do_dy))):
        local[k][0].wait()
        local[k][1].wait()
        buf[1024:, :] = jnp.concatenate([spec[k], jnp.zeros((14, 768), BF)], 0)
        step(rows(0))
        step(pl.ds(1024, 16))
        arrive[k, 1]()
        step(rows(1))
    for c, out in later:
        c.wait()
        out.start()
    for k, step in enumerate((do_x, do_dy)):
        for b in (2, 3):
            arrive[k, b]()
            step(rows(b))
    for c in remote:
        c.wait_send()
    for _, out in later:
        out.wait()
    for c in emitted:
        c.wait()


def front(i, patches, consts, parts, prev):
    v = lambda s: pltpu.VMEM(s, BF)
    dma = lambda n: pltpu.SemaphoreType.DMA((n,))
    out_shape = [jax.ShapeDtypeStruct((T, 2304), BF), jax.ShapeDtypeStruct((T, 768), BF)] + [TWO] * 4
    scratch = [v((T, 768)), v((T, 768)), v((2, 2, 768)), v((T, 2304)), v((T, 768)), v((T, 768)), v((T, 768)), dma(6), dma(4), dma(30)]
    extra = {}
    if i == 0:
        out_shape += [jax.ShapeDtypeStruct((2, 256, 768), BF)] * 2
        scratch += [dma(6), v((2, 2, 256, 768)), dma(8)]
        extra = dict(collective_id=0, has_side_effects=True)
    first = 10 + len(parts)
    return pl.pallas_call(
        functools.partial(front_kernel, i, first + len(prev)),
        in_specs=[ANY] * 4 + [VM] * 6 + [ANY] * (len(parts) + len(prev)),
        out_specs=[ANY] * len(out_shape), out_shape=out_shape, scratch_shapes=scratch,
        input_output_aliases={first + m: 2 + m for m in range(len(prev))},
        compiler_params=params(**extra),
        cost_estimate=pl.CostEstimate(flops=2 * T * 768 * 3072, bytes_accessed=24 * 1024 * 1024, transcendentals=0),
        name="front")(*patches, *consts, *parts, *prev)


def back_kernel(place, *refs):
    ins, refs = refs[:12], refs[12:]
    w_ref, wp_ref, ls, bp, lsc, give, keep, os_ref, vec = refs
    g, i = pl.program_id(0), pl.program_id(1)

    def rows(x, dy, a, *dq):
        xf, dyf = x[...].astype(F32), dy[...].astype(F32)
        dq = [d[...] for d in dq]
        x_hat, inv = layer_stats(xf)
        proj = nn(a[...], wp_ref[...]) + row(bp)
        out = (xf + row(lsc) * proj).astype(BF)
        dn = sum(nt(dq[j], w_ref[:, 768 * j:768 * j + 768]) for j in range(3)).astype(BF).astype(F32)
        gh = dn * row(ls)
        dr = inv * (gh - jnp.mean(gh, -1, keepdims=True) - x_hat * jnp.mean(gh * x_hat, -1, keepdims=True))
        red = lambda t: jnp.sum(t, axis=0, keepdims=True)
        sums = [red(dn * x_hat), red(dn), red(dyf * row(lsc)), red(dyf * proj)] + [red(d.astype(F32)) for d in dq]
        return out, (dyf + dr).astype(BF), jnp.concatenate(sums + [jnp.zeros((1, 768), F32)], 0)

    out, dx, v = rows(*ins[:6])

    @pl.when(g == 0)
    def _():
        give[0] = out
        give[1] = dx

        @pl.when(i == 0)
        def _():
            vec[...] = jnp.zeros((8, 768), F32)
        so, sdx, sv = rows(*ins[6:])
        os_ref[0] = so
        os_ref[1] = sdx
        vec[...] += jnp.where(place[0] == 0, 1.0, 0.0) * sv

    @pl.when(g == 1)
    def _():
        keep[0] = out
        keep[1] = dx

    vec[...] += v


def back(place, xs, dys, a, dqs, w_qkv, w_proj, ln_scale, b_proj, layer_scale):
    arrays = (xs, dys, a) + tuple(dqs)
    blk = pl.BlockSpec((None, 256, 768), lambda g, i, c: (i, 2 * c[0] + (c[1] ^ (1 - g)), 0))
    sblk = pl.BlockSpec((None, 16, 768), lambda g, i, c: (i, 64, 0))
    half = jax.ShapeDtypeStruct((2, 2, 256, 768), BF)
    return pl.pallas_call(
        back_kernel,
        grid_spec=pltpu.PrefetchScalarGridSpec(
            num_scalar_prefetch=1, grid=(2, 2),
            in_specs=[blk] * 6 + [sblk] * 6 + [whole((768, 2304)), whole((768, 768))] + [VM] * 3,
            out_specs=[pl.BlockSpec((2, None, 256, 768), lambda g, i, c: (0, i + g * (1 - i), 0, 0)),
                       pl.BlockSpec((2, None, 256, 768), lambda g, i, c: (0, i * g, 0, 0)),
                       pl.BlockSpec((2, None, 16, 768), lambda g, i, c: (0, i + g * (1 - i), 0, 0)), whole((8, 768))]),
        out_shape=[half, half, jax.ShapeDtypeStruct((2, 2, 16, 768), BF), jax.ShapeDtypeStruct((8, 768), F32)],
        compiler_params=params(),
        cost_estimate=pl.CostEstimate(flops=2 * 1056 * 768 * 3072, bytes_accessed=20 * 1024 * 1024, transcendentals=0),
        name="back")(place, *arrays, *arrays, w_qkv, w_proj, ln_scale, b_proj, layer_scale)


def finish_kernel(place, keep, got, keep_s, got_s, *refs):
    ins, (gq, gp, out, dx, out_s, dx_s) = refs[:6], refs[6:]
    for m in range(2):
        gq[:, 768 * m:768 * m + 768] = ins[2 * m][...] + ins[2 * m + 1][...]
    gp[...] = ins[4][...] + ins[5][...]
    m = pl.program_id(0)
    own = (m >> 1) == place[1]

    @pl.when(own)
    def _():
        out[...] = keep[0]
        dx[...] = keep[1]
        out_s[...] = keep_s[0, :2, :]
        dx_s[...] = keep_s[1, :2, :]

    @pl.when(jnp.logical_not(own))
    def _():
        out[...] = got[0]
        dx[...] = got[1]
        out_s[...] = got_s[0, :2, :]
        dx_s[...] = got_s[1, :2, :]


def finish(place, keep, got, keep_s, got_s, pairs):
    flat = [t for p in pairs for t in p]
    blk = pl.BlockSpec((192, 768), lambda g, c: (g, 0))
    src = pl.BlockSpec((2, None, 256, 768), lambda g, c: (0, g & 1, 0, 0))
    src_s = pl.BlockSpec((2, None, 16, 768), lambda g, c: (0, g & 1, 0, 0))
    dst = pl.BlockSpec((None, 256, 768), lambda g, c: (g, 0, 0))
    dst_s = pl.BlockSpec((None, 2, 768), lambda g, c: (g, 0, 0))
    big, small = jax.ShapeDtypeStruct((4, 256, 768), BF), jax.ShapeDtypeStruct((4, 2, 768), BF)
    return pl.pallas_call(
        finish_kernel,
        grid_spec=pltpu.PrefetchScalarGridSpec(
            num_scalar_prefetch=1, grid=(4,),
            in_specs=[src, src, src_s, src_s] + [blk] * 6,
            out_specs=[pl.BlockSpec((192, 1536), lambda g, c: (g, 0)), blk, dst, dst, dst_s, dst_s]),
        out_shape=[jax.ShapeDtypeStruct((768, 2304), F32), jax.ShapeDtypeStruct((768, 768), F32), big, big, small, small],
        compiler_params=params(),
        cost_estimate=pl.CostEstimate(flops=3 * 768 * 768, bytes_accessed=36 * 768 * 768, transcendentals=0),
        name="finish")(place, keep, got, keep_s, got_s, *flat)


def last_add_kernel(p, q, _, out):
    out[...] = p[...] + q[...]


def last_add(pair, gq):
    blk = pl.BlockSpec((192, 768), lambda g: (g, 0))
    return pl.pallas_call(
        last_add_kernel, grid=(4,), in_specs=[blk, blk, ANY],
        out_specs=pl.BlockSpec((192, 768), lambda g: (g, 2)),
        out_shape=jax.ShapeDtypeStruct((768, 2304), F32), input_output_aliases={2: 0},
        compiler_params=params(),
        cost_estimate=pl.CostEstimate(flops=768 * 768, bytes_accessed=12 * 768 * 768, transcendentals=0),
        name="last_add")(*pair, gq)


def solution(mesh):
    n = mesh.shape['sp']
    swaps = {b: [(s, s ^ b) for s in range(n)] for b in (1, 2, 3)}

    def swap(x, b):
        return lax.ppermute(x, 'sp', swaps[b])

    def local_block(x_special, x_patch, dy_special, dy_patch, ln_scale, ln_bias, w_qkv, b_qkv, w_proj, b_proj, layer_scale):
        shard = lax.axis_index('sp')
        place = jnp.stack([shard >> 1, shard & 1])
        patches = (x_patch, dy_patch, x_special, dy_special)
        consts = (w_qkv, b_qkv, ln_scale, ln_bias, w_proj, layer_scale)
        qkv, d_attn, *saved, mine, other = front(0, patches, consts, (), ())
        parts = (swap(other, 1), swap(mine, 2), swap(other, 3))
        prev = attention(0, qkv, d_attn, ())
        qkv, d_attn, *saved = front(1, patches, consts, parts, saved)
        a, *dqs = attention(1, qkv, d_attn, prev)
        normed, xs, d_proj, dys = saved
        give, keep, keep_s, vec = back(place, xs, dys, a, dqs, w_qkv, w_proj, ln_scale, b_proj, layer_scale)
        got, got_s = swap(give, 1), swap(keep_s, 1)
        t = vec + swap(vec, 1)
        t = t + swap(t, 2)
        vec, normed, a = lax.optimization_barrier((vec, normed, a))

        def tn(p, q):
            return lax.dot_general(p.reshape(2 * T, 768), q.reshape(2 * T, 768), (((0,), (0,)), ((), ())), preferred_element_type=F32)

        parts = [tn(normed, dqs[0]), tn(normed, dqs[1]), tn(a, d_proj), tn(normed, dqs[2])]
        pairs = [(p, swap(p, 1)) for p in parts]
        gq, gp, out, dx, out_s, dx_s = finish(place, keep, got, keep_s, got_s, pairs[:3])
        gq = last_add(pairs[3], gq)
        return out_s, out, dx_s, dx, t[0], t[1], gq, t[4:7].reshape(-1), gp, t[2], t[3]

    rows, seq, rep = P('dp'), P('dp', 'sp'), P()
    return jax.shard_map(local_block, mesh=mesh,
                         in_specs=(rows, seq, rows, seq) + (rep,) * 7,
                         out_specs=(rows, seq, rows, seq) + (rows,) * 7, check_vma=False)
```

```python
import functools
import jax, jax.numpy as jnp
from jax import lax
from jax.sharding import PartitionSpec as P
from jax.experimental import pallas as pl
from jax.experimental.pallas import tpu as pltpu
F32=jnp.float32; BF=jnp.bfloat16
T=1040; NT=1026; QB=256
NEG=-1e30
SUB=64
def nt(a,b): return lax.dot_general(a,b,(((1,),(1,)),((),())),preferred_element_type=F32)
def nn(a,b): return jnp.dot(a,b,preferred_element_type=F32)
CH=[(0,256),(256,256),(512,256),(768,272)]
def fold(x,op):
    r=x.shape[0]//8
    x=x.reshape(r,8,x.shape[1])
    g=[x[i] for i in range(r)]
    while len(g)>1:
        g=[op(g[i],g[i+1]) for i in range(0,len(g)-1,2)]+([g[-1]] if len(g)%2 else [])
    return g[0]

def attn_kernel(num_alias,q_ref,k_ref,v_ref,do_ref,*refs):
    a_ref,dq_ref,dk_ref,dv_ref,qs,s_scr,p_scr,ds_scr,dor,qr,kT,vT,doT,dvk,ms,lsum,fs,ss,sps,sds=refs[num_alias:]
    lane=lax.broadcasted_iota(jnp.int32,(1,128),1)
    qs[...]=(q_ref[...].astype(F32)*0.125).astype(BF)
    z=jnp.zeros((QB,128),BF)
    units=[(qb,h) for qb in range(4) for h in range(2)]
    U=len(units)
    st=[dict() for _ in units]
    def mask_q(u):
        qb,h=units[u]; mh=(lane<64) if h==0 else (lane>=64)
        qr[u*QB:(u+1)*QB,:]=jnp.where(mh,qs[qb*QB:(qb+1)*QB,:],z)
    def mask_do(u):
        qb,h=units[u]; mh=(lane<64) if h==0 else (lane>=64)
        dor[u*QB:(u+1)*QB,:]=jnp.where(mh,do_ref[qb*QB:(qb+1)*QB,:],z)
    nsub=1024//SUB+1
    def subs(c):
        r0,n=CH[c]
        out=[(r0+i,SUB,(r0+i)//SUB) for i in range(0,256,SUB)]
        if c==3: out.append((1024,16,nsub-1))
        return out
    ms[...]=jnp.full(ms.shape,NEG,F32)
    lsum[...]=jnp.zeros(lsum.shape,F32)
    def A(u,c):
        r0,n=CH[c]; s_ref=s_scr.at[u%4]
        if c==0: mask_q(u)
        s=nt(k_ref[r0:r0+n,:],qr[u*QB:(u+1)*QB,:])
        for r,k,i in subs(c):
            x=s[r-r0:r-r0+k]
            if r==1024:
                x=jnp.where(lax.broadcasted_iota(jnp.int32,(16,QB),0)<2,x,NEG)
            m=jnp.max(fold(x,jnp.maximum),axis=0,keepdims=True)
            e=jnp.exp(x-m)
            s_ref[r:r+k,:]=e
            ms[u%4,i:i+1,:]=m
            lsum[u%4,i:i+1,:]=jnp.sum(fold(e,jnp.add),axis=0,keepdims=True)
        if c==3:
            mm=ms[u%4]
            f=jnp.exp(mm-jnp.max(mm,axis=0,keepdims=True))
            fs[u%4]=f*(1.0/jnp.sum(lsum[u%4]*f,axis=0,keepdims=True))
    def C(u,c):
        qb,h=units[u]; r0,n=CH[c]; s_ref=s_scr.at[u%4]
        ps=[]
        for r,k,i in subs(c):
            p=s_ref[r:r+k,:]*fs[u%4,i:i+1,:]
            ps.append(p.astype(BF))
            s_ref[r:r+k,:]=p
            p_scr[r:r+k,u*QB:(u+1)*QB]=ps[-1]
        o=nn(vT[64*h:64*h+64,r0:r0+n],jnp.concatenate(ps,0))
        st[u]['o']=o if c==0 else st[u]['o']+o
        if c==3:
            st[u]['delta']=jnp.sum(st[u]['o']*doT[64*h:64*h+64,qb*QB:(qb+1)*QB].astype(F32),axis=0,keepdims=True)
            if h==1:
                a_ref[qb*QB:(qb+1)*QB,:]=jnp.concatenate([st[u-1]['o'],st[u]['o']],0).T.astype(BF)
    def D(u,c):
        qb,h=units[u]; r0,n=CH[c]; s_ref=s_scr.at[u%4]
        if c==0: mask_do(u)
        dp=nt(v_ref[r0:r0+n,:],dor[u*QB:(u+1)*QB,:])
        ps=[]
        for r,k,i in subs(c):
            x=dp[r-r0:r-r0+k].astype(BF).astype(F32)
            p=s_ref[r:r+k,:]
            ps.append((p*(x-st[u]['delta'])).astype(BF))
            ds_scr[r:r+k,u*QB:(u+1)*QB]=ps[-1]
        o=nn(kT[64*h:64*h+64,r0:r0+n],jnp.concatenate(ps,0))
        st[u]['dq']=o if c==0 else st[u]['dq']+o
        if c==3 and h==1:
            dq_ref[qb*QB:(qb+1)*QB,:]=(jnp.concatenate([st[u-1]['dq'],st[u]['dq']],0)*0.125).T.astype(BF)
    def E(qb,c):
        r0,n=CH[c]
        cols=slice(qb*512,(qb+1)*512)
        for w,(src,rhs) in enumerate(((p_scr,dor),(ds_scr,qr))):
            x=nn(src[r0:r0+n,cols],rhs[cols,:])
            dvk[w,r0:r0+n,:]=dvk[w,r0:r0+n,:]+x
    sp={}
    z16=jnp.zeros((16,128),BF)
    def pair_rows(x):
        return jnp.concatenate([jnp.where(lane<64,x,z16),jnp.where(lane>=64,x,z16)],0)
    def pick(xT):
        x=xT.T
        return jnp.where(lane<64,x[:16],x[16:])
    def SA():
        sp['qm']=pair_rows(qs[1024:,:])
        s=nt(k_ref[...],sp['qm'])
        s=jnp.where(lax.broadcasted_iota(jnp.int32,(T,32),0)<NT,s,NEG)
        m=jnp.max(fold(s,jnp.maximum),axis=0,keepdims=True); e=jnp.exp(s-m)
        sp['rl']=1.0/jnp.sum(fold(e,jnp.add),axis=0,keepdims=True)
        ss[...]=e
    def SB():
        sp['dom']=pair_rows(do_ref[1024:,:])
        sps[...]=(ss[...]*sp['rl']).astype(BF)
        oT=nn(vT[...],sps[...])
        sp['delta']=jnp.sum(oT*sp['dom'].T.astype(F32),axis=0,keepdims=True)
        a_ref[1024:,:]=pick(oT).astype(BF)
    def SC():
        dp=nt(v_ref[...],sp['dom']).astype(BF).astype(F32)
        sds[...]=((ss[...]*sp['rl'])*(dp-sp['delta'])).astype(BF)
        dq_ref[1024:,:]=pick(nn(kT[...],sds[...])*0.125).astype(BF)
    def SE():
        dvk[0]=nn(sps[...],sp['dom'])
        dvk[1]=nn(sds[...],sp['qm'])
    extra={(0,0):lambda:vT.__setitem__(Ellipsis,v_ref[...].T),(0,1):lambda:doT.__setitem__(Ellipsis,do_ref[...].T),
           (0,2):SA,(1,1):lambda:kT.__setitem__(Ellipsis,k_ref[...].T),(1,2):SB,(2,1):SC,(3,1):SE}
    for t in range(U+4):
        for c in range(4):
            if t<U: A(t,c)
            if 0<=t-1<U: C(t-1,c)
            if 0<=t-2<U: D(t-2,c)
            e=t-4
            if e>=0 and e//2<4 and c%2==0:
                E(e//2,(e%2)*2+c//2)
            if (t,c) in extra: extra[t,c]()
    if True:
        dv_ref[...]=dvk[0].astype(BF)
        dk_ref[...]=dvk[1].astype(BF)


LN_EPS = 1e-6
ANY = pl.BlockSpec(memory_space=pl.ANY)
VM = pl.BlockSpec(memory_space=pltpu.VMEM)
VMEM_LIMIT = 63 * 1024 * 1024
TWO = jax.ShapeDtypeStruct((2, T, 768), BF)


def whole(shape):
    return pl.BlockSpec(shape, lambda *g: (0,) * len(shape))


def params(**kw):
    return pltpu.CompilerParams(vmem_limit_bytes=VMEM_LIMIT, **kw)


def layer_stats(xf):
    cen = xf - jnp.mean(xf, axis=-1, keepdims=True)
    inv = lax.rsqrt(jnp.mean(cen * cen, axis=-1, keepdims=True) + LN_EPS)
    return cen * inv, inv


def row(ref):
    return ref[...].reshape(1, -1)


def attention(i, qkv, do, prev):
    spec = lambda o: pl.BlockSpec((T, 128), lambda j, o=o: (0, o + j))
    n = len(prev)
    return pl.pallas_call(
        functools.partial(attn_kernel, n), grid=(6,),
        in_specs=[spec(0), spec(6), spec(12), spec(0)] + [ANY] * n,
        out_specs=[pl.BlockSpec((None, T, 128), lambda j: (i, 0, j))] * 4,
        out_shape=[TWO] * 4,
        input_output_aliases={4 + m: m for m in range(n)},
        scratch_shapes=[pltpu.VMEM((T, 128), BF), pltpu.VMEM((4, T, QB), F32), pltpu.VMEM((T, 2048), BF), pltpu.VMEM((T, 2048), BF),
                        pltpu.VMEM((2048, 128), BF), pltpu.VMEM((2048, 128), BF),
                        pltpu.VMEM((128, T), BF), pltpu.VMEM((128, T), BF), pltpu.VMEM((128, T), BF), pltpu.VMEM((2, T, 128), F32)]
        + [pltpu.VMEM((4, 24, QB), F32)] * 3 + [pltpu.VMEM((T, 32), F32)] + [pltpu.VMEM((T, 32), BF)] * 2,
        compiler_params=params(),
        cost_estimate=pl.CostEstimate(flops=48 * 12 * 1026 * 1026 * 64, bytes_accessed=12 * 1024 * 1024, transcendentals=12 * 1026 * 1026),
        name="attn")(qkv, qkv, qkv, do, *prev)


def front_kernel(i, num_in, *refs):
    ins = refs[:num_in]
    x_patch, dy_patch, x_special, dy_special, wq, bq, ls, lb, wp, lsc = ins[:10]
    if i == 0:
        outs, refs = refs[num_in:num_in + 8], refs[num_in + 8:]
    else:
        outs, refs = refs[num_in:num_in + 6], refs[num_in + 6:]
    qkv_o, do_o, normed_o, xs_o, dproj_o, dys_o = outs[:6]
    xbuf, dbuf, spec, qkv, do, normed, dproj, recv, loc, osem = refs[:10]
    me = lax.axis_index('sp')
    core = me & 1
    img = 2 * core + i
    rows = lambda b: pl.ds(pl.multiple_of((me ^ b) * 256, 256), 256)
    remote, arrive = [], {}
    if i == 0:
        send, stage, ssem = refs[10:]
        dp = lax.axis_index('dp')
        barrier = pltpu.get_barrier_semaphore()
        for b in (1, 2, 3):
            pl.semaphore_signal(barrier, inc=1, device_id=(dp, me ^ b), device_id_type=pl.DeviceIdType.MESH)
        pl.semaphore_wait(barrier, 3)
        for k, (patch, buf) in enumerate(((x_patch, xbuf), (dy_patch, dbuf))):
            for b in (1, 2, 3):
                c = pltpu.make_async_remote_copy(
                    src_ref=patch.at[2 * (core ^ (b & 1))], dst_ref=buf.at[rows(0)],
                    send_sem=send.at[3 * k + b - 1], recv_sem=recv.at[3 * k + b - 1],
                    device_id=(dp, me ^ b), device_id_type=pl.DeviceIdType.MESH)
                c.start()
                remote.append(c)
                arrive[k, b] = c.wait_recv
    else:
        parts = ins[10:13]
        for k, buf in enumerate((xbuf, dbuf)):
            for b in (1, 2, 3):
                c = pltpu.make_async_copy(parts[b - 1].at[k], buf.at[rows(b)], recv.at[3 * k + b - 1])
                c.start()
                arrive[k, b] = c.wait
    local = []
    for k, (patch, buf, special) in enumerate(((x_patch, xbuf, x_special), (dy_patch, dbuf, dy_special))):
        own = pltpu.make_async_copy(patch.at[img], buf.at[rows(0)], loc.at[2 * k])
        sp = pltpu.make_async_copy(special.at[img], spec.at[k], loc.at[2 * k + 1])
        own.start()
        sp.start()
        local.append((own, sp))
    later = []
    if i == 0:
        for k, patch in enumerate((x_patch, dy_patch)):
            for m, target in enumerate((img + 1, 2 * (1 - core) + 1)):
                c = pltpu.make_async_copy(patch.at[target], stage.at[m, k], ssem.at[2 * m + k])
                c.start()
                later.append((c, pltpu.make_async_copy(stage.at[m, k], outs[6 + m].at[k], ssem.at[4 + 2 * m + k])))
    emitted = []

    def emit(src, dst, r):
        c = pltpu.make_async_copy(src.at[r], dst.at[r], osem.at[len(emitted)])
        c.start()
        emitted.append(c)

    def do_x(r):
        x = xbuf[r, :]
        x_hat, _ = layer_stats(x.astype(F32))
        nb = (x_hat * row(ls) + row(lb)).astype(BF)
        normed[r, :] = nb
        for j in range(3):
            c = slice(768 * j, 768 * j + 768)
            qkv[r, c] = (nn(nb, wq[:, c]) + row(bq)[:, c]).astype(BF)
        emit(xbuf, xs_o.at[i], r)
        emit(normed, normed_o.at[i], r)
        emit(qkv, qkv_o, r)

    def do_dy(r):
        d = (dbuf[r, :].astype(F32) * row(lsc)).astype(BF)
        dproj[r, :] = d
        do[r, :] = nt(d, wp[...]).astype(BF)
        emit(dbuf, dys_o.at[i], r)
        emit(dproj, dproj_o.at[i], r)
        emit(do, do_o, r)

    for k, (buf, step) in enumerate(((xbuf, do_x), (dbuf, do_dy))):
        local[k][0].wait()
        local[k][1].wait()
        buf[1024:, :] = jnp.concatenate([spec[k], jnp.zeros((14, 768), BF)], 0)
        step(rows(0))
        step(pl.ds(1024, 16))
        arrive[k, 1]()
        step(rows(1))
    for c, out in later:
        c.wait()
        out.start()
    for k, step in enumerate((do_x, do_dy)):
        for b in (2, 3):
            arrive[k, b]()
            step(rows(b))
    for c in remote:
        c.wait_send()
    for _, out in later:
        out.wait()
    for c in emitted:
        c.wait()


def front(i, patches, consts, parts, prev):
    v = lambda s: pltpu.VMEM(s, BF)
    dma = lambda n: pltpu.SemaphoreType.DMA((n,))
    out_shape = [jax.ShapeDtypeStruct((T, 2304), BF), jax.ShapeDtypeStruct((T, 768), BF)] + [TWO] * 4
    scratch = [v((T, 768)), v((T, 768)), v((2, 2, 768)), v((T, 2304)), v((T, 768)), v((T, 768)), v((T, 768)), dma(6), dma(4), dma(30)]
    extra = {}
    if i == 0:
        out_shape += [jax.ShapeDtypeStruct((2, 256, 768), BF)] * 2
        scratch += [dma(6), v((2, 2, 256, 768)), dma(8)]
        extra = dict(collective_id=0, has_side_effects=True)
    first = 10 + len(parts)
    return pl.pallas_call(
        functools.partial(front_kernel, i, first + len(prev)),
        in_specs=[ANY] * 4 + [VM] * 6 + [ANY] * (len(parts) + len(prev)),
        out_specs=[ANY] * len(out_shape), out_shape=out_shape, scratch_shapes=scratch,
        input_output_aliases={first + m: 2 + m for m in range(len(prev))},
        compiler_params=params(**extra),
        cost_estimate=pl.CostEstimate(flops=2 * T * 768 * 3072, bytes_accessed=24 * 1024 * 1024, transcendentals=0),
        name="front")(*patches, *consts, *parts, *prev)


def back_kernel(place, *refs):
    ins, refs = refs[:12], refs[12:]
    w_ref, wp_ref, ls, bp, lsc, give, keep, os_ref, vec, proj_s, dn_s = refs
    i = pl.program_id(0)
    a = jnp.concatenate([ins[2][...], ins[8][...]], 0)
    proj_s[...] = nn(a, wp_ref[...])
    dn_s[...] = sum(nt(jnp.concatenate([ins[3 + j][...], ins[9 + j][...]], 0), w_ref[:, 768 * j:768 * j + 768]) for j in range(3))

    @pl.when(i == 0)
    def _():
        vec[...] = jnp.zeros((8, 768), F32)

    total = vec[...]
    for s, (r0, n) in enumerate(((0, 256), (256, 256), (512, 16))):
        r = slice(r0, r0 + n)
        get = (lambda m: ins[m][r, :]) if s < 2 else (lambda m: ins[6 + m][...])
        xf, dyf = get(0).astype(F32), get(1).astype(F32)
        x_hat, inv = layer_stats(xf)
        proj = proj_s[r, :] + row(bp)
        out = (xf + row(lsc) * proj).astype(BF)
        dn = dn_s[r, :].astype(BF).astype(F32)
        gh = dn * row(ls)
        dr = inv * (gh - jnp.mean(gh, -1, keepdims=True) - x_hat * jnp.mean(gh * x_hat, -1, keepdims=True))
        dx = (dyf + dr).astype(BF)
        red = lambda t: jnp.sum(t, axis=0, keepdims=True)
        sums = [red(dn * x_hat), red(dn), red(dyf * row(lsc)), red(dyf * proj)] + [red(get(3 + j).astype(F32)) for j in range(3)]
        v = jnp.concatenate(sums + [jnp.zeros((1, 768), F32)], 0)
        if s < 2:
            total = total + v

            @pl.when(place[1] == s)
            def _():
                keep[0] = out
                keep[1] = dx

            @pl.when(place[1] != s)
            def _():
                give[0] = out
                give[1] = dx
        else:
            total = total + jnp.where(place[0] == 0, 1.0, 0.0) * v
            os_ref[0] = out
            os_ref[1] = dx
    vec[...] = total


def back(place, xs, dys, a, dqs, w_qkv, w_proj, ln_scale, b_proj, layer_scale):
    arrays = (xs, dys, a) + tuple(dqs)
    blk = pl.BlockSpec((None, 512, 768), lambda i, c: (i, c[0], 0))
    sblk = pl.BlockSpec((None, 16, 768), lambda i, c: (i, 64, 0))
    out = pl.BlockSpec((2, None, 256, 768), lambda i, c: (0, i, 0, 0))
    half = jax.ShapeDtypeStruct((2, 2, 256, 768), BF)
    return pl.pallas_call(
        back_kernel,
        grid_spec=pltpu.PrefetchScalarGridSpec(
            num_scalar_prefetch=1, grid=(2,),
            in_specs=[blk] * 6 + [sblk] * 6 + [whole((768, 2304)), whole((768, 768))] + [VM] * 3,
            out_specs=[out, out, pl.BlockSpec((2, None, 16, 768), lambda i, c: (0, i, 0, 0)), whole((8, 768))],
            scratch_shapes=[pltpu.VMEM((528, 768), F32)] * 2),
        out_shape=[half, half, jax.ShapeDtypeStruct((2, 2, 16, 768), BF), jax.ShapeDtypeStruct((8, 768), F32)],
        compiler_params=params(),
        cost_estimate=pl.CostEstimate(flops=2 * 1056 * 768 * 3072, bytes_accessed=20 * 1024 * 1024, transcendentals=0),
        name="back")(place, *arrays, *arrays, w_qkv, w_proj, ln_scale, b_proj, layer_scale)


def finish_kernel(place, keep, got, keep_s, got_s, *refs):
    ins, (gq, gp, out, dx, out_s, dx_s) = refs[:6], refs[6:]
    for m in range(2):
        gq[:, 768 * m:768 * m + 768] = ins[2 * m][...] + ins[2 * m + 1][...]
    gp[...] = ins[4][...] + ins[5][...]
    m = pl.program_id(0)
    own = (m >> 1) == place[1]

    @pl.when(own)
    def _():
        out[...] = keep[0]
        dx[...] = keep[1]
        out_s[...] = keep_s[0, :2, :]
        dx_s[...] = keep_s[1, :2, :]

    @pl.when(jnp.logical_not(own))
    def _():
        out[...] = got[0]
        dx[...] = got[1]
        out_s[...] = got_s[0, :2, :]
        dx_s[...] = got_s[1, :2, :]


def finish(place, keep, got, keep_s, got_s, pairs):
    flat = [t for p in pairs for t in p]
    blk = pl.BlockSpec((192, 768), lambda g, c: (g, 0))
    src = pl.BlockSpec((2, None, 256, 768), lambda g, c: (0, g & 1, 0, 0))
    src_s = pl.BlockSpec((2, None, 16, 768), lambda g, c: (0, g & 1, 0, 0))
    dst = pl.BlockSpec((None, 256, 768), lambda g, c: (g, 0, 0))
    dst_s = pl.BlockSpec((None, 2, 768), lambda g, c: (g, 0, 0))
    big, small = jax.ShapeDtypeStruct((4, 256, 768), BF), jax.ShapeDtypeStruct((4, 2, 768), BF)
    return pl.pallas_call(
        finish_kernel,
        grid_spec=pltpu.PrefetchScalarGridSpec(
            num_scalar_prefetch=1, grid=(4,),
            in_specs=[src, src, src_s, src_s] + [blk] * 6,
            out_specs=[pl.BlockSpec((192, 1536), lambda g, c: (g, 0)), blk, dst, dst, dst_s, dst_s]),
        out_shape=[jax.ShapeDtypeStruct((768, 2304), F32), jax.ShapeDtypeStruct((768, 768), F32), big, big, small, small],
        compiler_params=params(),
        cost_estimate=pl.CostEstimate(flops=3 * 768 * 768, bytes_accessed=36 * 768 * 768, transcendentals=0),
        name="finish")(place, keep, got, keep_s, got_s, *flat)


def last_add_kernel(p, q, _, out):
    out[...] = p[...] + q[...]


def last_add(pair, gq):
    blk = pl.BlockSpec((192, 768), lambda g: (g, 0))
    return pl.pallas_call(
        last_add_kernel, grid=(4,), in_specs=[blk, blk, ANY],
        out_specs=pl.BlockSpec((192, 768), lambda g: (g, 2)),
        out_shape=jax.ShapeDtypeStruct((768, 2304), F32), input_output_aliases={2: 0},
        compiler_params=params(),
        cost_estimate=pl.CostEstimate(flops=768 * 768, bytes_accessed=12 * 768 * 768, transcendentals=0),
        name="last_add")(*pair, gq)


def solution(mesh):
    n = mesh.shape['sp']
    swaps = {b: [(s, s ^ b) for s in range(n)] for b in (1, 2, 3)}

    def swap(x, b):
        return lax.ppermute(x, 'sp', swaps[b])

    def local_block(x_special, x_patch, dy_special, dy_patch, ln_scale, ln_bias, w_qkv, b_qkv, w_proj, b_proj, layer_scale):
        shard = lax.axis_index('sp')
        place = jnp.stack([shard >> 1, shard & 1])
        patches = (x_patch, dy_patch, x_special, dy_special)
        consts = (w_qkv, b_qkv, ln_scale, ln_bias, w_proj, layer_scale)
        qkv, d_attn, *saved, mine, other = front(0, patches, consts, (), ())
        parts = (swap(other, 1), swap(mine, 2), swap(other, 3))
        prev = attention(0, qkv, d_attn, ())
        qkv, d_attn, *saved = front(1, patches, consts, parts, saved)
        a, *dqs = attention(1, qkv, d_attn, prev)
        normed, xs, d_proj, dys = saved
        give, keep, keep_s, vec = back(place, xs, dys, a, dqs, w_qkv, w_proj, ln_scale, b_proj, layer_scale)
        got, got_s = swap(give, 1), swap(keep_s, 1)
        around = [swap(vec, b) for b in (1, 2, 3)]
        vec, normed = lax.optimization_barrier((vec, normed))

        def tn(p, q):
            return lax.dot_general(p.reshape(2 * T, 768), q.reshape(2 * T, 768), (((0,), (0,)), ((), ())), preferred_element_type=F32)

        parts = [tn(normed, dqs[0]), tn(normed, dqs[1])]
        around, normed, a = lax.optimization_barrier((around, normed, a))
        parts += [tn(a, d_proj), tn(normed, dqs[2])]
        t = (vec + around[0]) + (around[1] + around[2])
        pairs = [(p, swap(p, 1)) for p in parts]
        gq, gp, out, dx, out_s, dx_s = finish(place, keep, got, keep_s, got_s, pairs[:3])
        gq = last_add(pairs[3], gq)
        return out_s, out, dx_s, dx, t[0], t[1], gq, t[4:7].reshape(-1), gp, t[2], t[3]

    rows, seq, rep = P('dp'), P('dp', 'sp'), P()
    return jax.shard_map(local_block, mesh=mesh,
                         in_specs=(rows, seq, rows, seq) + (rep,) * 7,
                         out_specs=(rows, seq, rows, seq) + (rows,) * 7, check_vma=False)
```

```python
import functools
import jax, jax.numpy as jnp
from jax import lax
from jax.sharding import PartitionSpec as P
from jax.experimental import pallas as pl
from jax.experimental.pallas import tpu as pltpu
F32=jnp.float32; BF=jnp.bfloat16
T=1040; NT=1026; QB=256
NEG=-1e30
SUB=64
def nt(a,b): return lax.dot_general(a,b,(((1,),(1,)),((),())),preferred_element_type=F32)
def nn(a,b): return jnp.dot(a,b,preferred_element_type=F32)
CH=[(0,256),(256,256),(512,256),(768,272)]
def fold(x,op):
    r=x.shape[0]//8
    x=x.reshape(r,8,x.shape[1])
    g=[x[i] for i in range(r)]
    while len(g)>1:
        g=[op(g[i],g[i+1]) for i in range(0,len(g)-1,2)]+([g[-1]] if len(g)%2 else [])
    return g[0]

def attn_kernel(num_alias,q_ref,k_ref,v_ref,do_ref,*refs):
    a_ref,dq_ref,dk_ref,dv_ref,qs,s_scr,p_scr,ds_scr,dor,qr,kT,vT,doT,dvk,ms,lsum,fs,ss,sps,sds=refs[num_alias:]
    lane=lax.broadcasted_iota(jnp.int32,(1,128),1)
    qs[...]=(q_ref[...].astype(F32)*0.125).astype(BF)
    z=jnp.zeros((QB,128),BF)
    units=[(qb,h) for qb in range(4) for h in range(2)]
    U=len(units)
    st=[dict() for _ in units]
    def mask_q(u):
        qb,h=units[u]; mh=(lane<64) if h==0 else (lane>=64)
        qr[u*QB:(u+1)*QB,:]=jnp.where(mh,qs[qb*QB:(qb+1)*QB,:],z)
    def mask_do(u):
        qb,h=units[u]; mh=(lane<64) if h==0 else (lane>=64)
        dor[u*QB:(u+1)*QB,:]=jnp.where(mh,do_ref[qb*QB:(qb+1)*QB,:],z)
    nsub=1024//SUB+1
    def subs(c):
        r0,n=CH[c]
        out=[(r0+i,SUB,(r0+i)//SUB) for i in range(0,256,SUB)]
        if c==3: out.append((1024,16,nsub-1))
        return out
    ms[...]=jnp.full(ms.shape,NEG,F32)
    lsum[...]=jnp.zeros(lsum.shape,F32)
    def A(u,c):
        r0,n=CH[c]; s_ref=s_scr.at[u%4]
        if c==0: mask_q(u)
        s=nt(k_ref[r0:r0+n,:],qr[u*QB:(u+1)*QB,:])
        for r,k,i in subs(c):
            x=s[r-r0:r-r0+k]
            if r==1024:
                x=jnp.where(lax.broadcasted_iota(jnp.int32,(16,QB),0)<2,x,NEG)
            m=jnp.max(fold(x,jnp.maximum),axis=0,keepdims=True)
            e=jnp.exp(x-m)
            s_ref[r:r+k,:]=e
            ms[u%4,i:i+1,:]=m
            lsum[u%4,i:i+1,:]=jnp.sum(fold(e,jnp.add),axis=0,keepdims=True)
        if c==3:
            mm=ms[u%4]
            f=jnp.exp(mm-jnp.max(mm,axis=0,keepdims=True))
            fs[u%4]=f*(1.0/jnp.sum(lsum[u%4]*f,axis=0,keepdims=True))
    def C(u,c):
        qb,h=units[u]; r0,n=CH[c]; s_ref=s_scr.at[u%4]
        ps=[]
        for r,k,i in subs(c):
            p=s_ref[r:r+k,:]*fs[u%4,i:i+1,:]
            ps.append(p.astype(BF))
            s_ref[r:r+k,:]=p
            p_scr[r:r+k,u*QB:(u+1)*QB]=ps[-1]
        o=nn(vT[64*h:64*h+64,r0:r0+n],jnp.concatenate(ps,0))
        st[u]['o']=o if c==0 else st[u]['o']+o
        if c==3:
            st[u]['delta']=jnp.sum(st[u]['o']*doT[64*h:64*h+64,qb*QB:(qb+1)*QB].astype(F32),axis=0,keepdims=True)
            if h==1:
                a_ref[qb*QB:(qb+1)*QB,:]=jnp.concatenate([st[u-1]['o'],st[u]['o']],0).T.astype(BF)
    def D(u,c):
        qb,h=units[u]; r0,n=CH[c]; s_ref=s_scr.at[u%4]
        if c==0: mask_do(u)
        dp=nt(v_ref[r0:r0+n,:],dor[u*QB:(u+1)*QB,:])
        ps=[]
        for r,k,i in subs(c):
            x=dp[r-r0:r-r0+k].astype(BF).astype(F32)
            p=s_ref[r:r+k,:]
            ps.append((p*(x-st[u]['delta'])).astype(BF))
            ds_scr[r:r+k,u*QB:(u+1)*QB]=ps[-1]
        o=nn(kT[64*h:64*h+64,r0:r0+n],jnp.concatenate(ps,0))
        st[u]['dq']=o if c==0 else st[u]['dq']+o
        if c==3 and h==1:
            dq_ref[qb*QB:(qb+1)*QB,:]=(jnp.concatenate([st[u-1]['dq'],st[u]['dq']],0)*0.125).T.astype(BF)
    def E(qb,c):
        r0,n=CH[c]
        cols=slice(qb*512,(qb+1)*512)
        for w,(src,rhs) in enumerate(((p_scr,dor),(ds_scr,qr))):
            x=nn(src[r0:r0+n,cols],rhs[cols,:])
            dvk[w,r0:r0+n,:]=dvk[w,r0:r0+n,:]+x
    sp={}
    z16=jnp.zeros((16,128),BF)
    def pair_rows(x):
        return jnp.concatenate([jnp.where(lane<64,x,z16),jnp.where(lane>=64,x,z16)],0)
    def pick(xT):
        x=xT.T
        return jnp.where(lane<64,x[:16],x[16:])
    def SA():
        sp['qm']=pair_rows(qs[1024:,:])
        s=nt(k_ref[...],sp['qm'])
        s=jnp.where(lax.broadcasted_iota(jnp.int32,(T,32),0)<NT,s,NEG)
        m=jnp.max(fold(s,jnp.maximum),axis=0,keepdims=True); e=jnp.exp(s-m)
        sp['rl']=1.0/jnp.sum(fold(e,jnp.add),axis=0,keepdims=True)
        ss[...]=e
    def SB():
        sp['dom']=pair_rows(do_ref[1024:,:])
        sps[...]=(ss[...]*sp['rl']).astype(BF)
        oT=nn(vT[...],sps[...])
        sp['delta']=jnp.sum(oT*sp['dom'].T.astype(F32),axis=0,keepdims=True)
        a_ref[1024:,:]=pick(oT).astype(BF)
    def SC():
        dp=nt(v_ref[...],sp['dom']).astype(BF).astype(F32)
        sds[...]=((ss[...]*sp['rl'])*(dp-sp['delta'])).astype(BF)
        dq_ref[1024:,:]=pick(nn(kT[...],sds[...])*0.125).astype(BF)
    def SE():
        dvk[0]=nn(sps[...],sp['dom'])
        dvk[1]=nn(sds[...],sp['qm'])
    extra={(0,0):lambda:vT.__setitem__(Ellipsis,v_ref[...].T),(0,1):lambda:doT.__setitem__(Ellipsis,do_ref[...].T),
           (0,2):SA,(1,1):lambda:kT.__setitem__(Ellipsis,k_ref[...].T),(1,2):SB,(2,1):SC,(3,1):SE}
    for t in range(U+4):
        for c in range(4):
            if t<U: A(t,c)
            if 0<=t-1<U: C(t-1,c)
            if 0<=t-2<U: D(t-2,c)
            e=t-4
            if e>=0 and e//2<4 and c%2==0:
                E(e//2,(e%2)*2+c//2)
            if (t,c) in extra: extra[t,c]()
    if True:
        dv_ref[...]=dvk[0].astype(BF)
        dk_ref[...]=dvk[1].astype(BF)


LN_EPS = 1e-6
ANY = pl.BlockSpec(memory_space=pl.ANY)
VM = pl.BlockSpec(memory_space=pltpu.VMEM)
VMEM_LIMIT = 63 * 1024 * 1024
TWO = jax.ShapeDtypeStruct((2, T, 768), BF)


def whole(shape):
    return pl.BlockSpec(shape, lambda *g: (0,) * len(shape))


def params(**kw):
    return pltpu.CompilerParams(vmem_limit_bytes=VMEM_LIMIT, **kw)


def layer_stats(xf):
    cen = xf - jnp.mean(xf, axis=-1, keepdims=True)
    inv = lax.rsqrt(jnp.mean(cen * cen, axis=-1, keepdims=True) + LN_EPS)
    return cen * inv, inv


def row(ref):
    return ref[...].reshape(1, -1)


def attention(i, qkv, do, prev):
    spec = lambda o: pl.BlockSpec((T, 128), lambda j, o=o: (0, o + j))
    n = len(prev)
    return pl.pallas_call(
        functools.partial(attn_kernel, n), grid=(6,),
        in_specs=[spec(0), spec(6), spec(12), spec(0)] + [ANY] * n,
        out_specs=[pl.BlockSpec((None, T, 128), lambda j: (i, 0, j))] * 4,
        out_shape=[TWO] * 4,
        input_output_aliases={4 + m: m for m in range(n)},
        scratch_shapes=[pltpu.VMEM((T, 128), BF), pltpu.VMEM((4, T, QB), F32), pltpu.VMEM((T, 2048), BF), pltpu.VMEM((T, 2048), BF),
                        pltpu.VMEM((2048, 128), BF), pltpu.VMEM((2048, 128), BF),
                        pltpu.VMEM((128, T), BF), pltpu.VMEM((128, T), BF), pltpu.VMEM((128, T), BF), pltpu.VMEM((2, T, 128), F32)]
        + [pltpu.VMEM((4, 24, QB), F32)] * 3 + [pltpu.VMEM((T, 32), F32)] + [pltpu.VMEM((T, 32), BF)] * 2,
        compiler_params=params(),
        cost_estimate=pl.CostEstimate(flops=48 * 12 * 1026 * 1026 * 64, bytes_accessed=12 * 1024 * 1024, transcendentals=12 * 1026 * 1026),
        name="attn")(qkv, qkv, qkv, do, *prev)


def front_kernel(i, num_in, *refs):
    ins = refs[:num_in]
    x_patch, dy_patch, x_special, dy_special, wq_h, bq, ls, lb, wp_h, lsc = ins[:10]
    num_out = 10 if i == 0 else 6
    outs, refs = refs[num_in:num_in + num_out], refs[num_in + num_out:]
    if i == 0:
        qkv_o, do_o = (outs[0], outs[6]), (outs[1], outs[7])
    else:
        qkv_o, do_o = (None, outs[0]), (None, outs[1])
    normed_o, xs_o, dproj_o, dys_o = outs[2:6]
    buf, spec, qkv, do, normed, dproj, wq, wp, recv, loc, osem, wsem = refs[:12]
    me = lax.axis_index('sp')
    core = me & 1
    rows = lambda b: pl.ds(pl.multiple_of((me ^ b) * 256, 256), 256)
    remote, arrive, local, later = [], {}, {}, []
    if i == 0:
        send, stage, ssem = refs[12:]
        dp = lax.axis_index('dp')
        barrier = pltpu.get_barrier_semaphore()
        for b in (1, 2, 3):
            pl.semaphore_signal(barrier, inc=1, device_id=(dp, me ^ b), device_id_type=pl.DeviceIdType.MESH)
        pl.semaphore_wait(barrier, 3)
        plan = [(0, k, b) for k in range(2) for b in (2, 3, 1)] + [(1, k, 1) for k in range(2)]
        for n, (m, k, b) in enumerate(plan):
            c = pltpu.make_async_remote_copy(
                src_ref=(x_patch, dy_patch)[k].at[2 * (core ^ (b & 1)) + m], dst_ref=buf.at[m, k, rows(0)],
                send_sem=send.at[n], recv_sem=recv.at[n],
                device_id=(dp, me ^ b), device_id_type=pl.DeviceIdType.MESH)
            c.start()
            remote.append(c)
            arrive[m, k, b] = c.wait_recv
        for m in range(2):
            for k, (patch, special) in enumerate(((x_patch, x_special), (dy_patch, dy_special))):
                own = pltpu.make_async_copy(patch.at[2 * core + m], buf.at[m, k, rows(0)], loc.at[4 * m + 2 * k])
                sp = pltpu.make_async_copy(special.at[2 * core + m], spec.at[m, k], loc.at[4 * m + 2 * k + 1])
                own.start()
                sp.start()
                local[m, k] = (own, sp)
        for k, patch in enumerate((x_patch, dy_patch)):
            for m, target in enumerate((2 * core + 1, 2 * (1 - core) + 1)):
                c = pltpu.make_async_copy(patch.at[target], stage.at[m, k], ssem.at[2 * m + k])
                c.start()
                later.append((c, pltpu.make_async_copy(stage.at[m, k], outs[8 + m].at[k], ssem.at[4 + 2 * m + k])))
    else:
        for k in range(2):
            for b in (2, 3):
                c = pltpu.make_async_copy(ins[8 + b].at[k], buf.at[1, k, rows(b)], recv.at[2 * k + b - 2])
                c.start()
                arrive[1, k, b] = c.wait
    weights = [pltpu.make_async_copy(wq_h, wq, wsem.at[0]), pltpu.make_async_copy(wp_h, wp, wsem.at[1])]
    for c in weights:
        c.start()
    emitted = []

    def emit(src, dst, r):
        c = pltpu.make_async_copy(src.at[r], dst.at[r], osem.at[len(emitted)])
        c.start()
        emitted.append(c)

    def step(m, k, r):
        if k == 0:
            x_hat, _ = layer_stats(buf[m, 0, r, :].astype(F32))
            nb = (x_hat * row(ls) + row(lb)).astype(BF)
            normed[m, r, :] = nb
            for j in range(3):
                c = slice(768 * j, 768 * j + 768)
                qkv[m, r, c] = (nn(nb, wq[:, c]) + row(bq)[:, c]).astype(BF)
            emit(buf.at[m, 0], xs_o.at[m], r)
            emit(normed.at[m], normed_o.at[m], r)
            emit(qkv.at[m], qkv_o[m], r)
        else:
            d = (buf[m, 1, r, :].astype(F32) * row(lsc)).astype(BF)
            dproj[m, r, :] = d
            do[m, r, :] = nt(d, wp[...]).astype(BF)
            emit(buf.at[m, 1], dys_o.at[m], r)
            emit(dproj.at[m], dproj_o.at[m], r)
            emit(do.at[m], do_o[m], r)

    def near(m, k):
        own, sp = local[m, k]
        own.wait()
        sp.wait()
        buf[m, k, 1024:, :] = jnp.concatenate([spec[m, k], jnp.zeros((14, 768), BF)], 0)
        step(m, k, rows(0))
        step(m, k, pl.ds(1024, 16))
        arrive[m, k, 1]()
        step(m, k, rows(1))

    def far(m, k):
        for b in (2, 3):
            arrive[m, k, b]()
            step(m, k, rows(b))

    for c in weights:
        c.wait()
    if i == 0:
        near(0, 0)
        near(0, 1)
        for c, out in later:
            c.wait()
            out.start()
        near(1, 0)
        far(0, 0)
        near(1, 1)
        far(0, 1)
    else:
        far(1, 0)
        far(1, 1)
    for c in remote:
        c.wait_send()
    for _, out in later:
        out.wait()
    for c in emitted:
        c.wait()


def front(i, patches, consts, parts, prev):
    v = lambda *s: pltpu.VMEM(s, BF)
    dma = lambda n: pltpu.SemaphoreType.DMA((n,))
    wide, thin = jax.ShapeDtypeStruct((T, 2304), BF), jax.ShapeDtypeStruct((T, 768), BF)
    out_shape = [wide, thin] + [TWO] * 4
    scratch = [v(2, 2, T, 768), v(2, 2, 2, 768), v(2, T, 2304), v(2, T, 768), v(2, T, 768), v(2, T, 768),
               v(768, 2304), v(768, 768), dma(8), dma(8), dma(48), dma(2)]
    extra = {}
    if i == 0:
        out_shape += [wide, thin] + [jax.ShapeDtypeStruct((2, 256, 768), BF)] * 2
        scratch += [dma(8), v(2, 2, 256, 768), dma(8)]
        extra = dict(collective_id=0, has_side_effects=True)
    first = 10 + len(parts)
    return pl.pallas_call(
        functools.partial(front_kernel, i, first + len(prev)),
        in_specs=[ANY] * 5 + [VM] * 3 + [ANY, VM] + [ANY] * (len(parts) + len(prev)),
        out_specs=[ANY] * len(out_shape), out_shape=out_shape, scratch_shapes=scratch,
        input_output_aliases={first + m: m for m in range(len(prev))},
        compiler_params=params(**extra),
        cost_estimate=pl.CostEstimate(flops=2 * T * 768 * 3072, bytes_accessed=24 * 1024 * 1024, transcendentals=0),
        name="front")(*patches, *consts, *parts, *prev)


def back_kernel(place, *refs):
    ins, refs = refs[:12], refs[12:]
    w_ref, wp_ref, ls, bp, lsc, give, keep, vec, buf = refs
    i = pl.program_id(0)
    blocks = ((0, 256), (256, 256), (512, 16))

    def get(s, m):
        return ins[m][256 * s:256 * s + 256, :] if s < 2 else ins[6 + m][...]

    def products(s):
        dn = sum(nt(get(s, 3 + j), w_ref[:, 768 * j:768 * j + 768]) for j in range(3))
        return nn(get(s, 2), wp_ref[...]), dn

    def finish_rows(s, proj, dn):
        xf, dyf = get(s, 0).astype(F32), get(s, 1).astype(F32)
        x_hat, inv = layer_stats(xf)
        proj = proj + row(bp)
        dn = dn.astype(BF).astype(F32)
        gh = dn * row(ls)
        dr = inv * (gh - jnp.mean(gh, -1, keepdims=True) - x_hat * jnp.mean(gh * x_hat, -1, keepdims=True))
        r0, n = blocks[s]
        buf[0, r0:r0 + n, :] = (xf + row(lsc) * proj).astype(BF)
        buf[1, r0:r0 + n, :] = (dyf + dr).astype(BF)
        red = lambda t: jnp.sum(t, axis=0, keepdims=True)
        sums = [red(dn * x_hat), red(dn), red(dyf * row(lsc)), red(dyf * proj)] + [red(get(s, 3 + j).astype(F32)) for j in range(3)]
        return jnp.concatenate(sums + [jnp.zeros((1, 768), F32)], 0)

    p0 = products(0)
    p2 = products(2)
    v = finish_rows(0, *p0)
    p1 = products(1)
    v = v + jnp.where(place[0] == 0, 1.0, 0.0) * finish_rows(2, *p2)
    v = v + finish_rows(1, *p1)
    for k in range(2):
        keep[k, :256, :] = buf[k, pl.ds(pl.multiple_of(place[1] * 256, 256), 256), :]
        give[k, :256, :] = buf[k, pl.ds(pl.multiple_of((1 - place[1]) * 256, 256), 256), :]
        keep[k, 256:, :] = buf[k, 512:, :]
        give[k, 256:, :] = buf[k, 512:, :]

    @pl.when(i == 0)
    def _():
        vec[...] = v

    @pl.when(i == 1)
    def _():
        vec[...] += v


def back(place, xs, dys, a, dqs, w_qkv, w_proj, ln_scale, b_proj, layer_scale):
    arrays = (xs, dys, a) + tuple(dqs)
    blk = pl.BlockSpec((None, 512, 768), lambda i, c: (i, c[0], 0))
    sblk = pl.BlockSpec((None, 16, 768), lambda i, c: (i, 64, 0))
    out = pl.BlockSpec((2, None, 272, 768), lambda i, c: (0, i, 0, 0))
    half = jax.ShapeDtypeStruct((2, 2, 272, 768), BF)
    return pl.pallas_call(
        back_kernel,
        grid_spec=pltpu.PrefetchScalarGridSpec(
            num_scalar_prefetch=1, grid=(2,),
            in_specs=[blk] * 6 + [sblk] * 6 + [whole((768, 2304)), whole((768, 768))] + [VM] * 3,
            out_specs=[out, out, whole((8, 768))],
            scratch_shapes=[pltpu.VMEM((2, 528, 768), BF)]),
        out_shape=[half, half, jax.ShapeDtypeStruct((8, 768), F32)],
        compiler_params=params(),
        cost_estimate=pl.CostEstimate(flops=2 * 1056 * 768 * 3072, bytes_accessed=20 * 1024 * 1024, transcendentals=0),
        name="back")(place, *arrays, *arrays, w_qkv, w_proj, ln_scale, b_proj, layer_scale)


def finish_kernel(place, keep, got, *refs):
    ins, (gq, gp, out, dx, out_s, dx_s) = refs[:6], refs[6:]
    for m in range(2):
        gq[:, 768 * m:768 * m + 768] = ins[2 * m][...] + ins[2 * m + 1][...]
    gp[...] = ins[4][...] + ins[5][...]
    m = pl.program_id(0)
    own = (m >> 1) == place[1]

    @pl.when(own)
    def _():
        out[...] = keep[0, :256, :]
        dx[...] = keep[1, :256, :]
        out_s[...] = keep[0, 256:272, :][:2]
        dx_s[...] = keep[1, 256:272, :][:2]

    @pl.when(jnp.logical_not(own))
    def _():
        out[...] = got[0, :256, :]
        dx[...] = got[1, :256, :]
        out_s[...] = got[0, 256:272, :][:2]
        dx_s[...] = got[1, 256:272, :][:2]


def finish(place, keep, got, pairs):
    flat = [t for p in pairs for t in p]
    blk = pl.BlockSpec((192, 768), lambda g, c: (g, 0))
    src = pl.BlockSpec((2, None, 272, 768), lambda g, c: (0, g & 1, 0, 0))
    dst = pl.BlockSpec((None, 256, 768), lambda g, c: (g, 0, 0))
    dst_s = pl.BlockSpec((None, 2, 768), lambda g, c: (g, 0, 0))
    big, small = jax.ShapeDtypeStruct((4, 256, 768), BF), jax.ShapeDtypeStruct((4, 2, 768), BF)
    return pl.pallas_call(
        finish_kernel,
        grid_spec=pltpu.PrefetchScalarGridSpec(
            num_scalar_prefetch=1, grid=(4,),
            in_specs=[src, src] + [blk] * 6,
            out_specs=[pl.BlockSpec((192, 1536), lambda g, c: (g, 0)), blk, dst, dst, dst_s, dst_s]),
        out_shape=[jax.ShapeDtypeStruct((768, 2304), F32), jax.ShapeDtypeStruct((768, 768), F32), big, big, small, small],
        compiler_params=params(),
        cost_estimate=pl.CostEstimate(flops=3 * 768 * 768, bytes_accessed=36 * 768 * 768, transcendentals=0),
        name="finish")(place, keep, got, *flat)


def last_add_kernel(p, q, _, out):
    out[...] = p[...] + q[...]


def last_add(pair, gq):
    blk = pl.BlockSpec((192, 768), lambda g: (g, 0))
    return pl.pallas_call(
        last_add_kernel, grid=(4,), in_specs=[blk, blk, ANY],
        out_specs=pl.BlockSpec((192, 768), lambda g: (g, 2)),
        out_shape=jax.ShapeDtypeStruct((768, 2304), F32), input_output_aliases={2: 0},
        compiler_params=params(),
        cost_estimate=pl.CostEstimate(flops=768 * 768, bytes_accessed=12 * 768 * 768, transcendentals=0),
        name="last_add")(*pair, gq)


def solution(mesh):
    n = mesh.shape['sp']
    swaps = {b: [(s, s ^ b) for s in range(n)] for b in (1, 2, 3)}

    def swap(x, b):
        return lax.ppermute(x, 'sp', swaps[b])

    def local_block(x_special, x_patch, dy_special, dy_patch, ln_scale, ln_bias, w_qkv, b_qkv, w_proj, b_proj, layer_scale):
        shard = lax.axis_index('sp')
        place = jnp.stack([shard >> 1, shard & 1])
        patches = (x_patch, dy_patch, x_special, dy_special)
        consts = (w_qkv, b_qkv, ln_scale, ln_bias, w_proj, layer_scale)
        qkv, d_attn, *saved, qkv1, d_attn1, mine, other = front(0, patches, consts, (), ())
        parts = (swap(mine, 2), swap(other, 3))
        prev = attention(0, qkv, d_attn, ())
        qkv, d_attn, *saved = front(1, patches, consts, parts, (qkv1, d_attn1, *saved))
        a, *dqs = attention(1, qkv, d_attn, prev)
        normed, xs, d_proj, dys = saved
        give, keep, vec = back(place, xs, dys, a, dqs, w_qkv, w_proj, ln_scale, b_proj, layer_scale)
        got = swap(give, 1)
        around = [swap(vec, b) for b in (1, 2, 3)]
        vec, normed = lax.optimization_barrier((vec, normed))

        def tn(p, q):
            return lax.dot_general(p.reshape(2 * T, 768), q.reshape(2 * T, 768), (((0,), (0,)), ((), ())), preferred_element_type=F32)

        parts = [tn(normed, dqs[0]), tn(normed, dqs[1])]
        around, normed, a = lax.optimization_barrier((around, normed, a))
        parts += [tn(a, d_proj), tn(normed, dqs[2])]
        t = (vec + around[0]) + (around[1] + around[2])
        pairs = [(p, swap(p, 1)) for p in parts]
        gq, gp, out, dx, out_s, dx_s = finish(place, keep, got, pairs[:3])
        gq = last_add(pairs[3], gq)
        return out_s, out, dx_s, dx, t[0], t[1], gq, t[4:7].reshape(-1), gp, t[2], t[3]

    rows, seq, rep = P('dp'), P('dp', 'sp'), P()
    return jax.shard_map(local_block, mesh=mesh,
                         in_specs=(rows, seq, rows, seq) + (rep,) * 7,
                         out_specs=(rows, seq, rows, seq) + (rows,) * 7, check_vma=False)
```

```python
import functools
import jax, jax.numpy as jnp
from jax import lax
from jax.sharding import PartitionSpec as P
from jax.experimental import pallas as pl
from jax.experimental.pallas import tpu as pltpu
F32=jnp.float32; BF=jnp.bfloat16
T=1040; NT=1026; QB=256
NEG=-1e30
SUB=64
def nt(a,b): return lax.dot_general(a,b,(((1,),(1,)),((),())),preferred_element_type=F32)
def nn(a,b): return jnp.dot(a,b,preferred_element_type=F32)
CH=[(0,256),(256,256),(512,256),(768,272)]
def fold(x,op):
    r=x.shape[0]//8
    x=x.reshape(r,8,x.shape[1])
    g=[x[i] for i in range(r)]
    while len(g)>1:
        g=[op(g[i],g[i+1]) for i in range(0,len(g)-1,2)]+([g[-1]] if len(g)%2 else [])
    return g[0]

def attn_kernel(num_alias,q_ref,k_ref,v_ref,do_ref,*refs):
    a_ref,dq_ref,dk_ref,dv_ref,qs,s_scr,p_scr,ds_scr,dor,qr,kT,vT,doT,dvk,ms,lsum,fs,ss,sps,sds=refs[num_alias:]
    lane=lax.broadcasted_iota(jnp.int32,(1,128),1)
    qs[...]=(q_ref[...].astype(F32)*0.125).astype(BF)
    z=jnp.zeros((QB,128),BF)
    units=[(qb,h) for qb in range(4) for h in range(2)]
    U=len(units)
    st=[dict() for _ in units]
    def mask_q(u):
        qb,h=units[u]; mh=(lane<64) if h==0 else (lane>=64)
        qr[u*QB:(u+1)*QB,:]=jnp.where(mh,qs[qb*QB:(qb+1)*QB,:],z)
    def mask_do(u):
        qb,h=units[u]; mh=(lane<64) if h==0 else (lane>=64)
        dor[u*QB:(u+1)*QB,:]=jnp.where(mh,do_ref[qb*QB:(qb+1)*QB,:],z)
    nsub=1024//SUB+1
    def subs(c):
        r0,n=CH[c]
        out=[(r0+i,SUB,(r0+i)//SUB) for i in range(0,256,SUB)]
        if c==3: out.append((1024,16,nsub-1))
        return out
    ms[...]=jnp.full(ms.shape,NEG,F32)
    lsum[...]=jnp.zeros(lsum.shape,F32)
    def A(u,c):
        r0,n=CH[c]; s_ref=s_scr.at[u%4]
        if c==0: mask_q(u)
        s=nt(k_ref[r0:r0+n,:],qr[u*QB:(u+1)*QB,:])
        for r,k,i in subs(c):
            x=s[r-r0:r-r0+k]
            if r==1024:
                x=jnp.where(lax.broadcasted_iota(jnp.int32,(16,QB),0)<2,x,NEG)
            m=jnp.max(fold(x,jnp.maximum),axis=0,keepdims=True)
            e=jnp.exp(x-m)
            s_ref[r:r+k,:]=e
            ms[u%4,i:i+1,:]=m
            lsum[u%4,i:i+1,:]=jnp.sum(fold(e,jnp.add),axis=0,keepdims=True)
        if c==3:
            mm=ms[u%4]
            f=jnp.exp(mm-jnp.max(mm,axis=0,keepdims=True))
            fs[u%4]=f*(1.0/jnp.sum(lsum[u%4]*f,axis=0,keepdims=True))
    def C(u,c):
        qb,h=units[u]; r0,n=CH[c]; s_ref=s_scr.at[u%4]
        ps=[]
        for r,k,i in subs(c):
            p=s_ref[r:r+k,:]*fs[u%4,i:i+1,:]
            ps.append(p.astype(BF))
            s_ref[r:r+k,:]=p
            p_scr[r:r+k,u*QB:(u+1)*QB]=ps[-1]
        o=nn(vT[64*h:64*h+64,r0:r0+n],jnp.concatenate(ps,0))
        st[u]['o']=o if c==0 else st[u]['o']+o
        if c==3:
            st[u]['delta']=jnp.sum(st[u]['o']*doT[64*h:64*h+64,qb*QB:(qb+1)*QB].astype(F32),axis=0,keepdims=True)
            if h==1:
                a_ref[qb*QB:(qb+1)*QB,:]=jnp.concatenate([st[u-1]['o'],st[u]['o']],0).T.astype(BF)
    def D(u,c):
        qb,h=units[u]; r0,n=CH[c]; s_ref=s_scr.at[u%4]
        if c==0: mask_do(u)
        dp=nt(v_ref[r0:r0+n,:],dor[u*QB:(u+1)*QB,:])
        ps=[]
        for r,k,i in subs(c):
            x=dp[r-r0:r-r0+k].astype(BF).astype(F32)
            p=s_ref[r:r+k,:]
            ps.append((p*(x-st[u]['delta'])).astype(BF))
            ds_scr[r:r+k,u*QB:(u+1)*QB]=ps[-1]
        o=nn(kT[64*h:64*h+64,r0:r0+n],jnp.concatenate(ps,0))
        st[u]['dq']=o if c==0 else st[u]['dq']+o
        if c==3 and h==1:
            dq_ref[qb*QB:(qb+1)*QB,:]=(jnp.concatenate([st[u-1]['dq'],st[u]['dq']],0)*0.125).T.astype(BF)
    def E(qb,c):
        r0,n=CH[c]
        cols=slice(qb*512,(qb+1)*512)
        for w,(src,rhs) in enumerate(((p_scr,dor),(ds_scr,qr))):
            x=nn(src[r0:r0+n,cols],rhs[cols,:])
            dvk[w,r0:r0+n,:]=dvk[w,r0:r0+n,:]+x
    sp={}
    z16=jnp.zeros((16,128),BF)
    def pair_rows(x):
        return jnp.concatenate([jnp.where(lane<64,x,z16),jnp.where(lane>=64,x,z16)],0)
    def pick(xT):
        x=xT.T
        return jnp.where(lane<64,x[:16],x[16:])
    def SA():
        sp['qm']=pair_rows(qs[1024:,:])
        s=nt(k_ref[...],sp['qm'])
        s=jnp.where(lax.broadcasted_iota(jnp.int32,(T,32),0)<NT,s,NEG)
        m=jnp.max(fold(s,jnp.maximum),axis=0,keepdims=True); e=jnp.exp(s-m)
        sp['rl']=1.0/jnp.sum(fold(e,jnp.add),axis=0,keepdims=True)
        ss[...]=e
    def SB():
        sp['dom']=pair_rows(do_ref[1024:,:])
        sps[...]=(ss[...]*sp['rl']).astype(BF)
        oT=nn(vT[...],sps[...])
        sp['delta']=jnp.sum(oT*sp['dom'].T.astype(F32),axis=0,keepdims=True)
        a_ref[1024:,:]=pick(oT).astype(BF)
    def SC():
        dp=nt(v_ref[...],sp['dom']).astype(BF).astype(F32)
        sds[...]=((ss[...]*sp['rl'])*(dp-sp['delta'])).astype(BF)
        dq_ref[1024:,:]=pick(nn(kT[...],sds[...])*0.125).astype(BF)
    def SE():
        dvk[0]=nn(sps[...],sp['dom'])
        dvk[1]=nn(sds[...],sp['qm'])
    extra={(0,0):lambda:vT.__setitem__(Ellipsis,v_ref[...].T),(0,1):lambda:doT.__setitem__(Ellipsis,do_ref[...].T),
           (0,2):SA,(1,1):lambda:kT.__setitem__(Ellipsis,k_ref[...].T),(1,2):SB,(2,1):SC,(3,1):SE}
    for t in range(U+4):
        for c in range(4):
            if t<U: A(t,c)
            if 0<=t-1<U: C(t-1,c)
            if 0<=t-2<U: D(t-2,c)
            e=t-4
            if e>=0 and e//2<4 and c%2==0:
                E(e//2,(e%2)*2+c//2)
            if (t,c) in extra: extra[t,c]()
    if True:
        dv_ref[...]=dvk[0].astype(BF)
        dk_ref[...]=dvk[1].astype(BF)


LN_EPS = 1e-6
ANY = pl.BlockSpec(memory_space=pl.ANY)
VM = pl.BlockSpec(memory_space=pltpu.VMEM)
VMEM_LIMIT = 63 * 1024 * 1024
TWO = jax.ShapeDtypeStruct((2, T, 768), BF)


def whole(shape):
    return pl.BlockSpec(shape, lambda *g: (0,) * len(shape))


def params(**kw):
    return pltpu.CompilerParams(vmem_limit_bytes=VMEM_LIMIT, **kw)


def layer_stats(xf):
    cen = xf - jnp.mean(xf, axis=-1, keepdims=True)
    inv = lax.rsqrt(jnp.mean(cen * cen, axis=-1, keepdims=True) + LN_EPS)
    return cen * inv, inv


def row(ref):
    return ref[...].reshape(1, -1)


def attention(i, qkv, do, prev):
    spec = lambda o: pl.BlockSpec((T, 128), lambda j, o=o: (0, o + j))
    n = len(prev)
    return pl.pallas_call(
        functools.partial(attn_kernel, n), grid=(6,),
        in_specs=[spec(0), spec(6), spec(12), spec(0)] + [ANY] * n,
        out_specs=[pl.BlockSpec((None, T, 128), lambda j: (i, 0, j))] * 4,
        out_shape=[TWO] * 4,
        input_output_aliases={4 + m: m for m in range(n)},
        scratch_shapes=[pltpu.VMEM((T, 128), BF), pltpu.VMEM((4, T, QB), F32), pltpu.VMEM((T, 2048), BF), pltpu.VMEM((T, 2048), BF),
                        pltpu.VMEM((2048, 128), BF), pltpu.VMEM((2048, 128), BF),
                        pltpu.VMEM((128, T), BF), pltpu.VMEM((128, T), BF), pltpu.VMEM((128, T), BF), pltpu.VMEM((2, T, 128), F32)]
        + [pltpu.VMEM((4, 24, QB), F32)] * 3 + [pltpu.VMEM((T, 32), F32)] + [pltpu.VMEM((T, 32), BF)] * 2,
        compiler_params=params(),
        cost_estimate=pl.CostEstimate(flops=48 * 12 * 1026 * 1026 * 64, bytes_accessed=12 * 1024 * 1024, transcendentals=12 * 1026 * 1026),
        name="attn")(qkv, qkv, qkv, do, *prev)


def front_kernel(i, num_in, *refs):
    ins = refs[:num_in]
    x_patch, dy_patch, x_special, dy_special, wq_h, bq, ls, lb, wp_h, lsc = ins[:10]
    num_out = 10 if i == 0 else 6
    outs, refs = refs[num_in:num_in + num_out], refs[num_in + num_out:]
    if i == 0:
        qkv_o, do_o = (outs[0], outs[6]), (outs[1], outs[7])
    else:
        qkv_o, do_o = (None, outs[0]), (None, outs[1])
    normed_o, xs_o, dproj_o, dys_o = outs[2:6]
    buf, spec, qkv, do, normed, dproj, wq, wp, recv, loc, osem, wsem = refs[:12]
    me = lax.axis_index('sp')
    core = me & 1
    rows = lambda b: pl.ds(pl.multiple_of((me ^ b) * 256, 256), 256)
    remote, arrive, local, later = [], {}, {}, []
    if i == 0:
        send, stage, ssem = refs[12:]
        dp = lax.axis_index('dp')
        barrier = pltpu.get_barrier_semaphore()
        for b in (1, 2, 3):
            pl.semaphore_signal(barrier, inc=1, device_id=(dp, me ^ b), device_id_type=pl.DeviceIdType.MESH)
        pl.semaphore_wait(barrier, 3)
        plan = [(0, k, b) for k in range(2) for b in (2, 3, 1)] + [(1, k, 1) for k in range(2)]
        for n, (m, k, b) in enumerate(plan):
            c = pltpu.make_async_remote_copy(
                src_ref=(x_patch, dy_patch)[k].at[2 * (core ^ (b & 1)) + m], dst_ref=buf.at[m, k, rows(0)],
                send_sem=send.at[n], recv_sem=recv.at[n],
                device_id=(dp, me ^ b), device_id_type=pl.DeviceIdType.MESH)
            c.start()
            remote.append(c)
            arrive[m, k, b] = c.wait_recv
        for m in range(2):
            for k, (patch, special) in enumerate(((x_patch, x_special), (dy_patch, dy_special))):
                own = pltpu.make_async_copy(patch.at[2 * core + m], buf.at[m, k, rows(0)], loc.at[4 * m + 2 * k])
                sp = pltpu.make_async_copy(special.at[2 * core + m], spec.at[m, k], loc.at[4 * m + 2 * k + 1])
                own.start()
                sp.start()
                local[m, k] = (own, sp)
        for k, patch in enumerate((x_patch, dy_patch)):
            for m, target in enumerate((2 * core + 1, 2 * (1 - core) + 1)):
                c = pltpu.make_async_copy(patch.at[target], stage.at[m, k], ssem.at[2 * m + k])
                c.start()
                later.append((c, pltpu.make_async_copy(stage.at[m, k], outs[8 + m].at[k], ssem.at[4 + 2 * m + k])))
    else:
        for k in range(2):
            for b in (2, 3):
                c = pltpu.make_async_copy(ins[8 + b].at[k], buf.at[1, k, rows(b)], recv.at[2 * k + b - 2])
                c.start()
                arrive[1, k, b] = c.wait
    weights = [pltpu.make_async_copy(wq_h, wq, wsem.at[0]), pltpu.make_async_copy(wp_h, wp, wsem.at[1])]
    for c in weights:
        c.start()
    emitted = []

    def emit(src, dst, r):
        c = pltpu.make_async_copy(src.at[r], dst.at[r], osem.at[len(emitted)])
        c.start()
        emitted.append(c)

    def step(m, k, r):
        if k == 0:
            x_hat, _ = layer_stats(buf[m, 0, r, :].astype(F32))
            nb = (x_hat * row(ls) + row(lb)).astype(BF)
            normed[m, r, :] = nb
            for j in range(3):
                c = slice(768 * j, 768 * j + 768)
                qkv[m, r, c] = (nn(nb, wq[:, c]) + row(bq)[:, c]).astype(BF)
            emit(buf.at[m, 0], xs_o.at[m], r)
            emit(normed.at[m], normed_o.at[m], r)
            emit(qkv.at[m], qkv_o[m], r)
        else:
            d = (buf[m, 1, r, :].astype(F32) * row(lsc)).astype(BF)
            dproj[m, r, :] = d
            do[m, r, :] = nt(d, wp[...]).astype(BF)
            emit(buf.at[m, 1], dys_o.at[m], r)
            emit(dproj.at[m], dproj_o.at[m], r)
            emit(do.at[m], do_o[m], r)

    def near(m, k):
        own, sp = local[m, k]
        own.wait()
        sp.wait()
        buf[m, k, 1024:, :] = jnp.concatenate([spec[m, k], jnp.zeros((14, 768), BF)], 0)
        step(m, k, rows(0))
        step(m, k, pl.ds(1024, 16))
        arrive[m, k, 1]()
        step(m, k, rows(1))

    def far(m, k):
        for b in (2, 3):
            arrive[m, k, b]()
            step(m, k, rows(b))

    for c in weights:
        c.wait()
    if i == 0:
        near(0, 0)
        near(0, 1)
        for c, out in later:
            c.wait()
            out.start()
        near(1, 0)
        far(0, 0)
        near(1, 1)
        far(0, 1)
    else:
        far(1, 0)
        far(1, 1)
    for c in remote:
        c.wait_send()
    for _, out in later:
        out.wait()
    for c in emitted:
        c.wait()


def front(i, patches, consts, parts, prev):
    v = lambda *s: pltpu.VMEM(s, BF)
    dma = lambda n: pltpu.SemaphoreType.DMA((n,))
    wide, thin = jax.ShapeDtypeStruct((T, 2304), BF), jax.ShapeDtypeStruct((T, 768), BF)
    out_shape = [wide, thin] + [TWO] * 4
    scratch = [v(2, 2, T, 768), v(2, 2, 2, 768), v(2, T, 2304), v(2, T, 768), v(2, T, 768), v(2, T, 768),
               v(768, 2304), v(768, 768), dma(8), dma(8), dma(48), dma(2)]
    extra = {}
    if i == 0:
        out_shape += [wide, thin] + [jax.ShapeDtypeStruct((2, 256, 768), BF)] * 2
        scratch += [dma(8), v(2, 2, 256, 768), dma(8)]
        extra = dict(collective_id=0, has_side_effects=True)
    first = 10 + len(parts)
    return pl.pallas_call(
        functools.partial(front_kernel, i, first + len(prev)),
        in_specs=[ANY] * 5 + [VM] * 3 + [ANY, VM] + [ANY] * (len(parts) + len(prev)),
        out_specs=[ANY] * len(out_shape), out_shape=out_shape, scratch_shapes=scratch,
        input_output_aliases={first + m: m for m in range(len(prev))},
        compiler_params=params(**extra),
        cost_estimate=pl.CostEstimate(flops=2 * T * 768 * 3072, bytes_accessed=24 * 1024 * 1024, transcendentals=0),
        name="front")(*patches, *consts, *parts, *prev)


def back_kernel(place, *refs):
    ins, refs = refs[:12], refs[12:]
    w_ref, wp_ref, ls, bp, lsc, give, keep, vec, buf = refs
    i = pl.program_id(0)
    blocks = ((0, 256), (256, 256), (512, 16))

    def get(s, m):
        return ins[m][256 * s:256 * s + 256, :] if s < 2 else ins[6 + m][...]

    def products(s):
        full = (lambda m: get(s, m)) if s else (lambda m: jnp.concatenate([get(0, m), get(2, m)], 0))
        dn = sum(nt(full(3 + j), w_ref[:, 768 * j:768 * j + 768]) for j in range(3))
        return nn(full(2), wp_ref[...]), dn

    def finish_rows(s, proj, dn):
        xf, dyf = get(s, 0).astype(F32), get(s, 1).astype(F32)
        x_hat, inv = layer_stats(xf)
        proj = proj + row(bp)
        dn = dn.astype(BF).astype(F32)
        gh = dn * row(ls)
        dr = inv * (gh - jnp.mean(gh, -1, keepdims=True) - x_hat * jnp.mean(gh * x_hat, -1, keepdims=True))
        r0, n = blocks[s]
        buf[0, r0:r0 + n, :] = (xf + row(lsc) * proj).astype(BF)
        buf[1, r0:r0 + n, :] = (dyf + dr).astype(BF)
        red = lambda t: jnp.sum(t, axis=0, keepdims=True)
        sums = [red(dn * x_hat), red(dn), red(dyf * row(lsc)), red(dyf * proj)] + [red(get(s, 3 + j).astype(F32)) for j in range(3)]
        return jnp.concatenate(sums + [jnp.zeros((1, 768), F32)], 0)

    p0 = products(0)
    p1 = products(1)
    v = finish_rows(0, *(t[:256] for t in p0))
    v = v + jnp.where(place[0] == 0, 1.0, 0.0) * finish_rows(2, *(t[256:] for t in p0))
    v = v + finish_rows(1, *p1)
    for k in range(2):
        keep[k, :256, :] = buf[k, pl.ds(pl.multiple_of(place[1] * 256, 256), 256), :]
        give[k, :256, :] = buf[k, pl.ds(pl.multiple_of((1 - place[1]) * 256, 256), 256), :]
        keep[k, 256:, :] = buf[k, 512:, :]
        give[k, 256:, :] = buf[k, 512:, :]

    @pl.when(i == 0)
    def _():
        vec[...] = v

    @pl.when(i == 1)
    def _():
        vec[...] += v


def back(place, xs, dys, a, dqs, w_qkv, w_proj, ln_scale, b_proj, layer_scale):
    arrays = (xs, dys, a) + tuple(dqs)
    blk = pl.BlockSpec((None, 512, 768), lambda i, c: (i, c[0], 0))
    sblk = pl.BlockSpec((None, 16, 768), lambda i, c: (i, 64, 0))
    out = pl.BlockSpec((2, None, 272, 768), lambda i, c: (0, i, 0, 0))
    half = jax.ShapeDtypeStruct((2, 2, 272, 768), BF)
    return pl.pallas_call(
        back_kernel,
        grid_spec=pltpu.PrefetchScalarGridSpec(
            num_scalar_prefetch=1, grid=(2,),
            in_specs=[blk] * 6 + [sblk] * 6 + [whole((768, 2304)), whole((768, 768))] + [VM] * 3,
            out_specs=[out, out, whole((8, 768))],
            scratch_shapes=[pltpu.VMEM((2, 528, 768), BF)]),
        out_shape=[half, half, jax.ShapeDtypeStruct((8, 768), F32)],
        compiler_params=params(),
        cost_estimate=pl.CostEstimate(flops=2 * 1056 * 768 * 3072, bytes_accessed=20 * 1024 * 1024, transcendentals=0),
        name="back")(place, *arrays, *arrays, w_qkv, w_proj, ln_scale, b_proj, layer_scale)


def finish_kernel(place, keep, got, *refs):
    ins, (gq, gp, out, dx, out_s, dx_s) = refs[:6], refs[6:]
    for m in range(2):
        gq[:, 768 * m:768 * m + 768] = ins[2 * m][...] + ins[2 * m + 1][...]
    gp[...] = ins[4][...] + ins[5][...]
    m = pl.program_id(0)
    own = (m >> 1) == place[1]

    @pl.when(own)
    def _():
        out[...] = keep[0, :256, :]
        dx[...] = keep[1, :256, :]
        out_s[...] = keep[0, 256:272, :][:2]
        dx_s[...] = keep[1, 256:272, :][:2]

    @pl.when(jnp.logical_not(own))
    def _():
        out[...] = got[0, :256, :]
        dx[...] = got[1, :256, :]
        out_s[...] = got[0, 256:272, :][:2]
        dx_s[...] = got[1, 256:272, :][:2]


def finish(place, keep, got, pairs):
    flat = [t for p in pairs for t in p]
    blk = pl.BlockSpec((192, 768), lambda g, c: (g, 0))
    src = [pl.BlockSpec((2, None, 272, 768), lambda g, c, f=f: (0, jnp.clip(g - 2 * (f ^ c[1]), 0, 1), 0, 0)) for f in (0, 1)]
    dst = pl.BlockSpec((None, 256, 768), lambda g, c: (g, 0, 0))
    dst_s = pl.BlockSpec((None, 2, 768), lambda g, c: (g, 0, 0))
    big, small = jax.ShapeDtypeStruct((4, 256, 768), BF), jax.ShapeDtypeStruct((4, 2, 768), BF)
    return pl.pallas_call(
        finish_kernel,
        grid_spec=pltpu.PrefetchScalarGridSpec(
            num_scalar_prefetch=1, grid=(4,),
            in_specs=src + [blk] * 6,
            out_specs=[pl.BlockSpec((192, 1536), lambda g, c: (g, 0)), blk, dst, dst, dst_s, dst_s]),
        out_shape=[jax.ShapeDtypeStruct((768, 2304), F32), jax.ShapeDtypeStruct((768, 768), F32), big, big, small, small],
        compiler_params=params(),
        cost_estimate=pl.CostEstimate(flops=3 * 768 * 768, bytes_accessed=36 * 768 * 768, transcendentals=0),
        name="finish")(place, keep, got, *flat)


def last_add_kernel(p, q, _, out):
    out[...] = p[...] + q[...]


def last_add(pair, gq):
    blk = pl.BlockSpec((192, 768), lambda g: (g, 0))
    return pl.pallas_call(
        last_add_kernel, grid=(4,), in_specs=[blk, blk, ANY],
        out_specs=pl.BlockSpec((192, 768), lambda g: (g, 2)),
        out_shape=jax.ShapeDtypeStruct((768, 2304), F32), input_output_aliases={2: 0},
        compiler_params=params(),
        cost_estimate=pl.CostEstimate(flops=768 * 768, bytes_accessed=12 * 768 * 768, transcendentals=0),
        name="last_add")(*pair, gq)


def solution(mesh):
    n = mesh.shape['sp']
    swaps = {b: [(s, s ^ b) for s in range(n)] for b in (1, 2, 3)}

    def swap(x, b):
        return lax.ppermute(x, 'sp', swaps[b])

    def local_block(x_special, x_patch, dy_special, dy_patch, ln_scale, ln_bias, w_qkv, b_qkv, w_proj, b_proj, layer_scale):
        shard = lax.axis_index('sp')
        place = jnp.stack([shard >> 1, shard & 1])
        patches = (x_patch, dy_patch, x_special, dy_special)
        consts = (w_qkv, b_qkv, ln_scale, ln_bias, w_proj, layer_scale)
        qkv, d_attn, *saved, qkv1, d_attn1, mine, other = front(0, patches, consts, (), ())
        parts = (swap(mine, 2), swap(other, 3))
        prev = attention(0, qkv, d_attn, ())
        qkv, d_attn, *saved = front(1, patches, consts, parts, (qkv1, d_attn1, *saved))
        a, *dqs = attention(1, qkv, d_attn, prev)
        normed, xs, d_proj, dys = saved
        give, keep, vec = back(place, xs, dys, a, dqs, w_qkv, w_proj, ln_scale, b_proj, layer_scale)
        got = swap(give, 1)
        around = [swap(vec, b) for b in (1, 2, 3)]
        vec, normed = lax.optimization_barrier((vec, normed))

        def tn(p, q):
            return lax.dot_general(p.reshape(2 * T, 768), q.reshape(2 * T, 768), (((0,), (0,)), ((), ())), preferred_element_type=F32)

        parts = [tn(normed, dqs[0]), tn(normed, dqs[1])]
        around, got, normed, a = lax.optimization_barrier((around, got, normed, a))
        parts += [tn(a, d_proj), tn(normed, dqs[2])]
        t = (vec + around[0]) + (around[1] + around[2])
        pairs = [(p, swap(p, 1)) for p in parts]
        gq, gp, out, dx, out_s, dx_s = finish(place, keep, got, pairs[:3])
        gq = last_add(pairs[3], gq)
        return out_s, out, dx_s, dx, t[0], t[1], gq, t[4:7].reshape(-1), gp, t[2], t[3]

    rows, seq, rep = P('dp'), P('dp', 'sp'), P()
    return jax.shard_map(local_block, mesh=mesh,
                         in_specs=(rows, seq, rows, seq) + (rep,) * 7,
                         out_specs=(rows, seq, rows, seq) + (rows,) * 7, check_vma=False)
```

```python
import functools
import jax, jax.numpy as jnp
from jax import lax
from jax.sharding import PartitionSpec as P
from jax.experimental import pallas as pl
from jax.experimental.pallas import tpu as pltpu
F32=jnp.float32; BF=jnp.bfloat16
T=1040; NT=1026; QB=256
NEG=-1e30
SUB=64
def nt(a,b): return lax.dot_general(a,b,(((1,),(1,)),((),())),preferred_element_type=F32)
def nn(a,b): return jnp.dot(a,b,preferred_element_type=F32)
CH=[(0,256),(256,256),(512,256),(768,272)]
def fold(x,op):
    r=x.shape[0]//8
    x=x.reshape(r,8,x.shape[1])
    g=[x[i] for i in range(r)]
    while len(g)>1:
        g=[op(g[i],g[i+1]) for i in range(0,len(g)-1,2)]+([g[-1]] if len(g)%2 else [])
    return g[0]

def attn_kernel(num_alias,q_ref,k_ref,v_ref,do_ref,*refs):
    a_ref,dq_ref,dk_ref,dv_ref,qs,s_scr,p_scr,ds_scr,dor,qr,kT,vT,doT,dvk,ms,lsum,fs,ss,sps,sds=refs[num_alias:]
    lane=lax.broadcasted_iota(jnp.int32,(1,128),1)
    qs[...]=(q_ref[...].astype(F32)*0.125).astype(BF)
    z=jnp.zeros((QB,128),BF)
    units=[(qb,h) for qb in range(4) for h in range(2)]
    U=len(units)
    st=[dict() for _ in units]
    def mask_q(u):
        qb,h=units[u]; mh=(lane<64) if h==0 else (lane>=64)
        qr[u*QB:(u+1)*QB,:]=jnp.where(mh,qs[qb*QB:(qb+1)*QB,:],z)
    def mask_do(u):
        qb,h=units[u]; mh=(lane<64) if h==0 else (lane>=64)
        dor[u*QB:(u+1)*QB,:]=jnp.where(mh,do_ref[qb*QB:(qb+1)*QB,:],z)
    nsub=1024//SUB+1
    def subs(c):
        r0,n=CH[c]
        out=[(r0+i,SUB,(r0+i)//SUB) for i in range(0,256,SUB)]
        if c==3: out.append((1024,16,nsub-1))
        return out
    ms[...]=jnp.full(ms.shape,NEG,F32)
    lsum[...]=jnp.zeros(lsum.shape,F32)
    def A(u,c):
        r0,n=CH[c]; s_ref=s_scr.at[u%4]
        if c==0: mask_q(u)
        s=nt(k_ref[r0:r0+n,:],qr[u*QB:(u+1)*QB,:])
        for r,k,i in subs(c):
            x=s[r-r0:r-r0+k]
            if r==1024:
                x=jnp.where(lax.broadcasted_iota(jnp.int32,(16,QB),0)<2,x,NEG)
            m=jnp.max(fold(x,jnp.maximum),axis=0,keepdims=True)
            e=jnp.exp(x-m)
            s_ref[r:r+k,:]=e
            ms[u%4,i:i+1,:]=m
            lsum[u%4,i:i+1,:]=jnp.sum(fold(e,jnp.add),axis=0,keepdims=True)
        if c==3:
            mm=ms[u%4]
            f=jnp.exp(mm-jnp.max(mm,axis=0,keepdims=True))
            fs[u%4]=f*(1.0/jnp.sum(lsum[u%4]*f,axis=0,keepdims=True))
    def C(u,c):
        qb,h=units[u]; r0,n=CH[c]; s_ref=s_scr.at[u%4]
        ps=[]
        for r,k,i in subs(c):
            p=s_ref[r:r+k,:]*fs[u%4,i:i+1,:]
            ps.append(p.astype(BF))
            s_ref[r:r+k,:]=p
            p_scr[r:r+k,u*QB:(u+1)*QB]=ps[-1]
        o=nn(vT[64*h:64*h+64,r0:r0+n],jnp.concatenate(ps,0))
        st[u]['o']=o if c==0 else st[u]['o']+o
        if c==3:
            st[u]['delta']=jnp.sum(st[u]['o']*doT[64*h:64*h+64,qb*QB:(qb+1)*QB].astype(F32),axis=0,keepdims=True)
            if h==1:
                a_ref[qb*QB:(qb+1)*QB,:]=jnp.concatenate([st[u-1]['o'],st[u]['o']],0).T.astype(BF)
    def D(u,c):
        qb,h=units[u]; r0,n=CH[c]; s_ref=s_scr.at[u%4]
        if c==0: mask_do(u)
        dp=nt(v_ref[r0:r0+n,:],dor[u*QB:(u+1)*QB,:])
        ps=[]
        for r,k,i in subs(c):
            x=dp[r-r0:r-r0+k].astype(BF).astype(F32)
            p=s_ref[r:r+k,:]
            ps.append((p*(x-st[u]['delta'])).astype(BF))
            ds_scr[r:r+k,u*QB:(u+1)*QB]=ps[-1]
        o=nn(kT[64*h:64*h+64,r0:r0+n],jnp.concatenate(ps,0))
        st[u]['dq']=o if c==0 else st[u]['dq']+o
        if c==3 and h==1:
            dq_ref[qb*QB:(qb+1)*QB,:]=(jnp.concatenate([st[u-1]['dq'],st[u]['dq']],0)*0.125).T.astype(BF)
    def E(qb,c):
        r0,n=CH[c]
        cols=slice(qb*512,(qb+1)*512)
        for w,(src,rhs) in enumerate(((p_scr,dor),(ds_scr,qr))):
            x=nn(src[r0:r0+n,cols],rhs[cols,:])
            dvk[w,r0:r0+n,:]=dvk[w,r0:r0+n,:]+x
    sp={}
    z16=jnp.zeros((16,128),BF)
    def pair_rows(x):
        return jnp.concatenate([jnp.where(lane<64,x,z16),jnp.where(lane>=64,x,z16)],0)
    def pick(xT):
        x=xT.T
        return jnp.where(lane<64,x[:16],x[16:])
    def SA():
        sp['qm']=pair_rows(qs[1024:,:])
        s=nt(k_ref[...],sp['qm'])
        s=jnp.where(lax.broadcasted_iota(jnp.int32,(T,32),0)<NT,s,NEG)
        m=jnp.max(fold(s,jnp.maximum),axis=0,keepdims=True); e=jnp.exp(s-m)
        sp['rl']=1.0/jnp.sum(fold(e,jnp.add),axis=0,keepdims=True)
        ss[...]=e
    def SB():
        sp['dom']=pair_rows(do_ref[1024:,:])
        sps[...]=(ss[...]*sp['rl']).astype(BF)
        oT=nn(vT[...],sps[...])
        sp['delta']=jnp.sum(oT*sp['dom'].T.astype(F32),axis=0,keepdims=True)
        a_ref[1024:,:]=pick(oT).astype(BF)
    def SC():
        dp=nt(v_ref[...],sp['dom']).astype(BF).astype(F32)
        sds[...]=((ss[...]*sp['rl'])*(dp-sp['delta'])).astype(BF)
        dq_ref[1024:,:]=pick(nn(kT[...],sds[...])*0.125).astype(BF)
    def SE():
        dvk[0]=nn(sps[...],sp['dom'])
        dvk[1]=nn(sds[...],sp['qm'])
    extra={(0,0):lambda:vT.__setitem__(Ellipsis,v_ref[...].T),(0,1):lambda:doT.__setitem__(Ellipsis,do_ref[...].T),
           (0,2):SA,(1,1):lambda:kT.__setitem__(Ellipsis,k_ref[...].T),(1,2):SB,(2,1):SC,(3,1):SE}
    for t in range(U+4):
        for c in range(4):
            if t<U: A(t,c)
            if 0<=t-1<U: C(t-1,c)
            if 0<=t-2<U: D(t-2,c)
            e=t-4
            if e>=0 and e//2<4 and c%2==0:
                E(e//2,(e%2)*2+c//2)
            if (t,c) in extra: extra[t,c]()
    if True:
        dv_ref[...]=dvk[0].astype(BF)
        dk_ref[...]=dvk[1].astype(BF)


LN_EPS = 1e-6
ANY = pl.BlockSpec(memory_space=pl.ANY)
VM = pl.BlockSpec(memory_space=pltpu.VMEM)
VMEM_LIMIT = 63 * 1024 * 1024
TWO = jax.ShapeDtypeStruct((2, T, 768), BF)


def whole(shape):
    return pl.BlockSpec(shape, lambda *g: (0,) * len(shape))


def params(**kw):
    return pltpu.CompilerParams(vmem_limit_bytes=VMEM_LIMIT, **kw)


def layer_stats(xf):
    cen = xf - jnp.mean(xf, axis=-1, keepdims=True)
    inv = lax.rsqrt(jnp.mean(cen * cen, axis=-1, keepdims=True) + LN_EPS)
    return cen * inv, inv


def row(ref):
    return ref[...].reshape(1, -1)


def attention(i, qkv, do, prev):
    spec = lambda o: pl.BlockSpec((T, 128), lambda j, o=o: (0, o + j))
    n = len(prev)
    return pl.pallas_call(
        functools.partial(attn_kernel, n), grid=(6,),
        in_specs=[spec(0), spec(6), spec(12), spec(0)] + [ANY] * n,
        out_specs=[pl.BlockSpec((None, T, 128), lambda j: (i, 0, j))] * 4,
        out_shape=[TWO] * 4,
        input_output_aliases={4 + m: m for m in range(n)},
        scratch_shapes=[pltpu.VMEM((T, 128), BF), pltpu.VMEM((4, T, QB), F32), pltpu.VMEM((T, 2048), BF), pltpu.VMEM((T, 2048), BF),
                        pltpu.VMEM((2048, 128), BF), pltpu.VMEM((2048, 128), BF),
                        pltpu.VMEM((128, T), BF), pltpu.VMEM((128, T), BF), pltpu.VMEM((128, T), BF), pltpu.VMEM((2, T, 128), F32)]
        + [pltpu.VMEM((4, 24, QB), F32)] * 3 + [pltpu.VMEM((T, 32), F32)] + [pltpu.VMEM((T, 32), BF)] * 2,
        compiler_params=params(),
        cost_estimate=pl.CostEstimate(flops=48 * 12 * 1026 * 1026 * 64, bytes_accessed=12 * 1024 * 1024, transcendentals=12 * 1026 * 1026),
        name="attn")(qkv, qkv, qkv, do, *prev)


def front_kernel(i, num_in, *refs):
    ins = refs[:num_in]
    x_patch, dy_patch, x_special, dy_special, wq_h, bq, ls, lb, wp_h, lsc = ins[:10]
    num_out = 10 if i == 0 else 6
    outs, refs = refs[num_in:num_in + num_out], refs[num_in + num_out:]
    if i == 0:
        qkv_o, do_o = (outs[0], outs[6]), (outs[1], outs[7])
    else:
        qkv_o, do_o = (None, outs[0]), (None, outs[1])
    normed_o, xs_o, dproj_o, dys_o = outs[2:6]
    buf, spec, qkv, do, normed, dproj, wq, wp, recv, loc, osem, wsem = refs[:12]
    me = lax.axis_index('sp')
    core = me & 1
    rows = lambda b: pl.ds(pl.multiple_of((me ^ b) * 256, 256), 256)
    remote, arrive, local, later = [], {}, {}, []
    if i == 0:
        send, stage, ssem = refs[12:]
        dp = lax.axis_index('dp')
        barrier = pltpu.get_barrier_semaphore()
        for b in (1, 2, 3):
            pl.semaphore_signal(barrier, inc=1, device_id=(dp, me ^ b), device_id_type=pl.DeviceIdType.MESH)
        pl.semaphore_wait(barrier, 3)
        plan = [(0, k, b) for k in range(2) for b in (2, 3, 1)] + [(1, k, 1) for k in range(2)]
        for n, (m, k, b) in enumerate(plan):
            c = pltpu.make_async_remote_copy(
                src_ref=(x_patch, dy_patch)[k].at[2 * (core ^ (b & 1)) + m], dst_ref=buf.at[m, k, rows(0)],
                send_sem=send.at[n], recv_sem=recv.at[n],
                device_id=(dp, me ^ b), device_id_type=pl.DeviceIdType.MESH)
            c.start()
            remote.append(c)
            arrive[m, k, b] = c.wait_recv
        for m in range(2):
            for k, (patch, special) in enumerate(((x_patch, x_special), (dy_patch, dy_special))):
                own = pltpu.make_async_copy(patch.at[2 * core + m], buf.at[m, k, rows(0)], loc.at[4 * m + 2 * k])
                sp = pltpu.make_async_copy(special.at[2 * core + m], spec.at[m, k], loc.at[4 * m + 2 * k + 1])
                own.start()
                sp.start()
                local[m, k] = (own, sp)
        for k, patch in enumerate((x_patch, dy_patch)):
            for m, target in enumerate((2 * core + 1, 2 * (1 - core) + 1)):
                c = pltpu.make_async_copy(patch.at[target], stage.at[m, k], ssem.at[2 * m + k])
                c.start()
                later.append((c, pltpu.make_async_copy(stage.at[m, k], outs[8 + m].at[k], ssem.at[4 + 2 * m + k])))
    else:
        for k in range(2):
            for b in (2, 3):
                c = pltpu.make_async_copy(ins[8 + b].at[k], buf.at[1, k, rows(b)], recv.at[2 * k + b - 2])
                c.start()
                arrive[1, k, b] = c.wait
    weights = [pltpu.make_async_copy(wq_h, wq, wsem.at[0]), pltpu.make_async_copy(wp_h, wp, wsem.at[1])]
    for c in weights:
        c.start()
    emitted = []

    def emit(src, dst, r):
        c = pltpu.make_async_copy(src.at[r], dst.at[r], osem.at[len(emitted)])
        c.start()
        emitted.append(c)

    def step(m, k, r):
        if k == 0:
            x_hat, _ = layer_stats(buf[m, 0, r, :].astype(F32))
            nb = (x_hat * row(ls) + row(lb)).astype(BF)
            normed[m, r, :] = nb
            for j in range(3):
                c = slice(768 * j, 768 * j + 768)
                qkv[m, r, c] = (nn(nb, wq[:, c]) + row(bq)[:, c]).astype(BF)
            emit(buf.at[m, 0], xs_o.at[m], r)
            emit(normed.at[m], normed_o.at[m], r)
            emit(qkv.at[m], qkv_o[m], r)
        else:
            d = (buf[m, 1, r, :].astype(F32) * row(lsc)).astype(BF)
            dproj[m, r, :] = d
            do[m, r, :] = nt(d, wp[...]).astype(BF)
            emit(buf.at[m, 1], dys_o.at[m], r)
            emit(dproj.at[m], dproj_o.at[m], r)
            emit(do.at[m], do_o[m], r)

    def near(m, k):
        own, sp = local[m, k]
        own.wait()
        sp.wait()
        buf[m, k, 1024:, :] = jnp.concatenate([spec[m, k], jnp.zeros((14, 768), BF)], 0)
        step(m, k, rows(0))
        step(m, k, pl.ds(1024, 16))
        arrive[m, k, 1]()
        step(m, k, rows(1))

    def far(m, k):
        for b in (2, 3):
            arrive[m, k, b]()
            step(m, k, rows(b))

    for c in weights:
        c.wait()
    if i == 0:
        near(0, 0)
        near(0, 1)
        for c, out in later:
            c.wait()
            out.start()
        near(1, 0)
        far(0, 0)
        near(1, 1)
        far(0, 1)
    else:
        far(1, 0)
        far(1, 1)
    for c in remote:
        c.wait_send()
    for _, out in later:
        out.wait()
    for c in emitted:
        c.wait()


def front(i, patches, consts, parts, prev):
    v = lambda *s: pltpu.VMEM(s, BF)
    dma = lambda n: pltpu.SemaphoreType.DMA((n,))
    wide, thin = jax.ShapeDtypeStruct((T, 2304), BF), jax.ShapeDtypeStruct((T, 768), BF)
    out_shape = [wide, thin] + [TWO] * 4
    scratch = [v(2, 2, T, 768), v(2, 2, 2, 768), v(2, T, 2304), v(2, T, 768), v(2, T, 768), v(2, T, 768),
               v(768, 2304), v(768, 768), dma(8), dma(8), dma(48), dma(2)]
    extra = {}
    if i == 0:
        out_shape += [wide, thin] + [jax.ShapeDtypeStruct((2, 256, 768), BF)] * 2
        scratch += [dma(8), v(2, 2, 256, 768), dma(8)]
        extra = dict(collective_id=0, has_side_effects=True)
    first = 10 + len(parts)
    return pl.pallas_call(
        functools.partial(front_kernel, i, first + len(prev)),
        in_specs=[ANY] * 5 + [VM] * 3 + [ANY, VM] + [ANY] * (len(parts) + len(prev)),
        out_specs=[ANY] * len(out_shape), out_shape=out_shape, scratch_shapes=scratch,
        input_output_aliases={first + m: m for m in range(len(prev))},
        compiler_params=params(**extra),
        cost_estimate=pl.CostEstimate(flops=2 * T * 768 * 3072, bytes_accessed=24 * 1024 * 1024, transcendentals=0),
        name="front")(*patches, *consts, *parts, *prev)


def back_kernel(place, *refs):
    ins, refs = refs[:12], refs[12:]
    w_ref, wp_ref, ls, bp, lsc, give, keep, vec, buf = refs
    i = pl.program_id(0)
    blocks = ((0, 256), (256, 256), (512, 16))

    def get(s, m):
        return ins[m][256 * s:256 * s + 256, :] if s < 2 else ins[6 + m][...]

    def products(s):
        full = (lambda m: get(s, m)) if s else (lambda m: jnp.concatenate([get(0, m), get(2, m)], 0))
        dn = sum(nt(full(3 + j), w_ref[:, 768 * j:768 * j + 768]) for j in range(3))
        return nn(full(2), wp_ref[...]), dn

    def finish_rows(s, proj, dn):
        xf, dyf = get(s, 0).astype(F32), get(s, 1).astype(F32)
        x_hat, inv = layer_stats(xf)
        proj = proj + row(bp)
        dn = dn.astype(BF).astype(F32)
        gh = dn * row(ls)
        dr = inv * (gh - jnp.mean(gh, -1, keepdims=True) - x_hat * jnp.mean(gh * x_hat, -1, keepdims=True))
        r0, n = blocks[s]
        buf[0, r0:r0 + n, :] = (xf + row(lsc) * proj).astype(BF)
        buf[1, r0:r0 + n, :] = (dyf + dr).astype(BF)
        red = lambda t: jnp.sum(t, axis=0, keepdims=True)
        sums = [red(dn * x_hat), red(dn), red(dyf * row(lsc)), red(dyf * proj)] + [red(get(s, 3 + j).astype(F32)) for j in range(3)]
        return jnp.concatenate(sums + [jnp.zeros((1, 768), F32)], 0)

    p0 = products(0)
    p1 = products(1)
    v = finish_rows(0, *(t[:256] for t in p0))
    v = v + jnp.where(place[0] == 0, 1.0, 0.0) * finish_rows(2, *(t[256:] for t in p0))
    v = v + finish_rows(1, *p1)
    for k in range(2):
        keep[k, :256, :] = buf[k, pl.ds(pl.multiple_of(place[1] * 256, 256), 256), :]
        give[k, :256, :] = buf[k, pl.ds(pl.multiple_of((1 - place[1]) * 256, 256), 256), :]
        keep[k, 256:, :] = buf[k, 512:, :]
        give[k, 256:, :] = buf[k, 512:, :]

    @pl.when(i == 0)
    def _():
        vec[...] = v

    @pl.when(i == 1)
    def _():
        vec[...] += v


def back(place, xs, dys, a, dqs, w_qkv, w_proj, ln_scale, b_proj, layer_scale):
    arrays = (xs, dys, a) + tuple(dqs)
    blk = pl.BlockSpec((None, 512, 768), lambda i, c: (i, c[0], 0))
    sblk = pl.BlockSpec((None, 16, 768), lambda i, c: (i, 64, 0))
    out = pl.BlockSpec((2, None, 272, 768), lambda i, c: (0, i, 0, 0))
    half = jax.ShapeDtypeStruct((2, 2, 272, 768), BF)
    return pl.pallas_call(
        back_kernel,
        grid_spec=pltpu.PrefetchScalarGridSpec(
            num_scalar_prefetch=1, grid=(2,),
            in_specs=[blk] * 6 + [sblk] * 6 + [whole((768, 2304)), whole((768, 768))] + [VM] * 3,
            out_specs=[out, out, whole((8, 768))],
            scratch_shapes=[pltpu.VMEM((2, 528, 768), BF)]),
        out_shape=[half, half, jax.ShapeDtypeStruct((8, 768), F32)],
        compiler_params=params(),
        cost_estimate=pl.CostEstimate(flops=2 * 1056 * 768 * 3072, bytes_accessed=20 * 1024 * 1024, transcendentals=0),
        name="back")(place, *arrays, *arrays, w_qkv, w_proj, ln_scale, b_proj, layer_scale)


def grads_kernel(normed, dq, dk, dv, out, flipped):
    g = pl.program_id(0)

    @pl.when(g == 0)
    def _():
        flipped[...] = normed[...].reshape(2 * T, 768).T

    for j, ref in enumerate((dq, dk, dv)):
        @pl.when((g >= 3 * j) & (g < 3 * j + 3))
        def _(ref=ref):
            out[...] = nn(flipped[...], ref[...].reshape(2 * T, 256))


def grads(normed, dqs):
    return pl.pallas_call(
        grads_kernel, grid=(9,),
        in_specs=[VM] + [pl.BlockSpec((2, T, 256), lambda g, j=j: (0, 0, jnp.clip(g - 3 * j, 0, 2))) for j in range(3)],
        out_specs=pl.BlockSpec((768, 256), lambda g: (0, g)),
        out_shape=jax.ShapeDtypeStruct((768, 2304), F32),
        scratch_shapes=[pltpu.VMEM((768, 2 * T), BF)],
        compiler_params=params(),
        cost_estimate=pl.CostEstimate(flops=4 * T * 768 * 2304, bytes_accessed=20 * 1024 * 1024, transcendentals=0),
        name="grads")(normed, *dqs)


def finish_kernel(place, keep, got, own_w, got_w, gq, out, dx, out_s, dx_s):
    gq[...] = own_w[...] + got_w[...]
    own = (pl.program_id(0) >> 1) == place[1]

    def write(src):
        out[...] = src[0, :256, :]
        dx[...] = src[1, :256, :]
        out_s[...] = src[0, 256:272, :][:2]
        dx_s[...] = src[1, 256:272, :][:2]

    @pl.when(own)
    def _():
        write(keep)

    @pl.when(jnp.logical_not(own))
    def _():
        write(got)


def finish(place, keep, got, own_w, got_w):
    blk = pl.BlockSpec((192, 2304), lambda g, c: (g, 0))
    src = [pl.BlockSpec((2, None, 272, 768), lambda g, c, f=f: (0, jnp.clip(g - 2 * (f ^ c[1]), 0, 1), 0, 0)) for f in (0, 1)]
    dst = pl.BlockSpec((None, 256, 768), lambda g, c: (g, 0, 0))
    dst_s = pl.BlockSpec((None, 2, 768), lambda g, c: (g, 0, 0))
    big, small = jax.ShapeDtypeStruct((4, 256, 768), BF), jax.ShapeDtypeStruct((4, 2, 768), BF)
    return pl.pallas_call(
        finish_kernel,
        grid_spec=pltpu.PrefetchScalarGridSpec(
            num_scalar_prefetch=1, grid=(4,), in_specs=src + [blk, blk], out_specs=[blk, dst, dst, dst_s, dst_s]),
        out_shape=[jax.ShapeDtypeStruct((768, 2304), F32), big, big, small, small],
        compiler_params=params(),
        cost_estimate=pl.CostEstimate(flops=3 * 768 * 768, bytes_accessed=36 * 768 * 768, transcendentals=0),
        name="finish")(place, keep, got, own_w, got_w)


def solution(mesh):
    n = mesh.shape['sp']
    swaps = {b: [(s, s ^ b) for s in range(n)] for b in (1, 2, 3)}

    def swap(x, b):
        return lax.ppermute(x, 'sp', swaps[b])

    def local_block(x_special, x_patch, dy_special, dy_patch, ln_scale, ln_bias, w_qkv, b_qkv, w_proj, b_proj, layer_scale):
        shard = lax.axis_index('sp')
        place = jnp.stack([shard >> 1, shard & 1])
        patches = (x_patch, dy_patch, x_special, dy_special)
        consts = (w_qkv, b_qkv, ln_scale, ln_bias, w_proj, layer_scale)
        qkv, d_attn, *saved, qkv1, d_attn1, mine, other = front(0, patches, consts, (), ())
        parts = (swap(mine, 2), swap(other, 3))
        prev = attention(0, qkv, d_attn, ())
        qkv, d_attn, *saved = front(1, patches, consts, parts, (qkv1, d_attn1, *saved))
        a, *dqs = attention(1, qkv, d_attn, prev)
        normed, xs, d_proj, dys = saved
        gq = grads(normed, dqs)
        gq_got = swap(gq, 1)
        gq, a = lax.optimization_barrier((gq, a))
        gp = lax.dot_general(a.reshape(2 * T, 768), d_proj.reshape(2 * T, 768), (((0,), (0,)), ((), ())), preferred_element_type=F32)
        gp_got = swap(gp, 1)
        gp, xs = lax.optimization_barrier((gp, xs))
        give, keep, vec = back(place, xs, dys, a, dqs, w_qkv, w_proj, ln_scale, b_proj, layer_scale)
        give, vec, gp, gp_got = lax.optimization_barrier((give, vec, gp, gp_got))
        got = swap(give, 1)
        around = [swap(vec, b) for b in (1, 2, 3)]
        gp = gp + gp_got
        t = (vec + around[0]) + (around[1] + around[2])
        gq, out, dx, out_s, dx_s = finish(place, keep, got, gq, gq_got)
        return out_s, out, dx_s, dx, t[0], t[1], gq, t[4:7].reshape(-1), gp, t[2], t[3]

    rows, seq, rep = P('dp'), P('dp', 'sp'), P()
    return jax.shard_map(local_block, mesh=mesh,
                         in_specs=(rows, seq, rows, seq) + (rep,) * 7,
                         out_specs=(rows, seq, rows, seq) + (rows,) * 7, check_vma=False)
```

```python
import functools
import jax, jax.numpy as jnp
from jax import lax
from jax.sharding import PartitionSpec as P
from jax.experimental import pallas as pl
from jax.experimental.pallas import tpu as pltpu
F32=jnp.float32; BF=jnp.bfloat16
T=1040; NT=1026; QB=256
NEG=-1e30
SUB=64
def nt(a,b): return lax.dot_general(a,b,(((1,),(1,)),((),())),preferred_element_type=F32)
def nn(a,b): return jnp.dot(a,b,preferred_element_type=F32)
CH=[(0,256),(256,256),(512,256),(768,272)]
def fold(x,op):
    r=x.shape[0]//8
    x=x.reshape(r,8,x.shape[1])
    g=[x[i] for i in range(r)]
    while len(g)>1:
        g=[op(g[i],g[i+1]) for i in range(0,len(g)-1,2)]+([g[-1]] if len(g)%2 else [])
    return g[0]

def attn_kernel(num_alias,q_ref,k_ref,v_ref,do_ref,*refs):
    a_ref,dq_ref,dk_ref,dv_ref,qs,s_scr,p_scr,ds_scr,dor,qr,kT,vT,doT,dvk,ms,lsum,fs,ss,sps,sds=refs[num_alias:]
    lane=lax.broadcasted_iota(jnp.int32,(1,128),1)
    qs[...]=(q_ref[...].astype(F32)*0.125).astype(BF)
    z=jnp.zeros((QB,128),BF)
    units=[(qb,h) for qb in range(4) for h in range(2)]
    U=len(units)
    st=[dict() for _ in units]
    def mask_q(u):
        qb,h=units[u]; mh=(lane<64) if h==0 else (lane>=64)
        qr[u*QB:(u+1)*QB,:]=jnp.where(mh,qs[qb*QB:(qb+1)*QB,:],z)
    def mask_do(u):
        qb,h=units[u]; mh=(lane<64) if h==0 else (lane>=64)
        dor[u*QB:(u+1)*QB,:]=jnp.where(mh,do_ref[qb*QB:(qb+1)*QB,:],z)
    nsub=1024//SUB+1
    def subs(c):
        r0,n=CH[c]
        out=[(r0+i,SUB,(r0+i)//SUB) for i in range(0,256,SUB)]
        if c==3: out.append((1024,16,nsub-1))
        return out
    ms[...]=jnp.full(ms.shape,NEG,F32)
    lsum[...]=jnp.zeros(lsum.shape,F32)
    def A(u,c):
        r0,n=CH[c]; s_ref=s_scr.at[u%4]
        if c==0: mask_q(u)
        s=nt(k_ref[r0:r0+n,:],qr[u*QB:(u+1)*QB,:])
        for r,k,i in subs(c):
            x=s[r-r0:r-r0+k]
            if r==1024:
                x=jnp.where(lax.broadcasted_iota(jnp.int32,(16,QB),0)<2,x,NEG)
            m=jnp.max(fold(x,jnp.maximum),axis=0,keepdims=True)
            e=jnp.exp(x-m)
            s_ref[r:r+k,:]=e
            ms[u%4,i:i+1,:]=m
            lsum[u%4,i:i+1,:]=jnp.sum(fold(e,jnp.add),axis=0,keepdims=True)
        if c==3:
            mm=ms[u%4]
            f=jnp.exp(mm-jnp.max(mm,axis=0,keepdims=True))
            fs[u%4]=f*(1.0/jnp.sum(lsum[u%4]*f,axis=0,keepdims=True))
    def C(u,c):
        qb,h=units[u]; r0,n=CH[c]; s_ref=s_scr.at[u%4]
        ps=[]
        for r,k,i in subs(c):
            p=s_ref[r:r+k,:]*fs[u%4,i:i+1,:]
            ps.append(p.astype(BF))
            s_ref[r:r+k,:]=p
            p_scr[r:r+k,u*QB:(u+1)*QB]=ps[-1]
        o=nn(vT[64*h:64*h+64,r0:r0+n],jnp.concatenate(ps,0))
        st[u]['o']=o if c==0 else st[u]['o']+o
        if c==3:
            st[u]['delta']=jnp.sum(st[u]['o']*doT[64*h:64*h+64,qb*QB:(qb+1)*QB].astype(F32),axis=0,keepdims=True)
            if h==1:
                a_ref[qb*QB:(qb+1)*QB,:]=jnp.concatenate([st[u-1]['o'],st[u]['o']],0).T.astype(BF)
    def D(u,c):
        qb,h=units[u]; r0,n=CH[c]; s_ref=s_scr.at[u%4]
        if c==0: mask_do(u)
        dp=nt(v_ref[r0:r0+n,:],dor[u*QB:(u+1)*QB,:])
        ps=[]
        for r,k,i in subs(c):
            x=dp[r-r0:r-r0+k].astype(BF).astype(F32)
            p=s_ref[r:r+k,:]
            ps.append((p*(x-st[u]['delta'])).astype(BF))
            ds_scr[r:r+k,u*QB:(u+1)*QB]=ps[-1]
        o=nn(kT[64*h:64*h+64,r0:r0+n],jnp.concatenate(ps,0))
        st[u]['dq']=o if c==0 else st[u]['dq']+o
        if c==3 and h==1:
            dq_ref[qb*QB:(qb+1)*QB,:]=(jnp.concatenate([st[u-1]['dq'],st[u]['dq']],0)*0.125).T.astype(BF)
    def E(qb,c):
        r0,n=CH[c]
        cols=slice(qb*512,(qb+1)*512)
        for w,(src,rhs) in enumerate(((p_scr,dor),(ds_scr,qr))):
            x=nn(src[r0:r0+n,cols],rhs[cols,:])
            dvk[w,r0:r0+n,:]=dvk[w,r0:r0+n,:]+x
    sp={}
    z16=jnp.zeros((16,128),BF)
    def pair_rows(x):
        return jnp.concatenate([jnp.where(lane<64,x,z16),jnp.where(lane>=64,x,z16)],0)
    def pick(xT):
        x=xT.T
        return jnp.where(lane<64,x[:16],x[16:])
    def SA():
        sp['qm']=pair_rows(qs[1024:,:])
        s=nt(k_ref[...],sp['qm'])
        s=jnp.where(lax.broadcasted_iota(jnp.int32,(T,32),0)<NT,s,NEG)
        m=jnp.max(fold(s,jnp.maximum),axis=0,keepdims=True); e=jnp.exp(s-m)
        sp['rl']=1.0/jnp.sum(fold(e,jnp.add),axis=0,keepdims=True)
        ss[...]=e
    def SB():
        sp['dom']=pair_rows(do_ref[1024:,:])
        sps[...]=(ss[...]*sp['rl']).astype(BF)
        oT=nn(vT[...],sps[...])
        sp['delta']=jnp.sum(oT*sp['dom'].T.astype(F32),axis=0,keepdims=True)
        a_ref[1024:,:]=pick(oT).astype(BF)
    def SC():
        dp=nt(v_ref[...],sp['dom']).astype(BF).astype(F32)
        sds[...]=((ss[...]*sp['rl'])*(dp-sp['delta'])).astype(BF)
        dq_ref[1024:,:]=pick(nn(kT[...],sds[...])*0.125).astype(BF)
    def SE():
        dvk[0]=nn(sps[...],sp['dom'])
        dvk[1]=nn(sds[...],sp['qm'])
    extra={(0,0):lambda:vT.__setitem__(Ellipsis,v_ref[...].T),(0,1):lambda:doT.__setitem__(Ellipsis,do_ref[...].T),
           (0,2):SA,(1,1):lambda:kT.__setitem__(Ellipsis,k_ref[...].T),(1,2):SB,(2,1):SC,(3,1):SE}
    for t in range(U+4):
        for c in range(4):
            if t<U: A(t,c)
            if 0<=t-1<U: C(t-1,c)
            if 0<=t-2<U: D(t-2,c)
            e=t-4
            if e>=0 and e//2<4 and c%2==0:
                E(e//2,(e%2)*2+c//2)
            if (t,c) in extra: extra[t,c]()
    if True:
        dv_ref[...]=dvk[0].astype(BF)
        dk_ref[...]=dvk[1].astype(BF)


LN_EPS = 1e-6
ANY = pl.BlockSpec(memory_space=pl.ANY)
VM = pl.BlockSpec(memory_space=pltpu.VMEM)
VMEM_LIMIT = 63 * 1024 * 1024
TWO = jax.ShapeDtypeStruct((2, T, 768), BF)


def whole(shape):
    return pl.BlockSpec(shape, lambda *g: (0,) * len(shape))


def params(**kw):
    return pltpu.CompilerParams(vmem_limit_bytes=VMEM_LIMIT, **kw)


def layer_stats(xf):
    cen = xf - jnp.mean(xf, axis=-1, keepdims=True)
    inv = lax.rsqrt(jnp.mean(cen * cen, axis=-1, keepdims=True) + LN_EPS)
    return cen * inv, inv


def row(ref):
    return ref[...].reshape(1, -1)


def attention(i, qkv, do, prev):
    spec = lambda o: pl.BlockSpec((T, 128), lambda j, o=o: (0, o + j))
    n = len(prev)
    return pl.pallas_call(
        functools.partial(attn_kernel, n), grid=(6,),
        in_specs=[spec(0), spec(6), spec(12), spec(0)] + [ANY] * n,
        out_specs=[pl.BlockSpec((None, T, 128), lambda j: (i, 0, j))] * 4,
        out_shape=[TWO] * 4,
        input_output_aliases={4 + m: m for m in range(n)},
        scratch_shapes=[pltpu.VMEM((T, 128), BF), pltpu.VMEM((4, T, QB), F32), pltpu.VMEM((T, 2048), BF), pltpu.VMEM((T, 2048), BF),
                        pltpu.VMEM((2048, 128), BF), pltpu.VMEM((2048, 128), BF),
                        pltpu.VMEM((128, T), BF), pltpu.VMEM((128, T), BF), pltpu.VMEM((128, T), BF), pltpu.VMEM((2, T, 128), F32)]
        + [pltpu.VMEM((4, 24, QB), F32)] * 3 + [pltpu.VMEM((T, 32), F32)] + [pltpu.VMEM((T, 32), BF)] * 2,
        compiler_params=params(),
        cost_estimate=pl.CostEstimate(flops=48 * 12 * 1026 * 1026 * 64, bytes_accessed=12 * 1024 * 1024, transcendentals=12 * 1026 * 1026),
        name="attn")(qkv, qkv, qkv, do, *prev)


def front_kernel(i, num_in, *refs):
    ins = refs[:num_in]
    x_patch, dy_patch, x_special, dy_special, wq_h, bq, ls, lb, wp_h, lsc = ins[:10]
    num_out = 10 if i == 0 else 6
    outs, refs = refs[num_in:num_in + num_out], refs[num_in + num_out:]
    if i == 0:
        qkv_o, do_o = (outs[0], outs[6]), (outs[1], outs[7])
    else:
        qkv_o, do_o = (None, outs[0]), (None, outs[1])
    normed_o, xs_o, dproj_o, dys_o = outs[2:6]
    buf, spec, qkv, do, normed, dproj, wq, wp, recv, loc, osem, wsem = refs[:12]
    me = lax.axis_index('sp')
    core = me & 1
    rows = lambda b: pl.ds(pl.multiple_of((me ^ b) * 256, 256), 256)
    remote, arrive, local, later = [], {}, {}, []
    if i == 0:
        send, stage, ssem = refs[12:]
        dp = lax.axis_index('dp')
        barrier = pltpu.get_barrier_semaphore()
        for b in (1, 2, 3):
            pl.semaphore_signal(barrier, inc=1, device_id=(dp, me ^ b), device_id_type=pl.DeviceIdType.MESH)
        pl.semaphore_wait(barrier, 3)
        plan = [(0, k, b) for k in range(2) for b in (2, 3, 1)] + [(1, k, 1) for k in range(2)]
        for n, (m, k, b) in enumerate(plan):
            c = pltpu.make_async_remote_copy(
                src_ref=(x_patch, dy_patch)[k].at[2 * (core ^ (b & 1)) + m], dst_ref=buf.at[m, k, rows(0)],
                send_sem=send.at[n], recv_sem=recv.at[n],
                device_id=(dp, me ^ b), device_id_type=pl.DeviceIdType.MESH)
            c.start()
            remote.append(c)
            arrive[m, k, b] = c.wait_recv
        for m in range(2):
            for k, (patch, special) in enumerate(((x_patch, x_special), (dy_patch, dy_special))):
                own = pltpu.make_async_copy(patch.at[2 * core + m], buf.at[m, k, rows(0)], loc.at[4 * m + 2 * k])
                sp = pltpu.make_async_copy(special.at[2 * core + m], spec.at[m, k], loc.at[4 * m + 2 * k + 1])
                own.start()
                sp.start()
                local[m, k] = (own, sp)
        for k, patch in enumerate((x_patch, dy_patch)):
            for m, target in enumerate((2 * core + 1, 2 * (1 - core) + 1)):
                c = pltpu.make_async_copy(patch.at[target], stage.at[m, k], ssem.at[2 * m + k])
                c.start()
                later.append((c, pltpu.make_async_copy(stage.at[m, k], outs[8 + m].at[k], ssem.at[4 + 2 * m + k])))
    else:
        for k in range(2):
            for b in (2, 3):
                c = pltpu.make_async_copy(ins[8 + b].at[k], buf.at[1, k, rows(b)], recv.at[2 * k + b - 2])
                c.start()
                arrive[1, k, b] = c.wait
    weights = [pltpu.make_async_copy(wq_h, wq, wsem.at[0]), pltpu.make_async_copy(wp_h, wp, wsem.at[1])]
    for c in weights:
        c.start()
    emitted = []

    def emit(src, dst, r):
        c = pltpu.make_async_copy(src.at[r], dst.at[r], osem.at[len(emitted)])
        c.start()
        emitted.append(c)

    def step(m, k, r):
        if k == 0:
            x_hat, _ = layer_stats(buf[m, 0, r, :].astype(F32))
            nb = (x_hat * row(ls) + row(lb)).astype(BF)
            normed[m, r, :] = nb
            for j in range(3):
                c = slice(768 * j, 768 * j + 768)
                qkv[m, r, c] = (nn(nb, wq[:, c]) + row(bq)[:, c]).astype(BF)
            emit(buf.at[m, 0], xs_o.at[m], r)
            emit(normed.at[m], normed_o.at[m], r)
            emit(qkv.at[m], qkv_o[m], r)
        else:
            d = (buf[m, 1, r, :].astype(F32) * row(lsc)).astype(BF)
            dproj[m, r, :] = d
            do[m, r, :] = nt(d, wp[...]).astype(BF)
            emit(buf.at[m, 1], dys_o.at[m], r)
            emit(dproj.at[m], dproj_o.at[m], r)
            emit(do.at[m], do_o[m], r)

    def near(m, k):
        own, sp = local[m, k]
        own.wait()
        sp.wait()
        buf[m, k, 1024:, :] = jnp.concatenate([spec[m, k], jnp.zeros((14, 768), BF)], 0)
        step(m, k, rows(0))
        step(m, k, pl.ds(1024, 16))
        arrive[m, k, 1]()
        step(m, k, rows(1))

    def far(m, k):
        for b in (2, 3):
            arrive[m, k, b]()
            step(m, k, rows(b))

    for c in weights:
        c.wait()
    if i == 0:
        near(0, 0)
        near(0, 1)
        for c, out in later:
            c.wait()
            out.start()
        near(1, 0)
        far(0, 0)
        near(1, 1)
        far(0, 1)
    else:
        far(1, 0)
        far(1, 1)
    for c in remote:
        c.wait_send()
    for _, out in later:
        out.wait()
    for c in emitted:
        c.wait()


def front(i, patches, consts, parts, prev):
    v = lambda *s: pltpu.VMEM(s, BF)
    dma = lambda n: pltpu.SemaphoreType.DMA((n,))
    wide, thin = jax.ShapeDtypeStruct((T, 2304), BF), jax.ShapeDtypeStruct((T, 768), BF)
    out_shape = [wide, thin] + [TWO] * 4
    scratch = [v(2, 2, T, 768), v(2, 2, 2, 768), v(2, T, 2304), v(2, T, 768), v(2, T, 768), v(2, T, 768),
               v(768, 2304), v(768, 768), dma(8), dma(8), dma(48), dma(2)]
    extra = {}
    if i == 0:
        out_shape += [wide, thin] + [jax.ShapeDtypeStruct((2, 256, 768), BF)] * 2
        scratch += [dma(8), v(2, 2, 256, 768), dma(8)]
        extra = dict(collective_id=0, has_side_effects=True)
    first = 10 + len(parts)
    return pl.pallas_call(
        functools.partial(front_kernel, i, first + len(prev)),
        in_specs=[ANY] * 5 + [VM] * 3 + [ANY, VM] + [ANY] * (len(parts) + len(prev)),
        out_specs=[ANY] * len(out_shape), out_shape=out_shape, scratch_shapes=scratch,
        input_output_aliases={first + m: m for m in range(len(prev))},
        compiler_params=params(**extra),
        cost_estimate=pl.CostEstimate(flops=2 * T * 768 * 3072, bytes_accessed=24 * 1024 * 1024, transcendentals=0),
        name="front")(*patches, *consts, *parts, *prev)


def back_kernel(place, *refs):
    ins, refs = refs[:12], refs[12:]
    w_ref, wp_ref, ls, bp, lsc, give, keep, vec, buf = refs
    i = pl.program_id(0)
    blocks = ((0, 256), (256, 256), (512, 16))

    def get(s, m):
        return ins[m][256 * s:256 * s + 256, :] if s < 2 else ins[6 + m][...]

    def products(s):
        full = (lambda m: get(s, m)) if s else (lambda m: jnp.concatenate([get(0, m), get(2, m)], 0))
        dn = sum(nt(full(3 + j), w_ref[:, 768 * j:768 * j + 768]) for j in range(3))
        return nn(full(2), wp_ref[...]), dn

    def finish_rows(s, proj, dn):
        xf, dyf = get(s, 0).astype(F32), get(s, 1).astype(F32)
        x_hat, inv = layer_stats(xf)
        proj = proj + row(bp)
        dn = dn.astype(BF).astype(F32)
        gh = dn * row(ls)
        dr = inv * (gh - jnp.mean(gh, -1, keepdims=True) - x_hat * jnp.mean(gh * x_hat, -1, keepdims=True))
        r0, n = blocks[s]
        buf[0, r0:r0 + n, :] = (xf + row(lsc) * proj).astype(BF)
        buf[1, r0:r0 + n, :] = (dyf + dr).astype(BF)
        red = lambda t: jnp.sum(t, axis=0, keepdims=True)
        sums = [red(dn * x_hat), red(dn), red(dyf * row(lsc)), red(dyf * proj)] + [red(get(s, 3 + j).astype(F32)) for j in range(3)]
        return jnp.concatenate(sums + [jnp.zeros((1, 768), F32)], 0)

    p0 = products(0)
    p1 = products(1)
    v = finish_rows(0, *(t[:256] for t in p0))
    v = v + jnp.where(place[0] == 0, 1.0, 0.0) * finish_rows(2, *(t[256:] for t in p0))
    v = v + finish_rows(1, *p1)
    for k in range(2):
        keep[k, :256, :] = buf[k, pl.ds(pl.multiple_of(place[1] * 256, 256), 256), :]
        give[k, :256, :] = buf[k, pl.ds(pl.multiple_of((1 - place[1]) * 256, 256), 256), :]
        keep[k, 256:, :] = buf[k, 512:, :]
        give[k, 256:, :] = buf[k, 512:, :]

    @pl.when(i == 0)
    def _():
        vec[...] = v

    @pl.when(i == 1)
    def _():
        vec[...] += v


def back(place, xs, dys, a, dqs, w_qkv, w_proj, ln_scale, b_proj, layer_scale):
    arrays = (xs, dys, a) + tuple(dqs)
    blk = pl.BlockSpec((None, 512, 768), lambda i, c: (i, c[0], 0))
    sblk = pl.BlockSpec((None, 16, 768), lambda i, c: (i, 64, 0))
    out = pl.BlockSpec((2, None, 272, 768), lambda i, c: (0, i, 0, 0))
    half = jax.ShapeDtypeStruct((2, 2, 272, 768), BF)
    return pl.pallas_call(
        back_kernel,
        grid_spec=pltpu.PrefetchScalarGridSpec(
            num_scalar_prefetch=1, grid=(2,),
            in_specs=[blk] * 6 + [sblk] * 6 + [whole((768, 2304)), whole((768, 768))] + [VM] * 3,
            out_specs=[out, out, whole((8, 768))],
            scratch_shapes=[pltpu.VMEM((2, 528, 768), BF)]),
        out_shape=[half, half, jax.ShapeDtypeStruct((8, 768), F32)],
        compiler_params=params(),
        cost_estimate=pl.CostEstimate(flops=2 * 1056 * 768 * 3072, bytes_accessed=20 * 1024 * 1024, transcendentals=0),
        name="back")(place, *arrays, *arrays, w_qkv, w_proj, ln_scale, b_proj, layer_scale)


def finish_kernel(place, keep, got, *refs):
    ins, (gq, gp, out, dx, out_s, dx_s) = refs[:8], refs[8:]
    for m in range(3):
        gq[:, 768 * m:768 * m + 768] = ins[2 * m][...] + ins[2 * m + 1][...]
    gp[...] = ins[6][...] + ins[7][...]
    m = pl.program_id(0)
    own = (m >> 1) == place[1]

    @pl.when(own)
    def _():
        out[...] = keep[0, :256, :]
        dx[...] = keep[1, :256, :]
        out_s[...] = keep[0, 256:272, :][:2]
        dx_s[...] = keep[1, 256:272, :][:2]

    @pl.when(jnp.logical_not(own))
    def _():
        out[...] = got[0, :256, :]
        dx[...] = got[1, :256, :]
        out_s[...] = got[0, 256:272, :][:2]
        dx_s[...] = got[1, 256:272, :][:2]


def finish(place, keep, got, pairs):
    flat = [t for p in pairs for t in p]
    blk = pl.BlockSpec((192, 768), lambda g, c: (g, 0))
    src = [pl.BlockSpec((2, None, 272, 768), lambda g, c, f=f: (0, jnp.clip(g - 2 * (f ^ c[1]), 0, 1), 0, 0)) for f in (0, 1)]
    dst = pl.BlockSpec((None, 256, 768), lambda g, c: (g, 0, 0))
    dst_s = pl.BlockSpec((None, 2, 768), lambda g, c: (g, 0, 0))
    big, small = jax.ShapeDtypeStruct((4, 256, 768), BF), jax.ShapeDtypeStruct((4, 2, 768), BF)
    return pl.pallas_call(
        finish_kernel,
        grid_spec=pltpu.PrefetchScalarGridSpec(
            num_scalar_prefetch=1, grid=(4,),
            in_specs=src + [blk] * 8,
            out_specs=[pl.BlockSpec((192, 2304), lambda g, c: (g, 0)), blk, dst, dst, dst_s, dst_s]),
        out_shape=[jax.ShapeDtypeStruct((768, 2304), F32), jax.ShapeDtypeStruct((768, 768), F32), big, big, small, small],
        compiler_params=params(),
        cost_estimate=pl.CostEstimate(flops=3 * 768 * 768, bytes_accessed=36 * 768 * 768, transcendentals=0),
        name="finish")(place, keep, got, *flat)


def solution(mesh):
    n = mesh.shape['sp']
    swaps = {b: [(s, s ^ b) for s in range(n)] for b in (1, 2, 3)}

    def swap(x, b):
        return lax.ppermute(x, 'sp', swaps[b])

    def local_block(x_special, x_patch, dy_special, dy_patch, ln_scale, ln_bias, w_qkv, b_qkv, w_proj, b_proj, layer_scale):
        shard = lax.axis_index('sp')
        place = jnp.stack([shard >> 1, shard & 1])
        patches = (x_patch, dy_patch, x_special, dy_special)
        consts = (w_qkv, b_qkv, ln_scale, ln_bias, w_proj, layer_scale)
        qkv, d_attn, *saved, qkv1, d_attn1, mine, other = front(0, patches, consts, (), ())
        parts = (swap(mine, 2), swap(other, 3))
        prev = attention(0, qkv, d_attn, ())
        qkv, d_attn, *saved = front(1, patches, consts, parts, (qkv1, d_attn1, *saved))
        a, *dqs = attention(1, qkv, d_attn, prev)
        normed, xs, d_proj, dys = saved

        def tn(p, q):
            return lax.dot_general(p.reshape(2 * T, 768), q.reshape(2 * T, 768), (((0,), (0,)), ((), ())), preferred_element_type=F32)

        parts = [tn(normed, d) for d in dqs] + [tn(a, d_proj)]
        *parts, xs = lax.optimization_barrier((*parts, xs))
        pairs = [(p, swap(p, 1)) for p in parts]
        give, keep, vec = back(place, xs, dys, a, dqs, w_qkv, w_proj, ln_scale, b_proj, layer_scale)
        got = swap(give, 1)
        around = [swap(vec, b) for b in (1, 2, 3)]
        t = (vec + around[0]) + (around[1] + around[2])
        gq, gp, out, dx, out_s, dx_s = finish(place, keep, got, pairs)
        return out_s, out, dx_s, dx, t[0], t[1], gq, t[4:7].reshape(-1), gp, t[2], t[3]

    rows, seq, rep = P('dp'), P('dp', 'sp'), P()
    return jax.shard_map(local_block, mesh=mesh,
                         in_specs=(rows, seq, rows, seq) + (rep,) * 7,
                         out_specs=(rows, seq, rows, seq) + (rows,) * 7, check_vma=False)
```
